32 devices in a mesh: lon: 8 (over y, x, core), lat: 4 (over z).
Axes of the slice: x: 2, y: 2, z: 4, core: 2. Of those that a mesh axis runs over, the one named last changes fastest.
Arguments:
- surface_forcing: float32 [96, 1024], P('lat', 'lon'), may hold values from -33 to 33
- sea_mask: int32 [96, 1024], P('lat', 'lon'), may hold values 0 or 1
- level_count: int32 [96, 1024], P('lat', 'lon'), may hold values from 1 to 40
- state: float32 [4, 40, 96, 1024], P(None, None, 'lat', 'lon'), may hold values from -6 to 6
Outputs:
- surface_height: float32 [96, 1024], P('lat', 'lon')
- residual: float32 [96, 1024], P('lat', 'lon')
- tendency: float32 [4, 40, 96, 1024], P(None, None, 'lat', 'lon')
The draws below stay inside these ranges and needn't reach their ends.
All inputs are finite; a program needn't handle non-finite values. No bound on the sum of `sea_mask` on one device may be relied on, other than what follows from the above.
Results may differ from the reference program's by a relative error of at most 0.0003.
Values sent between devices are 32-bit elements; how exact they have to be, the bound alone decides.
A program may use at most 64 MiB of HBM per device.

```python
import jax
import jax.numpy as jnp
from jax import lax

LEV = 40
ITERS = 4
NX = 1024
NY = 96


def draw_surface_forcing(key, part):
    row_frac = jnp.arange(NY, dtype=jnp.float32) / NY
    column_frac = jnp.arange(NX, dtype=jnp.float32) / NX
    growth = jnp.exp(jnp.log(3.0) * (row_frac[:, None] + column_frac[None, :]))
    key_rough = jax.random.fold_in(jax.random.fold_in(key, 11), 0)
    values = jax.random.truncated_normal(key_rough, -3.0, 3.0, (NY, NX), jnp.float32) * growth
    return values


def plant(values, own_key, least, top_value):
    spot = [jax.random.randint(jax.random.fold_in(own_key, axis), (), 0, length) for axis, length in enumerate(values.shape)]
    main_axis = values.shape.index(max(values.shape))
    neighbour = spot[:main_axis] + [(spot[main_axis] + 1) % values.shape[main_axis]] + spot[main_axis + 1:]
    return values.at[tuple(spot)].set(least).at[tuple(neighbour)].set(top_value)


def shard_levels(key, shape, pieces, low, largest):
    def one(axis_at, parts):
        draws = jax.random.uniform(jax.random.fold_in(jax.random.fold_in(key, 6), axis_at), (parts,), jnp.float32, low / len(pieces), largest / len(pieces))
        return jnp.repeat(jnp.exp(draws), shape[axis_at] // parts).reshape((-1,) + (1,) * (len(shape) - axis_at - 1))

    gain = one(*pieces[0])
    for cut in pieces[1:]:
        gain = gain * one(*cut)
    return gain


def centred(key, dims, scale, most, cuts=(), kind=jnp.bfloat16):
    entries = scale * jax.random.normal(key, dims, jnp.float32)
    if cuts:
        entries = entries * shard_levels(key, dims, cuts, -0.22, 0.18)
    return jnp.clip(entries, -most, most).astype(kind)


def setup_inputs(seed: int = 0) -> dict:
    arg_keys = jax.random.split(jax.random.key(seed), 5)
    return {
        "surface_forcing": draw_surface_forcing(jax.random.fold_in(arg_keys[4], 71), 0),
        "sea_mask": plant((jax.random.randint(arg_keys[1], (NY, NX), 0, 4) < 3).astype(jnp.int32), jax.random.fold_in(arg_keys[1], 1), 0, 1),
        "level_count": plant(jax.random.randint(arg_keys[2], (NY, NX), 1, LEV + 1), jax.random.fold_in(arg_keys[2], 1), 1, LEV).astype(jnp.int32),
        "state": centred(arg_keys[3], (4, LEV, NY, NX), 1.0, 6.0, ((2, 4), (3, 8)), jnp.float32),
    }


damping = 0.05
face_scale = 1.0
viscosity = 0.02


def wrap_pad(field, width):
    field = jnp.concatenate([field[..., -width:], field, field[..., :width]], axis=-1)
    spec = [(0, 0)] * (field.ndim - 2) + [(width, width), (0, 0)]
    return jnp.pad(field, spec)


def trim_rims(field, margin):
    return field[..., margin:field.shape[-2] - margin, margin:field.shape[-1] - margin]


def face_coeffs(depth, width_out, width_in):
    offset = width_in - width_out
    height = depth.shape[0] - 2 * offset
    breadth = depth.shape[1] - 2 * offset
    center = depth[offset:offset + height, offset:offset + breadth]
    east_face = face_scale * jnp.minimum(center, depth[offset:offset + height, offset + 1:offset + 1 + breadth])
    west_face = face_scale * jnp.minimum(center, depth[offset:offset + height, offset - 1:offset - 1 + breadth])
    north_face = face_scale * jnp.minimum(center, depth[offset + 1:offset + 1 + height, offset:offset + breadth])
    south_face = face_scale * jnp.minimum(center, depth[offset - 1:offset - 1 + height, offset:offset + breadth])
    diagonal = damping + east_face + west_face + north_face + south_face
    return diagonal, east_face, west_face, north_face, south_face


def operator_apply(padded, coeffs):
    diagonal, east_face, west_face, north_face, south_face = coeffs
    return (diagonal * padded[1:-1, 1:-1] - east_face * padded[1:-1, 2:] - west_face * padded[1:-1, :-2]
            - north_face * padded[2:, 1:-1] - south_face * padded[:-2, 1:-1])


def laplace(field, active):
    center = field[..., 1:-1, 1:-1]
    active_center = active[..., 1:-1, 1:-1]
    east_part = active_center * active[..., 1:-1, 2:] * (field[..., 1:-1, 2:] - center)
    west_part = active_center * active[..., 1:-1, :-2] * (center - field[..., 1:-1, :-2])
    north_part = active_center * active[..., 2:, 1:-1] * (field[..., 2:, 1:-1] - center)
    south_part = active_center * active[..., :-2, 1:-1] * (center - field[..., :-2, 1:-1])
    return east_part - west_part + north_part - south_part


def advect(field, active):
    east_flow = field[2]
    north_flow = field[3]
    center = field[..., 1:-1, 1:-1]
    active_center = active[..., 1:-1, 1:-1]
    flow_center = east_flow[..., 1:-1, 1:-1]
    lift_center = north_flow[..., 1:-1, 1:-1]
    east_speed = 0.25 * active_center * active[..., 1:-1, 2:] * (flow_center + east_flow[..., 1:-1, 2:])
    west_speed = 0.25 * active_center * active[..., 1:-1, :-2] * (flow_center + east_flow[..., 1:-1, :-2])
    north_speed = 0.25 * active_center * active[..., 2:, 1:-1] * (lift_center + north_flow[..., 2:, 1:-1])
    south_speed = 0.25 * active_center * active[..., :-2, 1:-1] * (lift_center + north_flow[..., :-2, 1:-1])
    return (east_speed * (center + field[..., 1:-1, 2:]) - west_speed * (center + field[..., 1:-1, :-2])
            + north_speed * (center + field[..., 2:, 1:-1]) - south_speed * (center + field[..., :-2, 1:-1]))


def tendency_of(state_wide, active_wide):
    inner_active = trim_rims(active_wide, 1)
    smoothed = laplace(laplace(state_wide, active_wide), inner_active)
    flux = advect(trim_rims(state_wide, 1), inner_active)
    return trim_rims(active_wide, 2) * (-flux - viscosity * smoothed)


def reference(surface_forcing, sea_mask, level_count, state):
    sea = sea_mask.astype(jnp.float32)
    depth = sea * level_count.astype(jnp.float32) / LEV
    coeffs = face_coeffs(wrap_pad(depth, 1), 0, 1)
    forcing = sea * surface_forcing
    solution = jnp.zeros_like(forcing)
    residual = forcing
    search = residual / coeffs[0]
    direction = search
    product = jnp.sum(residual * search)
    for step_index in range(ITERS):
        image = operator_apply(wrap_pad(direction, 1), coeffs)
        alpha_step = product / jnp.sum(direction * image)
        solution = solution + alpha_step * direction
        residual = residual - alpha_step * image
        if step_index + 1 < ITERS:
            search = residual / coeffs[0]
            product_next = jnp.sum(residual * search)
            direction = search + (product_next / product) * direction
            product = product_next

    def level_tendency(level):
        active = (level < level_count).astype(jnp.float32) * sea
        layer = lax.dynamic_index_in_dim(state, level, 1, keepdims=False)
        return tendency_of(wrap_pad(layer, 2), wrap_pad(active, 2))

    stacked = lax.map(level_tendency, jnp.arange(LEV, dtype=jnp.int32))
    return solution, residual, jnp.moveaxis(stacked, 0, 1)
```

```python
import functools

import jax
import jax.numpy as jnp
from jax import lax
from jax.experimental import pallas as pl
from jax.experimental.pallas import tpu as pltpu
from jax.sharding import PartitionSpec as P

ITERS = 4
DAMPING = 0.05
VISCOSITY = 0.02
SUB = 8
MESH = pl.DeviceIdType.MESH


def east(a, b, lane):
    ra, rb = pltpu.roll(a, 127, 1), pltpu.roll(b, 127, 1)
    keep = lane < 127
    return jnp.where(keep, ra, rb), jnp.where(keep, rb, ra)


def west(a, b, lane):
    ra, rb = pltpu.roll(a, 1, 1), pltpu.roll(b, 1, 1)
    keep = lane > 0
    return jnp.where(keep, ra, rb), jnp.where(keep, rb, ra)


def north(x):
    return pltpu.roll(x, x.shape[0] - 1, 0)


def south(x):
    return pltpu.roll(x, 1, 0)


def exchange(
    sizes,
    forcing_ref, sea_ref, count_ref, state_ref,
    tend_ref, basis_ref, diag_ref, total_ref,
    force_buf, sea_buf, count_buf, q_ref, lap_ref, near_ref,
    pack_ref, side_ref, pair_ref, vert_ref,
    strip_out, strip_in, corner_out, corner_in, center_ref, slap_ref,
    part_ref, lon_in, mid_ref, lat_in,
    load_sem, side_sem, vert_sem, strip_sem, row_sem, corner_sem, lon_sem, lat_sem,
):
    n_lon, n_lat, fields, levels, rows = sizes
    planes = fields * levels
    depth_tiles = levels // SUB
    tiles = planes // SUB
    ilon, ilat = lax.axis_index("lon"), lax.axis_index("lat")
    has = {1: ilat < n_lat - 1, -1: ilat > 0}

    def at(dlon, dlat):
        return {
            "lon": lax.rem(ilon + dlon + n_lon, n_lon),
            "lat": lax.rem(ilat + dlat + n_lat, n_lat),
        }

    barrier = pltpu.get_barrier_semaphore()
    for off in range(1, n_lon):
        pl.semaphore_signal(barrier, inc=1, device_id=at(off, 0), device_id_type=MESH)
    for off in range(1, n_lat):
        pl.semaphore_signal(barrier, inc=1, device_id=at(0, off), device_id_type=MESH)
    for dlon, dlat in ((-1, -1), (1, -1), (-1, 1), (1, 1)):
        pl.semaphore_signal(barrier, inc=1, device_id=at(dlon, dlat), device_id_type=MESH)

    inputs = [
        pltpu.make_async_copy(src, dst, load_sem.at[i])
        for i, (src, dst) in enumerate(((forcing_ref, force_buf), (sea_ref, sea_buf), (count_ref, count_buf)))
    ]
    for load in inputs:
        load.start()
    for j in range(rows):
        pltpu.make_async_copy(state_ref.at[:, j, :], q_ref.at[j + 2, pl.ds(0, planes)], load_sem.at[3]).start()

    def remote(src, dst, sems, index, where):
        return pltpu.make_async_remote_copy(
            src_ref=src, dst_ref=dst, send_sem=sems.at[(0,) + index], recv_sem=sems.at[(1,) + index],
            device_id=where, device_id_type=MESH,
        )

    def drained(ref, sems, index):
        pltpu.make_async_copy(ref, ref, sems.at[index]).wait()

    lane8 = lax.broadcasted_iota(jnp.int32, (SUB, 128), 1)
    sub8 = lax.broadcasted_iota(jnp.int32, (SUB, 128), 0)
    kio = [(sub8 + SUB * t).astype(jnp.float32) for t in range(depth_tiles)]
    slot8 = lane8 % 4
    last_lane, first_lane = lane8 == 127, lane8 == 0
    own = pl.ds(planes, SUB)

    def tile(t):
        return pl.ds(SUB * t, SUB)

    sides = ((0, -1, 0), (1, 1, rows - SUB))
    for v, dlat, _ in sides:
        @pl.when(jnp.logical_not(has[-dlat]))
        def _(v=v):
            vert_ref[v] = jnp.zeros_like(vert_ref[v])
            corner_in[v] = jnp.zeros_like(corner_in[v])
            for r in range(2):
                jj = rows + 2 + r if v == 0 else r
                q_ref[jj] = jnp.zeros_like(q_ref[jj])

    for load in inputs:
        load.wait()
    lane_r = lax.broadcasted_iota(jnp.int32, (rows, 128), 1)
    sea = sea_buf[...].astype(jnp.float32)
    wet = sea * count_buf[...].astype(jnp.float32)
    force = sea * force_buf[...]
    pair_ref[0] = force
    pair_ref[1] = wet
    inner_half = jnp.where(lane_r < 64, pltpu.roll(wet, 32, 1), pltpu.roll(wet, 96, 1))
    pack_ref[...] = jnp.where((lane_r >= 32) & (lane_r < 96), inner_half, force)
    for j in range(rows):
        q_ref[j + 2, own, :] = jnp.broadcast_to(wet[j : j + 1], (SUB, 128))

    pl.semaphore_wait(barrier, n_lon + n_lat + 2)

    for h, dlon in ((0, 1), (1, -1)):
        remote(pack_ref, side_ref.at[h], side_sem, (), at(dlon, 0)).start()
    for v, dlat, start in sides:
        @pl.when(has[dlat])
        def _(v=v, dlat=dlat, start=start):
            part = pl.ds(start, SUB)
            for h, dlon in ((0, 1), (1, -1)):
                remote(pack_ref.at[part], vert_ref.at[v, 2 + h], vert_sem, (v,), at(dlon, dlat)).start()
            remote(pair_ref.at[:, part], vert_ref.at[v, pl.ds(0, 2)], vert_sem, (v,), at(0, dlat)).start()

    pltpu.make_async_copy(
        q_ref.at[pl.ds(2, rows), pl.ds(0, planes)], q_ref.at[pl.ds(2, rows), pl.ds(0, planes)], load_sem.at[3]
    ).wait()

    packed = [jnp.zeros((SUB, 128), jnp.float32)] * (tiles + 1)
    for j in range(rows):
        here = lane8 // 4 == j + 1
        level = q_ref[j + 2, own, :]
        active = [k < level for k in kio]
        for t in range(tiles + 1):
            if t < tiles:
                q = jnp.where(active[t % depth_tiles], q_ref[j + 2, tile(t), :], 0.0)
                q_ref[j + 2, tile(t), :] = q
            else:
                q = level
            packed[t] = jnp.where(here, pltpu.roll(q, 4 * (j + 1) + 2, 1), packed[t])
    corners = [jnp.zeros((SUB, 128), jnp.float32)] * 2
    for t in range(tiles + 1):
        strip_out[tile(t), :] = packed[t]
        for v, j in ((0, 0), (1, rows - 1)):
            moved = pltpu.roll(packed[t], (4 * t - 4 * (j + 1)) % 128, 1)
            corners[v] = jnp.where(lane8 // 4 == t, moved, corners[v])
    for v in range(2):
        corner_out[v] = corners[v]

    for h, dlon in ((0, 1), (1, -1)):
        remote(strip_out, strip_in.at[h], strip_sem, (), at(dlon, 0)).start()
    for v, dlat, _ in sides:
        @pl.when(has[dlat])
        def _(v=v, dlat=dlat):
            mine = pl.ds(2, 2) if v == 0 else pl.ds(rows, 2)
            there = pl.ds(rows + 2, 2) if v == 0 else pl.ds(0, 2)
            for h, dlon in ((0, 1), (1, -1)):
                remote(corner_out.at[v], corner_in.at[v, h], corner_sem, (v,), at(dlon, dlat)).start()
            remote(q_ref.at[mine], q_ref.at[there], row_sem, (v,), at(0, dlat)).start()

    def received(ref, sems, v, dlat):
        @pl.when(has[-dlat])
        def _():
            drained(ref, sems, (1, v))

    drained(side_ref, side_sem, (1,))
    for v, dlat, _ in sides:
        received(vert_ref.at[v], vert_sem, v, dlat)

    from_west = jnp.concatenate([side_ref[0], vert_ref[0, 2], vert_ref[1, 2]], axis=0)
    from_east = jnp.concatenate([side_ref[1], vert_ref[0, 3], vert_ref[1, 3]], axis=0)
    lane_t = lax.broadcasted_iota(jnp.int32, (rows + 2 * SUB, 128), 1)
    low = lane_t < 64
    force_a = jnp.concatenate([pair_ref[0], vert_ref[0, 0], vert_ref[1, 0]], axis=0)
    wet_a = jnp.concatenate([pair_ref[1], vert_ref[0, 1], vert_ref[1, 1]], axis=0)
    force_b = jnp.where(low, from_east, from_west)
    wet_b = jnp.where(low, pltpu.roll(from_east, 96, 1), pltpu.roll(from_west, 32, 1))
    depth_a, depth_b = wet_a / levels, wet_b / levels
    da, db = east(depth_a, depth_b, lane_t)
    ea, eb = jnp.minimum(depth_a, da), jnp.minimum(depth_b, db)
    wa, wb = west(ea, eb, lane_t)
    na, nb = jnp.minimum(depth_a, north(depth_a)), jnp.minimum(depth_b, north(depth_b))
    sa, sb = south(na), south(nb)
    diag_a = DAMPING + ea + wa + na + sa
    diag_b = DAMPING + eb + wb + nb + sb
    inv_a, inv_b = 1.0 / diag_a, 1.0 / diag_b
    va, vb = force_a * inv_a, force_b * inv_b
    ea, wa, na, sa = (c * inv_a for c in (ea, wa, na, sa))
    eb, wb, nb, sb = (c * inv_b for c in (eb, wb, nb, sb))
    diag = diag_a[:rows]
    diag_ref[...] = diag
    basis = [va[:rows]]
    for _ in range(ITERS):
        qe, qeb = east(va, vb, lane_t)
        qw, qwb = west(va, vb, lane_t)
        va, vb = (
            ea * qe + wa * qw + na * north(va) + sa * south(va),
            eb * qeb + wb * qwb + nb * north(vb) + sb * south(vb),
        )
        basis.append(va[:rows])
    for i, x in enumerate(basis):
        basis_ref[i] = x
    moments = []
    for m in range(2 * ITERS):
        moments.append(jnp.sum(diag * basis[m // 2] * basis[(m + 1) // 2], axis=0, keepdims=True))
    part_ref[...] = jnp.concatenate(moments, axis=0)
    for off in range(1, n_lon):
        remote(part_ref, lon_in.at[off - 1], lon_sem, (), at(off, 0)).start()

    drained(strip_in, strip_sem, (1,))
    for v, dlat, _ in sides:
        received(corner_in.at[v], corner_sem, v, dlat)

    def swap(x, step):
        return jnp.where(slot8 < 2, pltpu.roll(x, 128 - step, 1), pltpu.roll(x, step, 1))

    def arrange(t):
        g = jnp.where(slot8 < 2, strip_in[0, tile(t), :], strip_in[1, tile(t), :])
        for v, j in ((0, rows), (1, -1)):
            corner = jnp.where(slot8 < 2, corner_in[v, 0], corner_in[v, 1])
            moved = pltpu.roll(corner, (4 * (j + 1) - 4 * t) % 128, 1)
            g = jnp.where(lane8 // 4 == j + 1, moved, g)
        center = swap(g, 1)
        return center, strip_out[tile(t), :], swap(g, 2), pltpu.roll(center, 124, 1), pltpu.roll(center, 4, 1)

    ring = arrange(tiles)
    center_ref[tile(tiles), :] = ring[0]
    edge_coef = []
    for k in kio:
        count = sum(jnp.where(k < w, 1.0, 0.0) for w in ring[1:])
        first = jnp.where(k < ring[0], -VISCOSITY, 0.0)
        edge_coef.append((first, first * count))
    for t in range(tiles):
        center, a, b, c, d = arrange(t)
        center_ref[tile(t), :] = center
        first, second = edge_coef[t % depth_tiles]
        slap_ref[tile(t), :] = first * ((a + b) + (c + d)) - second * center

    def beside(x, edge):
        return (
            jnp.where(last_lane, edge, pltpu.roll(x, 127, 1)),
            jnp.where(first_lane, edge, pltpu.roll(x, 1, 1)),
        )

    def laplace(jj, inside):
        shift = 130 - 4 * jj
        level = q_ref[jj, own, :]
        around = beside(level, pltpu.roll(center_ref[own, :], shift, 1)) + (q_ref[jj + 1, own, :], q_ref[jj - 1, own, :])
        for k in range(depth_tiles):
            here, oe, ow, on, os = (kio[k] < x for x in (level,) + around)
            ones = [jnp.where(x, 1.0, 0.0) for x in (oe, ow, on, os)]
            count = (ones[0] + ones[1]) + (ones[2] + ones[3])
            first = jnp.where(here, -VISCOSITY, 0.0)
            second = first * count

            def plane(f):
                at_tile = tile(f * depth_tiles + k)
                q = q_ref[jj, at_tile, :]
                qe, qw = beside(q, pltpu.roll(center_ref[at_tile, :], shift, 1))
                qn, qs = q_ref[jj + 1, at_tile, :], q_ref[jj - 1, at_tile, :]
                lap_ref[jj - 1, at_tile, :] = first * ((qe + qw) + (qn + qs)) - second * q
                return q, qe, qw, qn, qs

            if not inside:
                for f in range(fields):
                    plane(f)
                continue
            near_ref[jj - 2, tile(k), :] = count
            quarter = jnp.where(here, 0.25, 0.0)
            planes_of = {2: plane(2), 3: plane(3)}
            u, ue, uw, _, _ = planes_of[2]
            v, _, _, vn, vs = planes_of[3]
            fe = jnp.where(oe, quarter * (u + ue), 0.0)
            fw = jnp.where(ow, quarter * (u + uw), 0.0)
            fn = jnp.where(on, quarter * (v + vn), 0.0)
            fs = jnp.where(os, quarter * (v + vs), 0.0)
            net = (fw - fe) + (fs - fn)
            for f in (2, 3, 0, 1):
                q, qe, qw, qn, qs = planes_of[f] if f in planes_of else plane(f)
                tend_ref[jj - 2, tile(f * depth_tiles + k), :] = (
                    net * q + (fw * qw - fe * qe) + (fs * qs - fn * qn)
                )

    def finish(j):
        shift = 122 - 4 * j
        level = q_ref[j + 2, own, :]
        for k in range(depth_tiles):
            here = kio[k] < level
            count = near_ref[j, tile(k), :]
            for f in range(fields):
                at_tile = tile(f * depth_tiles + k)
                lap = lap_ref[j + 1, at_tile, :]
                le, lw = beside(lap, pltpu.roll(slap_ref[at_tile, :], shift, 1))
                total = (le + lw) + (lap_ref[j + 2, at_tile, :] + lap_ref[j, at_tile, :])
                tend_ref[j, at_tile, :] += jnp.where(here, total, 0.0) - count * lap

    def sweep(fn, start, stop, unroll):
        assert (stop - start) % unroll == 0

        def body(i, carry):
            for r in range(unroll):
                fn(start + unroll * i + r)
            return carry

        lax.fori_loop(0, (stop - start) // unroll, body, 0)

    sweep(lambda jj: laplace(jj, True), 3, rows + 1, 2)

    drained(lon_in, lon_sem, (1,))
    total = part_ref[...]
    for i in range(n_lon - 1):
        total = total + lon_in[i]
    mid_ref[...] = total
    for off in range(1, n_lat):
        remote(mid_ref, lat_in.at[off - 1], lat_sem, (), at(0, off)).start()

    sweep(finish, 2, rows - 2, 2)

    for v, dlat, _ in sides:
        rim = q_ref.at[pl.ds(rows + 2, 2)] if v == 0 else q_ref.at[pl.ds(0, 2)]
        received(rim, row_sem, v, dlat)
    for jj, inside in ((1, False), (2, True), (rows + 1, True), (rows + 2, False)):
        laplace(jj, inside)
    for j in (0, 1, rows - 2, rows - 1):
        finish(j)

    drained(lat_in, lat_sem, (1,))
    total = mid_ref[...]
    for i in range(n_lat - 1):
        total = total + lat_in[i]
    total_ref[...] = total

    drained(side_ref, side_sem, (0,))
    drained(strip_in, strip_sem, (0,))
    drained(lon_in, lon_sem, (0,))
    drained(lat_in, lat_sem, (0,))
    for v, dlat, _ in sides:
        @pl.when(has[dlat])
        def _(v=v):
            drained(vert_ref.at[v], vert_sem, (0, v))
            drained(corner_in.at[v], corner_sem, (0, v))
            drained(q_ref.at[pl.ds(0, 2)], row_sem, (0, v))


def deliver(tend_in, basis_in, diag_in, total_in, height_ref, resid_ref, tend_ref, height_buf, resid_buf, sem):
    rows = tend_in.shape[0]
    stores = [pltpu.make_async_copy(tend_in.at[j], tend_ref.at[:, j, :], sem.at[0]) for j in range(rows)]
    for store in stores:
        store.start()
    total = jnp.broadcast_to(jnp.sum(total_in[...], axis=1, keepdims=True), (2 * ITERS, 128))
    mu = [total[m : m + 1] for m in range(2 * ITERS)]

    def inner(x, y):
        sums = [None] * (len(x) + len(y) - 1)
        for i, xi in enumerate(x):
            for j, yj in enumerate(y):
                sums[i + j] = xi * yj if sums[i + j] is None else sums[i + j] + xi * yj
        out = sums[0] * mu[0]
        for m in range(1, len(sums)):
            out = out + sums[m] * mu[m]
        return out

    one = jnp.ones((1, 128), jnp.float32)
    zero = jnp.zeros((1, 128), jnp.float32)
    z, p, h = [one], [one], []
    rz = mu[0]
    for it in range(ITERS):
        image = [hi - lo for hi, lo in zip(p + [zero], [zero] + p)]
        alpha = rz / inner(p, image)
        h = [x + alpha * y for x, y in zip(h + [zero], p)]
        z = [x - alpha * y for x, y in zip(z + [zero], image)]
        if it + 1 < ITERS:
            new = inner(z, z)
            beta = new / rz
            p = [x + beta * y for x, y in zip(z, p + [zero])]
            rz = new
    height = h[0] * basis_in[0]
    for i in range(1, ITERS):
        height = height + h[i] * basis_in[i]
    resid = z[0] * basis_in[0]
    for i in range(1, ITERS + 1):
        resid = resid + z[i] * basis_in[i]
    height_buf[...] = height
    resid_buf[...] = diag_in[...] * resid
    last = [
        pltpu.make_async_copy(height_buf, height_ref, sem.at[1]),
        pltpu.make_async_copy(resid_buf, resid_ref, sem.at[2]),
    ]
    for store in last:
        store.start()
    pltpu.make_async_copy(tend_in, tend_in, sem.at[0]).wait()
    for store in last:
        store.wait()


def per_device(n_lon, n_lat, forcing, sea, count, state):
    fields, levels, rows, width = state.shape
    planes = fields * levels
    tall = planes + SUB
    assert levels % SUB == 0 and width == 128 and rows % SUB == 0 and rows >= 2 * SUB
    assert 4 * (rows + 2) <= width and 4 * (planes // SUB + 1) <= width
    sizes = (n_lon, n_lat, fields, levels, rows)
    f32 = jnp.float32
    vmem = pl.BlockSpec(memory_space=pltpu.VMEM)
    hbm = pl.BlockSpec(memory_space=pltpu.HBM)
    dma = pltpu.SemaphoreType.DMA
    held = pl.pallas_call(
        functools.partial(exchange, sizes),
        out_shape=(
            pltpu.VMEM((rows, planes, width), f32),
            pltpu.VMEM((ITERS + 1, rows, width), f32),
            pltpu.VMEM((rows, width), f32),
            pltpu.VMEM((2 * ITERS, width), f32),
        ),
        in_specs=[hbm] * 4,
        out_specs=(vmem,) * 4,
        scratch_shapes=[
            pltpu.VMEM((rows, width), f32),
            pltpu.VMEM((rows, width), jnp.int32),
            pltpu.VMEM((rows, width), jnp.int32),
            pltpu.VMEM((rows + 4, tall, width), f32),
            pltpu.VMEM((rows + 2, planes, width), f32),
            pltpu.VMEM((rows, levels, width), f32),
            pltpu.VMEM((rows, width), f32),
            pltpu.VMEM((2, rows, width), f32),
            pltpu.VMEM((2, rows, width), f32),
            pltpu.VMEM((2, 4, SUB, width), f32),
            pltpu.VMEM((tall, width), f32),
            pltpu.VMEM((2, tall, width), f32),
            pltpu.VMEM((2, SUB, width), f32),
            pltpu.VMEM((2, 2, SUB, width), f32),
            pltpu.VMEM((tall, width), f32),
            pltpu.VMEM((planes, width), f32),
            pltpu.VMEM((2 * ITERS, width), f32),
            pltpu.VMEM((n_lon - 1, 2 * ITERS, width), f32),
            pltpu.VMEM((2 * ITERS, width), f32),
            pltpu.VMEM((n_lat - 1, 2 * ITERS, width), f32),
            dma((4,)),
            dma((2,)),
            dma((2, 2)),
            dma((2,)),
            dma((2, 2)),
            dma((2, 2)),
            dma((2,)),
            dma((2,)),
        ],
        compiler_params=pltpu.CompilerParams(collective_id=0, has_side_effects=True, vmem_limit_bytes=24 << 20),
    )(forcing, sea, count, state.reshape(planes, rows, width))
    small = jax.ShapeDtypeStruct((rows, width), f32)
    height, resid, tend = pl.pallas_call(
        deliver,
        out_shape=(small, small, jax.ShapeDtypeStruct((planes, rows, width), f32)),
        in_specs=[vmem] * 4,
        out_specs=(hbm,) * 3,
        scratch_shapes=[
            pltpu.VMEM((rows, width), f32),
            pltpu.VMEM((rows, width), f32),
            dma((3,)),
        ],
        compiler_params=pltpu.CompilerParams(vmem_limit_bytes=16 << 20),
    )(*held)
    return height, resid, tend.reshape(state.shape)


def solution(mesh):
    return jax.shard_map(
        functools.partial(per_device, mesh.shape["lon"], mesh.shape["lat"]),
        mesh=mesh,
        in_specs=(P("lat", "lon"), P("lat", "lon"), P("lat", "lon"), P(None, None, "lat", "lon")),
        out_specs=(P("lat", "lon"), P("lat", "lon"), P(None, None, "lat", "lon")),
        check_vma=False,
    )
```

```python
import functools

import jax
import jax.numpy as jnp
from jax import lax
from jax.experimental import pallas as pl
from jax.experimental.pallas import tpu as pltpu
from jax.sharding import PartitionSpec as P

ITERS = 4
DAMPING = 0.05
VISCOSITY = 0.02
SUB = 8
MESH = pl.DeviceIdType.MESH


def east(a, b, lane):
    ra, rb = pltpu.roll(a, 127, 1), pltpu.roll(b, 127, 1)
    keep = lane < 127
    return jnp.where(keep, ra, rb), jnp.where(keep, rb, ra)


def west(a, b, lane):
    ra, rb = pltpu.roll(a, 1, 1), pltpu.roll(b, 1, 1)
    keep = lane > 0
    return jnp.where(keep, ra, rb), jnp.where(keep, rb, ra)


def north(x):
    return pltpu.roll(x, x.shape[0] - 1, 0)


def south(x):
    return pltpu.roll(x, 1, 0)


def exchange(
    sizes,
    forcing_ref, sea_ref, count_ref, state_ref,
    tend_ref, basis_ref, diag_ref, total_ref,
    force_buf, sea_buf, count_buf, q_ref, lap_ref, near_ref,
    pack_ref, side_ref, pair_ref, vert_ref,
    strip_out, strip_in, corner_out, corner_in, center_ref, slap_ref,
    part_ref, lon_in, mid_ref, lat_in,
    load_sem, side_sem, vert_sem, strip_sem, row_sem, corner_sem, lon_sem, lat_sem,
):
    n_lon, n_lat, fields, levels, rows = sizes
    planes = fields * levels
    depth_tiles = levels // SUB
    tiles = planes // SUB
    ilon, ilat = lax.axis_index("lon"), lax.axis_index("lat")
    has = {1: ilat < n_lat - 1, -1: ilat > 0}

    def at(dlon, dlat):
        return {
            "lon": lax.rem(ilon + dlon + n_lon, n_lon),
            "lat": lax.rem(ilat + dlat + n_lat, n_lat),
        }

    barrier = pltpu.get_barrier_semaphore()
    for off in range(1, n_lon):
        pl.semaphore_signal(barrier, inc=1, device_id=at(off, 0), device_id_type=MESH)
    for off in range(1, n_lat):
        pl.semaphore_signal(barrier, inc=1, device_id=at(0, off), device_id_type=MESH)
    for dlon, dlat in ((-1, -1), (1, -1), (-1, 1), (1, 1)):
        pl.semaphore_signal(barrier, inc=1, device_id=at(dlon, dlat), device_id_type=MESH)

    inputs = [
        pltpu.make_async_copy(src, dst, load_sem.at[i])
        for i, (src, dst) in enumerate(((forcing_ref, force_buf), (sea_ref, sea_buf), (count_ref, count_buf)))
    ]
    for load in inputs:
        load.start()
    for j in range(rows):
        pltpu.make_async_copy(state_ref.at[:, j, :], q_ref.at[j + 2, pl.ds(0, planes)], load_sem.at[3]).start()

    def remote(src, dst, sems, index, where):
        return pltpu.make_async_remote_copy(
            src_ref=src, dst_ref=dst, send_sem=sems.at[(0,) + index], recv_sem=sems.at[(1,) + index],
            device_id=where, device_id_type=MESH,
        )

    def drained(ref, sems, index):
        pltpu.make_async_copy(ref, ref, sems.at[index]).wait()

    lane8 = lax.broadcasted_iota(jnp.int32, (SUB, 128), 1)
    sub8 = lax.broadcasted_iota(jnp.int32, (SUB, 128), 0)
    kio = [(sub8 + SUB * t).astype(jnp.float32) for t in range(depth_tiles)]
    slot8 = lane8 % 4
    last_lane, first_lane = lane8 == 127, lane8 == 0
    own = pl.ds(planes, SUB)

    def tile(t):
        return pl.ds(SUB * t, SUB)

    sides = ((0, -1, 0), (1, 1, rows - SUB))
    for v, dlat, _ in sides:
        @pl.when(jnp.logical_not(has[-dlat]))
        def _(v=v):
            vert_ref[v] = jnp.zeros_like(vert_ref[v])
            corner_in[v] = jnp.zeros_like(corner_in[v])
            for r in range(2):
                jj = rows + 2 + r if v == 0 else r
                q_ref[jj] = jnp.zeros_like(q_ref[jj])

    for load in inputs:
        load.wait()
    lane_r = lax.broadcasted_iota(jnp.int32, (rows, 128), 1)
    sea = sea_buf[...].astype(jnp.float32)
    wet = sea * count_buf[...].astype(jnp.float32)
    force = sea * force_buf[...]
    pair_ref[0] = force
    pair_ref[1] = wet
    inner_half = jnp.where(lane_r < 64, pltpu.roll(wet, 32, 1), pltpu.roll(wet, 96, 1))
    pack_ref[...] = jnp.where((lane_r >= 32) & (lane_r < 96), inner_half, force)
    for j in range(rows):
        q_ref[j + 2, own, :] = jnp.broadcast_to(wet[j : j + 1], (SUB, 128))

    pl.semaphore_wait(barrier, n_lon + n_lat + 2)

    for h, dlon in ((0, 1), (1, -1)):
        remote(pack_ref, side_ref.at[h], side_sem, (), at(dlon, 0)).start()
    for v, dlat, start in sides:
        @pl.when(has[dlat])
        def _(v=v, dlat=dlat, start=start):
            part = pl.ds(start, SUB)
            for h, dlon in ((0, 1), (1, -1)):
                remote(pack_ref.at[part], vert_ref.at[v, 2 + h], vert_sem, (v,), at(dlon, dlat)).start()
            remote(pair_ref.at[:, part], vert_ref.at[v, pl.ds(0, 2)], vert_sem, (v,), at(0, dlat)).start()

    pltpu.make_async_copy(
        q_ref.at[pl.ds(2, rows), pl.ds(0, planes)], q_ref.at[pl.ds(2, rows), pl.ds(0, planes)], load_sem.at[3]
    ).wait()

    packed = [jnp.zeros((SUB, 128), jnp.float32)] * (tiles + 1)
    for j in range(rows):
        here = lane8 // 4 == j + 1
        level = q_ref[j + 2, own, :]
        active = [k < level for k in kio]
        for t in range(tiles + 1):
            if t < tiles:
                q = jnp.where(active[t % depth_tiles], q_ref[j + 2, tile(t), :], 0.0)
                q_ref[j + 2, tile(t), :] = q
            else:
                q = level
            packed[t] = jnp.where(here, pltpu.roll(q, 4 * (j + 1) + 2, 1), packed[t])
    corners = [jnp.zeros((SUB, 128), jnp.float32)] * 2
    for t in range(tiles + 1):
        strip_out[tile(t), :] = packed[t]
        for v, j in ((0, 0), (1, rows - 1)):
            moved = pltpu.roll(packed[t], (4 * t - 4 * (j + 1)) % 128, 1)
            corners[v] = jnp.where(lane8 // 4 == t, moved, corners[v])
    for v in range(2):
        corner_out[v] = corners[v]

    for h, dlon in ((0, 1), (1, -1)):
        remote(strip_out, strip_in.at[h], strip_sem, (), at(dlon, 0)).start()
    for v, dlat, _ in sides:
        @pl.when(has[dlat])
        def _(v=v, dlat=dlat):
            mine = pl.ds(2, 2) if v == 0 else pl.ds(rows, 2)
            there = pl.ds(rows + 2, 2) if v == 0 else pl.ds(0, 2)
            for h, dlon in ((0, 1), (1, -1)):
                remote(corner_out.at[v], corner_in.at[v, h], corner_sem, (v,), at(dlon, dlat)).start()
            remote(q_ref.at[mine], q_ref.at[there], row_sem, (v,), at(0, dlat)).start()

    def received(ref, sems, v, dlat):
        @pl.when(has[-dlat])
        def _():
            drained(ref, sems, (1, v))

    drained(side_ref, side_sem, (1,))
    for v, dlat, _ in sides:
        received(vert_ref.at[v], vert_sem, v, dlat)

    from_west = jnp.concatenate([side_ref[0], vert_ref[0, 2], vert_ref[1, 2]], axis=0)
    from_east = jnp.concatenate([side_ref[1], vert_ref[0, 3], vert_ref[1, 3]], axis=0)
    lane_t = lax.broadcasted_iota(jnp.int32, (rows + 2 * SUB, 128), 1)
    low = lane_t < 64
    force_a = jnp.concatenate([pair_ref[0], vert_ref[0, 0], vert_ref[1, 0]], axis=0)
    wet_a = jnp.concatenate([pair_ref[1], vert_ref[0, 1], vert_ref[1, 1]], axis=0)
    force_b = jnp.where(low, from_east, from_west)
    wet_b = jnp.where(low, pltpu.roll(from_east, 96, 1), pltpu.roll(from_west, 32, 1))
    depth_a, depth_b = wet_a / levels, wet_b / levels
    da, db = east(depth_a, depth_b, lane_t)
    ea, eb = jnp.minimum(depth_a, da), jnp.minimum(depth_b, db)
    wa, wb = west(ea, eb, lane_t)
    na, nb = jnp.minimum(depth_a, north(depth_a)), jnp.minimum(depth_b, north(depth_b))
    sa, sb = south(na), south(nb)
    diag_a = DAMPING + ea + wa + na + sa
    diag_b = DAMPING + eb + wb + nb + sb
    inv_a, inv_b = 1.0 / diag_a, 1.0 / diag_b
    va, vb = force_a * inv_a, force_b * inv_b
    ea, wa, na, sa = (c * inv_a for c in (ea, wa, na, sa))
    eb, wb, nb, sb = (c * inv_b for c in (eb, wb, nb, sb))
    diag = diag_a[:rows]
    diag_ref[...] = diag
    basis = [va[:rows]]
    for _ in range(ITERS):
        qe, qeb = east(va, vb, lane_t)
        qw, qwb = west(va, vb, lane_t)
        va, vb = (
            ea * qe + wa * qw + na * north(va) + sa * south(va),
            eb * qeb + wb * qwb + nb * north(vb) + sb * south(vb),
        )
        basis.append(va[:rows])
    for i, x in enumerate(basis):
        basis_ref[i] = x
    moments = []
    for m in range(2 * ITERS):
        moments.append(jnp.sum(diag * basis[m // 2] * basis[(m + 1) // 2], axis=0, keepdims=True))
    part_ref[...] = jnp.concatenate(moments, axis=0)
    for off in range(1, n_lon):
        remote(part_ref, lon_in.at[off - 1], lon_sem, (), at(off, 0)).start()

    drained(strip_in, strip_sem, (1,))
    for v, dlat, _ in sides:
        received(corner_in.at[v], corner_sem, v, dlat)

    def swap(x, step):
        return jnp.where(slot8 < 2, pltpu.roll(x, 128 - step, 1), pltpu.roll(x, step, 1))

    def arrange(t):
        g = jnp.where(slot8 < 2, strip_in[0, tile(t), :], strip_in[1, tile(t), :])
        for v, j in ((0, rows), (1, -1)):
            corner = jnp.where(slot8 < 2, corner_in[v, 0], corner_in[v, 1])
            moved = pltpu.roll(corner, (4 * (j + 1) - 4 * t) % 128, 1)
            g = jnp.where(lane8 // 4 == j + 1, moved, g)
        center = swap(g, 1)
        return center, strip_out[tile(t), :], swap(g, 2), pltpu.roll(center, 124, 1), pltpu.roll(center, 4, 1)

    ring = arrange(tiles)
    center_ref[tile(tiles), :] = ring[0]
    edge_coef = []
    for k in kio:
        count = sum(jnp.where(k < w, 1.0, 0.0) for w in ring[1:])
        first = jnp.where(k < ring[0], -VISCOSITY, 0.0)
        edge_coef.append((first, first * count))
    for t in range(tiles):
        center, a, b, c, d = arrange(t)
        center_ref[tile(t), :] = center
        first, second = edge_coef[t % depth_tiles]
        slap_ref[tile(t), :] = first * ((a + b) + (c + d)) - second * center

    def beside(x, edge):
        return (
            jnp.where(last_lane, edge, pltpu.roll(x, 127, 1)),
            jnp.where(first_lane, edge, pltpu.roll(x, 1, 1)),
        )

    def laplace(jj, inside):
        shift = 130 - 4 * jj
        level = q_ref[jj, own, :]
        around = beside(level, pltpu.roll(center_ref[own, :], shift, 1)) + (q_ref[jj + 1, own, :], q_ref[jj - 1, own, :])
        for k in range(depth_tiles):
            here, oe, ow, on, os = (kio[k] < x for x in (level,) + around)
            ones = [jnp.where(x, 1.0, 0.0) for x in (oe, ow, on, os)]
            count = (ones[0] + ones[1]) + (ones[2] + ones[3])
            first = jnp.where(here, -VISCOSITY, 0.0)
            second = first * count

            def plane(f):
                at_tile = tile(f * depth_tiles + k)
                q = q_ref[jj, at_tile, :]
                qe, qw = beside(q, pltpu.roll(center_ref[at_tile, :], shift, 1))
                qn, qs = q_ref[jj + 1, at_tile, :], q_ref[jj - 1, at_tile, :]
                lap_ref[jj - 1, at_tile, :] = first * ((qe + qw) + (qn + qs)) - second * q
                return q, qe, qw, qn, qs

            if not inside:
                for f in range(fields):
                    plane(f)
                continue
            near_ref[jj - 2, tile(k), :] = count
            quarter = jnp.where(here, 0.25, 0.0)
            planes_of = {2: plane(2), 3: plane(3)}
            u, ue, uw, _, _ = planes_of[2]
            v, _, _, vn, vs = planes_of[3]
            fe = jnp.where(oe, quarter * (u + ue), 0.0)
            fw = jnp.where(ow, quarter * (u + uw), 0.0)
            fn = jnp.where(on, quarter * (v + vn), 0.0)
            fs = jnp.where(os, quarter * (v + vs), 0.0)
            net = (fw - fe) + (fs - fn)
            for f in (2, 3, 0, 1):
                q, qe, qw, qn, qs = planes_of[f] if f in planes_of else plane(f)
                tend_ref[jj - 2, tile(f * depth_tiles + k), :] = (
                    net * q + (fw * qw - fe * qe) + (fs * qs - fn * qn)
                )

    def finish(j):
        shift = 122 - 4 * j
        level = q_ref[j + 2, own, :]
        for k in range(depth_tiles):
            here = kio[k] < level
            count = near_ref[j, tile(k), :]
            for f in range(fields):
                at_tile = tile(f * depth_tiles + k)
                lap = lap_ref[j + 1, at_tile, :]
                le, lw = beside(lap, pltpu.roll(slap_ref[at_tile, :], shift, 1))
                total = (le + lw) + (lap_ref[j + 2, at_tile, :] + lap_ref[j, at_tile, :])
                tend_ref[j, at_tile, :] += jnp.where(here, total, 0.0) - count * lap

    def sweep(fn, start, stop, unroll):
        assert (stop - start) % unroll == 0

        def body(i, carry):
            for r in range(unroll):
                fn(start + unroll * i + r)
            return carry

        lax.fori_loop(0, (stop - start) // unroll, body, 0)

    sweep(lambda jj: laplace(jj, True), 3, rows + 1, 2)

    drained(lon_in, lon_sem, (1,))
    total = part_ref[...]
    for i in range(n_lon - 1):
        total = total + lon_in[i]
    mid_ref[...] = total
    for off in range(1, n_lat):
        remote(mid_ref, lat_in.at[off - 1], lat_sem, (), at(0, off)).start()

    sweep(finish, 2, rows - 2, 2)

    for v, dlat, _ in sides:
        rim = q_ref.at[pl.ds(rows + 2, 2)] if v == 0 else q_ref.at[pl.ds(0, 2)]
        received(rim, row_sem, v, dlat)
    for jj, inside in ((1, False), (2, True), (rows + 1, True), (rows + 2, False)):
        laplace(jj, inside)
    for j in (0, 1, rows - 2, rows - 1):
        finish(j)

    drained(lat_in, lat_sem, (1,))
    total = mid_ref[...]
    for i in range(n_lat - 1):
        total = total + lat_in[i]
    total_ref[...] = total

    drained(side_ref, side_sem, (0,))
    drained(strip_in, strip_sem, (0,))
    drained(lon_in, lon_sem, (0,))
    drained(lat_in, lat_sem, (0,))
    for v, dlat, _ in sides:
        @pl.when(has[dlat])
        def _(v=v):
            drained(vert_ref.at[v], vert_sem, (0, v))
            drained(corner_in.at[v], corner_sem, (0, v))
            drained(q_ref.at[pl.ds(0, 2)], row_sem, (0, v))


def deliver(tend_in, basis_in, diag_in, total_in, height_ref, resid_ref, tend_ref, height_buf, resid_buf, sem):
    rows = tend_in.shape[0]
    stores = [pltpu.make_async_copy(tend_in.at[j], tend_ref.at[:, j, :], sem.at[0]) for j in range(rows)]
    for store in stores:
        store.start()
    total = jnp.broadcast_to(jnp.sum(total_in[...], axis=1, keepdims=True), (2 * ITERS, 128))
    mu = [total[m : m + 1] for m in range(2 * ITERS)]

    def inner(x, y):
        sums = [None] * (len(x) + len(y) - 1)
        for i, xi in enumerate(x):
            for j, yj in enumerate(y):
                sums[i + j] = xi * yj if sums[i + j] is None else sums[i + j] + xi * yj
        out = sums[0] * mu[0]
        for m in range(1, len(sums)):
            out = out + sums[m] * mu[m]
        return out

    one = jnp.ones((1, 128), jnp.float32)
    zero = jnp.zeros((1, 128), jnp.float32)
    z, p, h = [one], [one], []
    rz = mu[0]
    for it in range(ITERS):
        image = [hi - lo for hi, lo in zip(p + [zero], [zero] + p)]
        alpha = rz / inner(p, image)
        h = [x + alpha * y for x, y in zip(h + [zero], p)]
        z = [x - alpha * y for x, y in zip(z + [zero], image)]
        if it + 1 < ITERS:
            new = inner(z, z)
            beta = new / rz
            p = [x + beta * y for x, y in zip(z, p + [zero])]
            rz = new
    height = h[0] * basis_in[0]
    for i in range(1, ITERS):
        height = height + h[i] * basis_in[i]
    resid = z[0] * basis_in[0]
    for i in range(1, ITERS + 1):
        resid = resid + z[i] * basis_in[i]
    height_buf[...] = height
    resid_buf[...] = diag_in[...] * resid
    last = [
        pltpu.make_async_copy(height_buf, height_ref, sem.at[1]),
        pltpu.make_async_copy(resid_buf, resid_ref, sem.at[2]),
    ]
    for store in last:
        store.start()
    pltpu.make_async_copy(tend_in, tend_in, sem.at[0]).wait()
    for store in last:
        store.wait()


def per_device(n_lon, n_lat, forcing, sea, count, state):
    fields, levels, rows, width = state.shape
    planes = fields * levels
    tall = planes + SUB
    assert levels % SUB == 0 and width == 128 and rows % SUB == 0 and rows >= 2 * SUB
    assert 4 * (rows + 2) <= width and 4 * (planes // SUB + 1) <= width
    sizes = (n_lon, n_lat, fields, levels, rows)
    f32 = jnp.float32
    vmem = pl.BlockSpec(memory_space=pltpu.VMEM)
    hbm = pl.BlockSpec(memory_space=pltpu.HBM)
    dma = pltpu.SemaphoreType.DMA
    held = pl.pallas_call(
        functools.partial(exchange, sizes),
        out_shape=(
            pltpu.VMEM((rows, planes, width), f32),
            pltpu.VMEM((ITERS + 1, rows, width), f32),
            pltpu.VMEM((rows, width), f32),
            pltpu.VMEM((2 * ITERS, width), f32),
        ),
        in_specs=[hbm] * 4,
        out_specs=(vmem,) * 4,
        scratch_shapes=[
            pltpu.VMEM((rows, width), f32),
            pltpu.VMEM((rows, width), jnp.int32),
            pltpu.VMEM((rows, width), jnp.int32),
            pltpu.VMEM((rows + 4, tall, width), f32),
            pltpu.VMEM((rows + 2, planes, width), f32),
            pltpu.VMEM((rows, levels, width), f32),
            pltpu.VMEM((rows, width), f32),
            pltpu.VMEM((2, rows, width), f32),
            pltpu.VMEM((2, rows, width), f32),
            pltpu.VMEM((2, 4, SUB, width), f32),
            pltpu.VMEM((tall, width), f32),
            pltpu.VMEM((2, tall, width), f32),
            pltpu.VMEM((2, SUB, width), f32),
            pltpu.VMEM((2, 2, SUB, width), f32),
            pltpu.VMEM((tall, width), f32),
            pltpu.VMEM((planes, width), f32),
            pltpu.VMEM((2 * ITERS, width), f32),
            pltpu.VMEM((n_lon - 1, 2 * ITERS, width), f32),
            pltpu.VMEM((2 * ITERS, width), f32),
            pltpu.VMEM((n_lat - 1, 2 * ITERS, width), f32),
            dma((4,)),
            dma((2,)),
            dma((2, 2)),
            dma((2,)),
            dma((2, 2)),
            dma((2, 2)),
            dma((2,)),
            dma((2,)),
        ],
        compiler_params=pltpu.CompilerParams(collective_id=0, has_side_effects=True),
    )(forcing, sea, count, state.reshape(planes, rows, width))
    small = jax.ShapeDtypeStruct((rows, width), f32)
    height, resid, tend = pl.pallas_call(
        deliver,
        out_shape=(small, small, jax.ShapeDtypeStruct((planes, rows, width), f32)),
        in_specs=[vmem] * 4,
        out_specs=(hbm,) * 3,
        scratch_shapes=[
            pltpu.VMEM((rows, width), f32),
            pltpu.VMEM((rows, width), f32),
            dma((3,)),
        ],
        compiler_params=pltpu.CompilerParams(vmem_limit_bytes=16 << 20),
    )(*held)
    return height, resid, tend.reshape(state.shape)


def solution(mesh):
    return jax.shard_map(
        functools.partial(per_device, mesh.shape["lon"], mesh.shape["lat"]),
        mesh=mesh,
        in_specs=(P("lat", "lon"), P("lat", "lon"), P("lat", "lon"), P(None, None, "lat", "lon")),
        out_specs=(P("lat", "lon"), P("lat", "lon"), P(None, None, "lat", "lon")),
        check_vma=False,
    )
```

```python
import functools

import jax
import jax.numpy as jnp
from jax import lax
from jax.experimental import pallas as pl
from jax.experimental.pallas import tpu as pltpu
from jax.sharding import PartitionSpec as P

ITERS = 4
DAMPING = 0.05
VISCOSITY = 0.02
SUB = 8
MESH = pl.DeviceIdType.MESH


def east(a, b, lane):
    ra, rb = pltpu.roll(a, 127, 1), pltpu.roll(b, 127, 1)
    keep = lane < 127
    return jnp.where(keep, ra, rb), jnp.where(keep, rb, ra)


def west(a, b, lane):
    ra, rb = pltpu.roll(a, 1, 1), pltpu.roll(b, 1, 1)
    keep = lane > 0
    return jnp.where(keep, ra, rb), jnp.where(keep, rb, ra)


def north(x):
    return pltpu.roll(x, x.shape[0] - 1, 0)


def south(x):
    return pltpu.roll(x, 1, 0)


def exchange(
    sizes,
    forcing_ref, sea_ref, count_ref, state_ref,
    tend_ref, basis_ref, diag_ref, total_ref,
    force_buf, sea_buf, count_buf, q_ref, lap_ref, near_ref,
    pack_ref, side_ref, pair_ref, vert_ref,
    strip_out, strip_in, corner_out, corner_in, center_ref, slap_ref,
    part_ref, all_in,
    load_sem, side_sem, vert_sem, strip_sem, row_sem, corner_sem, all_sem, ready_sem,
):
    n_lon, n_lat, fields, levels, rows = sizes
    planes = fields * levels
    depth_tiles = levels // SUB
    tiles = planes // SUB
    ilon, ilat = lax.axis_index("lon"), lax.axis_index("lat")
    has = {1: ilat < n_lat - 1, -1: ilat > 0}

    def at(dlon, dlat):
        return {
            "lon": lax.rem(ilon + dlon + n_lon, n_lon),
            "lat": lax.rem(ilat + dlat + n_lat, n_lat),
        }

    barrier = pltpu.get_barrier_semaphore()
    for off in range(1, n_lon):
        pl.semaphore_signal(barrier, inc=1, device_id=at(off, 0), device_id_type=MESH)
    for off in range(1, n_lat):
        pl.semaphore_signal(barrier, inc=1, device_id=at(0, off), device_id_type=MESH)
    for dlat in (-1, 1):
        @pl.when(has[dlat])
        def _(dlat=dlat):
            for dlon in (-1, 1):
                pl.semaphore_signal(barrier, inc=1, device_id=at(dlon, dlat), device_id_type=MESH)

    inputs = [
        pltpu.make_async_copy(src, dst, load_sem.at[i])
        for i, (src, dst) in enumerate(((forcing_ref, force_buf), (sea_ref, sea_buf), (count_ref, count_buf)))
    ]
    for load in inputs:
        load.start()
    for j in range(rows):
        pltpu.make_async_copy(state_ref.at[:, j, :], q_ref.at[j + 2, pl.ds(0, planes)], load_sem.at[3]).start()

    def remote(src, dst, sems, index, where):
        return pltpu.make_async_remote_copy(
            src_ref=src, dst_ref=dst, send_sem=sems.at[(0,) + index], recv_sem=sems.at[(1,) + index],
            device_id=where, device_id_type=MESH,
        )

    def drained(ref, sems, index):
        pltpu.make_async_copy(ref, ref, sems.at[index]).wait()

    lane8 = lax.broadcasted_iota(jnp.int32, (SUB, 128), 1)
    sub8 = lax.broadcasted_iota(jnp.int32, (SUB, 128), 0)
    kio = [(sub8 + SUB * t).astype(jnp.float32) for t in range(depth_tiles)]
    slot8 = lane8 % 4
    last_lane, first_lane = lane8 == 127, lane8 == 0
    own = pl.ds(planes, SUB)

    def tile(t):
        return pl.ds(SUB * t, SUB)

    sides = ((0, -1, 0), (1, 1, rows - SUB))
    for v, dlat, _ in sides:
        @pl.when(jnp.logical_not(has[-dlat]))
        def _(v=v):
            vert_ref[v] = jnp.zeros_like(vert_ref[v])
            corner_in[v] = jnp.zeros_like(corner_in[v])
            for r in range(2):
                jj = rows + 2 + r if v == 0 else r
                q_ref[jj] = jnp.zeros_like(q_ref[jj])

    for load in inputs:
        load.wait()
    lane_r = lax.broadcasted_iota(jnp.int32, (rows, 128), 1)
    sea = sea_buf[...].astype(jnp.float32)
    wet = sea * count_buf[...].astype(jnp.float32)
    force = sea * force_buf[...]
    pair_ref[0] = force
    pair_ref[1] = wet
    inner_half = jnp.where(lane_r < 64, pltpu.roll(wet, 32, 1), pltpu.roll(wet, 96, 1))
    pack_ref[...] = jnp.where((lane_r >= 32) & (lane_r < 96), inner_half, force)
    for j in range(rows):
        q_ref[j + 2, own, :] = jnp.broadcast_to(wet[j : j + 1], (SUB, 128))

    diagonals = 2 * (has[1].astype(jnp.int32) + has[-1].astype(jnp.int32))
    pl.semaphore_wait(barrier, n_lon + n_lat - 2 + diagonals)

    for h, dlon in ((0, 1), (1, -1)):
        remote(pack_ref, side_ref.at[h], side_sem, (), at(dlon, 0)).start()
    for v, dlat, start in sides:
        @pl.when(has[dlat])
        def _(v=v, dlat=dlat, start=start):
            part = pl.ds(start, SUB)
            for h, dlon in ((0, 1), (1, -1)):
                remote(pack_ref.at[part], vert_ref.at[v, 2 + h], vert_sem, (v,), at(dlon, dlat)).start()
            remote(pair_ref.at[:, part], vert_ref.at[v, pl.ds(0, 2)], vert_sem, (v,), at(0, dlat)).start()

    for off in range(1, n_lat):
        pl.semaphore_signal(ready_sem, inc=1, device_id=at(0, off), device_id_type=MESH)

    pltpu.make_async_copy(
        q_ref.at[pl.ds(2, rows), pl.ds(0, planes)], q_ref.at[pl.ds(2, rows), pl.ds(0, planes)], load_sem.at[3]
    ).wait()

    packed = [jnp.zeros((SUB, 128), jnp.float32)] * (tiles + 1)
    for j in range(rows):
        here = lane8 // 4 == j + 1
        level = q_ref[j + 2, own, :]
        active = [k < level for k in kio]
        for t in range(tiles + 1):
            if t < tiles:
                q = jnp.where(active[t % depth_tiles], q_ref[j + 2, tile(t), :], 0.0)
                q_ref[j + 2, tile(t), :] = q
            else:
                q = level
            packed[t] = jnp.where(here, pltpu.roll(q, 4 * (j + 1) + 2, 1), packed[t])
    corners = [jnp.zeros((SUB, 128), jnp.float32)] * 2
    for t in range(tiles + 1):
        strip_out[tile(t), :] = packed[t]
        for v, j in ((0, 0), (1, rows - 1)):
            moved = pltpu.roll(packed[t], (4 * t - 4 * (j + 1)) % 128, 1)
            corners[v] = jnp.where(lane8 // 4 == t, moved, corners[v])
    for v in range(2):
        corner_out[v] = corners[v]

    for h, dlon in ((0, 1), (1, -1)):
        remote(strip_out, strip_in.at[h], strip_sem, (), at(dlon, 0)).start()
    for v, dlat, _ in sides:
        @pl.when(has[dlat])
        def _(v=v, dlat=dlat):
            mine = pl.ds(2, 2) if v == 0 else pl.ds(rows, 2)
            there = pl.ds(rows + 2, 2) if v == 0 else pl.ds(0, 2)
            for h, dlon in ((0, 1), (1, -1)):
                remote(corner_out.at[v], corner_in.at[v, h], corner_sem, (v,), at(dlon, dlat)).start()
            remote(q_ref.at[mine], q_ref.at[there], row_sem, (v,), at(0, dlat)).start()

    def received(ref, sems, v, dlat):
        @pl.when(has[-dlat])
        def _():
            drained(ref, sems, (1, v))

    drained(side_ref, side_sem, (1,))
    for v, dlat, _ in sides:
        received(vert_ref.at[v], vert_sem, v, dlat)

    from_west = jnp.concatenate([side_ref[0], vert_ref[0, 2], vert_ref[1, 2]], axis=0)
    from_east = jnp.concatenate([side_ref[1], vert_ref[0, 3], vert_ref[1, 3]], axis=0)
    lane_t = lax.broadcasted_iota(jnp.int32, (rows + 2 * SUB, 128), 1)
    low = lane_t < 64
    force_a = jnp.concatenate([pair_ref[0], vert_ref[0, 0], vert_ref[1, 0]], axis=0)
    wet_a = jnp.concatenate([pair_ref[1], vert_ref[0, 1], vert_ref[1, 1]], axis=0)
    force_b = jnp.where(low, from_east, from_west)
    wet_b = jnp.where(low, pltpu.roll(from_east, 96, 1), pltpu.roll(from_west, 32, 1))
    depth_a, depth_b = wet_a / levels, wet_b / levels
    da, db = east(depth_a, depth_b, lane_t)
    ea, eb = jnp.minimum(depth_a, da), jnp.minimum(depth_b, db)
    da, db = west(depth_a, depth_b, lane_t)
    wa, wb = jnp.minimum(depth_a, da), jnp.minimum(depth_b, db)
    na, nb = jnp.minimum(depth_a, north(depth_a)), jnp.minimum(depth_b, north(depth_b))
    sa, sb = south(na), south(nb)
    diag_a = DAMPING + ea + wa + na + sa
    diag_b = DAMPING + eb + wb + nb + sb
    inv_a, inv_b = 1.0 / diag_a, 1.0 / diag_b
    va, vb = force_a * inv_a, force_b * inv_b
    ea, wa, na, sa = (c * inv_a for c in (ea, wa, na, sa))
    eb, wb, nb, sb = (c * inv_b for c in (eb, wb, nb, sb))
    diag = diag_a[:rows]
    diag_ref[...] = diag
    basis = [va[:rows]]
    for _ in range(ITERS):
        qe, qeb = east(va, vb, lane_t)
        qw, qwb = west(va, vb, lane_t)
        va, vb = (
            ea * qe + wa * qw + na * north(va) + sa * south(va),
            eb * qeb + wb * qwb + nb * north(vb) + sb * south(vb),
        )
        basis.append(va[:rows])
    for i, x in enumerate(basis):
        basis_ref[i] = x
    moments = []
    for m in range(2 * ITERS):
        moments.append(jnp.sum(diag * basis[m // 2] * basis[(m + 1) // 2], axis=0, keepdims=True))
    sums = jnp.broadcast_to(jnp.sum(jnp.concatenate(moments, axis=0), axis=1, keepdims=True), (2 * ITERS, 128))
    sums = jnp.where(lane8 // (128 // (2 * ITERS)) == sub8, sums, 0.0)
    part_ref[...] = jnp.sum(sums, axis=0, keepdims=True)
    pl.semaphore_wait(ready_sem, n_lat - 1)
    for off in sorted(range(1, n_lon * n_lat), key=lambda off: -min(off % n_lat, n_lat - off % n_lat)):
        remote(part_ref, all_in.at[off - 1], all_sem, (), at(off // n_lat, off % n_lat)).start()

    drained(strip_in, strip_sem, (1,))
    for v, dlat, _ in sides:
        received(corner_in.at[v], corner_sem, v, dlat)

    def swap(x, step):
        return jnp.where(slot8 < 2, pltpu.roll(x, 128 - step, 1), pltpu.roll(x, step, 1))

    def arrange(t):
        g = jnp.where(slot8 < 2, strip_in[0, tile(t), :], strip_in[1, tile(t), :])
        for v, j in ((0, rows), (1, -1)):
            corner = jnp.where(slot8 < 2, corner_in[v, 0], corner_in[v, 1])
            moved = pltpu.roll(corner, (4 * (j + 1) - 4 * t) % 128, 1)
            g = jnp.where(lane8 // 4 == j + 1, moved, g)
        center = swap(g, 1)
        return center, strip_out[tile(t), :], swap(g, 2), pltpu.roll(center, 124, 1), pltpu.roll(center, 4, 1)

    ring = arrange(tiles)
    center_ref[tile(tiles), :] = ring[0]
    edge_coef = []
    for k in kio:
        count = sum(jnp.where(k < w, 1.0, 0.0) for w in ring[1:])
        first = jnp.where(k < ring[0], -VISCOSITY, 0.0)
        edge_coef.append((first, first * count))
    for t in range(tiles):
        center, a, b, c, d = arrange(t)
        center_ref[tile(t), :] = center
        first, second = edge_coef[t % depth_tiles]
        slap_ref[tile(t), :] = first * ((a + b) + (c + d)) - second * center

    def beside(x, edge):
        return (
            jnp.where(last_lane, edge, pltpu.roll(x, 127, 1)),
            jnp.where(first_lane, edge, pltpu.roll(x, 1, 1)),
        )

    def laplace(jj, inside):
        shift = 130 - 4 * jj
        level = q_ref[jj, own, :]
        around = beside(level, pltpu.roll(center_ref[own, :], shift, 1)) + (q_ref[jj + 1, own, :], q_ref[jj - 1, own, :])
        for k in range(depth_tiles):
            here, oe, ow, on, os = (kio[k] < x for x in (level,) + around)
            ones = [jnp.where(x, 1.0, 0.0) for x in (oe, ow, on, os)]
            count = (ones[0] + ones[1]) + (ones[2] + ones[3])
            first = jnp.where(here, -VISCOSITY, 0.0)
            second = first * count

            def plane(f):
                at_tile = tile(f * depth_tiles + k)
                q = q_ref[jj, at_tile, :]
                qe, qw = beside(q, pltpu.roll(center_ref[at_tile, :], shift, 1))
                qn, qs = q_ref[jj + 1, at_tile, :], q_ref[jj - 1, at_tile, :]
                lap_ref[jj - 1, at_tile, :] = first * ((qe + qw) + (qn + qs)) - second * q
                return q, qe, qw, qn, qs

            if not inside:
                for f in range(fields):
                    plane(f)
                continue
            near_ref[jj - 2, tile(k), :] = count
            quarter = jnp.where(here, 0.25, 0.0)
            planes_of = {2: plane(2), 3: plane(3)}
            u, ue, uw, _, _ = planes_of[2]
            v, _, _, vn, vs = planes_of[3]
            fe = jnp.where(oe, quarter * (u + ue), 0.0)
            fw = jnp.where(ow, quarter * (u + uw), 0.0)
            fn = jnp.where(on, quarter * (v + vn), 0.0)
            fs = jnp.where(os, quarter * (v + vs), 0.0)
            net = (fw - fe) + (fs - fn)
            for f in (2, 3, 0, 1):
                q, qe, qw, qn, qs = planes_of[f] if f in planes_of else plane(f)
                tend_ref[jj - 2, tile(f * depth_tiles + k), :] = (
                    net * q + (fw * qw - fe * qe) + (fs * qs - fn * qn)
                )

    def finish(j):
        shift = 122 - 4 * j
        level = q_ref[j + 2, own, :]
        for k in range(depth_tiles):
            here = kio[k] < level
            count = near_ref[j, tile(k), :]
            for f in range(fields):
                at_tile = tile(f * depth_tiles + k)
                lap = lap_ref[j + 1, at_tile, :]
                le, lw = beside(lap, pltpu.roll(slap_ref[at_tile, :], shift, 1))
                total = (le + lw) + (lap_ref[j + 2, at_tile, :] + lap_ref[j, at_tile, :])
                tend_ref[j, at_tile, :] += jnp.where(here, total, 0.0) - count * lap

    def sweep(fn, start, stop, unroll):
        assert (stop - start) % unroll == 0

        def body(i, carry):
            for r in range(unroll):
                fn(start + unroll * i + r)
            return carry

        lax.fori_loop(0, (stop - start) // unroll, body, 0)

    sweep(lambda jj: laplace(jj, True), 3, rows + 1, 2)

    sweep(finish, 2, rows - 2, 2)

    for v, dlat, _ in sides:
        rim = q_ref.at[pl.ds(rows + 2, 2)] if v == 0 else q_ref.at[pl.ds(0, 2)]
        received(rim, row_sem, v, dlat)
    for jj, inside in ((1, False), (2, True), (rows + 1, True), (rows + 2, False)):
        laplace(jj, inside)
    for j in (0, 1, rows - 2, rows - 1):
        finish(j)

    drained(all_in, all_sem, (1,))
    total = part_ref[...]
    for i in range(n_lon * n_lat - 1):
        total = total + all_in[i]
    total_ref[...] = jnp.broadcast_to(total, total_ref.shape)

    drained(side_ref, side_sem, (0,))
    drained(strip_in, strip_sem, (0,))
    drained(all_in, all_sem, (0,))
    for v, dlat, _ in sides:
        @pl.when(has[dlat])
        def _(v=v):
            drained(vert_ref.at[v], vert_sem, (0, v))
            drained(corner_in.at[v], corner_sem, (0, v))
            drained(q_ref.at[pl.ds(0, 2)], row_sem, (0, v))


def deliver(tend_in, basis_in, diag_in, total_in, height_ref, resid_ref, tend_ref, height_buf, resid_buf, sem):
    rows = tend_in.shape[0]
    stores = [pltpu.make_async_copy(tend_in.at[j], tend_ref.at[:, j, :], sem.at[0]) for j in range(rows)]
    for store in stores:
        store.start()
    part = 128 // (2 * ITERS)
    shape = (2 * ITERS, 128)
    mine = lax.broadcasted_iota(jnp.int32, shape, 1) == part * lax.broadcasted_iota(jnp.int32, shape, 0)
    total = jnp.broadcast_to(jnp.sum(jnp.where(mine, total_in[...], 0.0), axis=1, keepdims=True), shape)
    mu = [total[m : m + 1] for m in range(2 * ITERS)]

    def inner(x, y):
        sums = [None] * (len(x) + len(y) - 1)
        for i, xi in enumerate(x):
            for j, yj in enumerate(y):
                sums[i + j] = xi * yj if sums[i + j] is None else sums[i + j] + xi * yj
        out = sums[0] * mu[0]
        for m in range(1, len(sums)):
            out = out + sums[m] * mu[m]
        return out

    one = jnp.ones((1, 128), jnp.float32)
    zero = jnp.zeros((1, 128), jnp.float32)
    z, p, h = [one], [one], []
    rz = mu[0]
    for it in range(ITERS):
        image = [hi - lo for hi, lo in zip(p + [zero], [zero] + p)]
        alpha = rz / inner(p, image)
        h = [x + alpha * y for x, y in zip(h + [zero], p)]
        z = [x - alpha * y for x, y in zip(z + [zero], image)]
        if it + 1 < ITERS:
            new = inner(z, z)
            beta = new / rz
            p = [x + beta * y for x, y in zip(z, p + [zero])]
            rz = new
    height = h[0] * basis_in[0]
    for i in range(1, ITERS):
        height = height + h[i] * basis_in[i]
    resid = z[0] * basis_in[0]
    for i in range(1, ITERS + 1):
        resid = resid + z[i] * basis_in[i]
    height_buf[...] = height
    resid_buf[...] = diag_in[...] * resid
    last = [
        pltpu.make_async_copy(height_buf, height_ref, sem.at[1]),
        pltpu.make_async_copy(resid_buf, resid_ref, sem.at[2]),
    ]
    for store in last:
        store.start()
    pltpu.make_async_copy(tend_in, tend_in, sem.at[0]).wait()
    for store in last:
        store.wait()


def per_device(n_lon, n_lat, forcing, sea, count, state):
    fields, levels, rows, width = state.shape
    planes = fields * levels
    tall = planes + SUB
    assert levels % SUB == 0 and width == 128 and rows % SUB == 0 and rows >= 2 * SUB
    assert 4 * (rows + 2) <= width and 4 * (planes // SUB + 1) <= width
    sizes = (n_lon, n_lat, fields, levels, rows)
    f32 = jnp.float32
    vmem = pl.BlockSpec(memory_space=pltpu.VMEM)
    hbm = pl.BlockSpec(memory_space=pltpu.HBM)
    dma = pltpu.SemaphoreType.DMA
    held = pl.pallas_call(
        functools.partial(exchange, sizes),
        out_shape=(
            pltpu.VMEM((rows, planes, width), f32),
            pltpu.VMEM((ITERS + 1, rows, width), f32),
            pltpu.VMEM((rows, width), f32),
            pltpu.VMEM((2 * ITERS, width), f32),
        ),
        in_specs=[hbm] * 4,
        out_specs=(vmem,) * 4,
        scratch_shapes=[
            pltpu.VMEM((rows, width), f32),
            pltpu.VMEM((rows, width), jnp.int32),
            pltpu.VMEM((rows, width), jnp.int32),
            pltpu.VMEM((rows + 4, tall, width), f32),
            pltpu.VMEM((rows + 2, planes, width), f32),
            pltpu.VMEM((rows, levels, width), f32),
            pltpu.VMEM((rows, width), f32),
            pltpu.VMEM((2, rows, width), f32),
            pltpu.VMEM((2, rows, width), f32),
            pltpu.VMEM((2, 4, SUB, width), f32),
            pltpu.VMEM((tall, width), f32),
            pltpu.VMEM((2, tall, width), f32),
            pltpu.VMEM((2, SUB, width), f32),
            pltpu.VMEM((2, 2, SUB, width), f32),
            pltpu.VMEM((tall, width), f32),
            pltpu.VMEM((planes, width), f32),
            pltpu.VMEM((1, width), f32),
            pltpu.VMEM((n_lon * n_lat - 1, 1, width), f32),
            dma((4,)),
            dma((2,)),
            dma((2, 2)),
            dma((2,)),
            dma((2, 2)),
            dma((2, 2)),
            dma((2,)),
            pltpu.SemaphoreType.REGULAR,
        ],
        compiler_params=pltpu.CompilerParams(collective_id=0, has_side_effects=True),
    )(forcing, sea, count, state.reshape(planes, rows, width))
    small = jax.ShapeDtypeStruct((rows, width), f32)
    height, resid, tend = pl.pallas_call(
        deliver,
        out_shape=(small, small, jax.ShapeDtypeStruct((planes, rows, width), f32)),
        in_specs=[vmem] * 4,
        out_specs=(hbm,) * 3,
        scratch_shapes=[
            pltpu.VMEM((rows, width), f32),
            pltpu.VMEM((rows, width), f32),
            dma((3,)),
        ],
        compiler_params=pltpu.CompilerParams(vmem_limit_bytes=16 << 20),
    )(*held)
    return height, resid, tend.reshape(state.shape)


def solution(mesh):
    return jax.shard_map(
        functools.partial(per_device, mesh.shape["lon"], mesh.shape["lat"]),
        mesh=mesh,
        in_specs=(P("lat", "lon"), P("lat", "lon"), P("lat", "lon"), P(None, None, "lat", "lon")),
        out_specs=(P("lat", "lon"), P("lat", "lon"), P(None, None, "lat", "lon")),
        check_vma=False,
    )
```

```python
import functools

import jax
import jax.numpy as jnp
from jax import lax
from jax.experimental import pallas as pl
from jax.experimental.pallas import tpu as pltpu
from jax.sharding import PartitionSpec as P

ITERS = 4
DAMPING = 0.05
VISCOSITY = 0.02
SUB = 8
MESH = pl.DeviceIdType.MESH


def east(a, b, lane):
    ra, rb = pltpu.roll(a, 127, 1), pltpu.roll(b, 127, 1)
    keep = lane < 127
    return jnp.where(keep, ra, rb), jnp.where(keep, rb, ra)


def west(a, b, lane):
    ra, rb = pltpu.roll(a, 1, 1), pltpu.roll(b, 1, 1)
    keep = lane > 0
    return jnp.where(keep, ra, rb), jnp.where(keep, rb, ra)


def north(x):
    return pltpu.roll(x, x.shape[0] - 1, 0)


def south(x):
    return pltpu.roll(x, 1, 0)


def exchange(
    sizes,
    forcing_ref, sea_ref, count_ref, state_ref,
    tend_ref, basis_ref, diag_ref, total_ref,
    force_buf, sea_buf, count_buf, q_ref, lap_ref, near_ref,
    pack_ref, side_ref, pair_ref, vert_ref,
    strip_own, strip_out, strip_in, corner_out, corner_in, center_ref, slap_ref,
    part_ref, all_in,
    load_sem, side_sem, vert_sem, strip_sem, row_sem, corner_sem, all_sem, ready_sem,
):
    n_lon, n_lat, fields, levels, rows = sizes
    planes = fields * levels
    depth_tiles = levels // SUB
    tiles = planes // SUB
    ilon, ilat = lax.axis_index("lon"), lax.axis_index("lat")
    has = {1: ilat < n_lat - 1, -1: ilat > 0}

    def at(dlon, dlat):
        return {
            "lon": lax.rem(ilon + dlon + n_lon, n_lon),
            "lat": lax.rem(ilat + dlat + n_lat, n_lat),
        }

    barrier = pltpu.get_barrier_semaphore()
    for off in range(1, n_lon):
        pl.semaphore_signal(barrier, inc=1, device_id=at(off, 0), device_id_type=MESH)
    for off in range(1, n_lat):
        pl.semaphore_signal(barrier, inc=1, device_id=at(0, off), device_id_type=MESH)
    for dlat in (-1, 1):
        @pl.when(has[dlat])
        def _(dlat=dlat):
            for dlon in (-1, 1):
                pl.semaphore_signal(barrier, inc=1, device_id=at(dlon, dlat), device_id_type=MESH)

    inputs = [
        pltpu.make_async_copy(src, dst, load_sem.at[i])
        for i, (src, dst) in enumerate(((forcing_ref, force_buf), (sea_ref, sea_buf), (count_ref, count_buf)))
    ]
    for load in inputs:
        load.start()
    for j in range(rows):
        pltpu.make_async_copy(state_ref.at[:, j, :], q_ref.at[j + 2, pl.ds(0, planes)], load_sem.at[3]).start()

    def remote(src, dst, sems, index, where):
        return pltpu.make_async_remote_copy(
            src_ref=src, dst_ref=dst, send_sem=sems.at[(0,) + index], recv_sem=sems.at[(1,) + index],
            device_id=where, device_id_type=MESH,
        )

    def drained(ref, sems, index):
        pltpu.make_async_copy(ref, ref, sems.at[index]).wait()

    lane8 = lax.broadcasted_iota(jnp.int32, (SUB, 128), 1)
    sub8 = lax.broadcasted_iota(jnp.int32, (SUB, 128), 0)
    kio = [(sub8 + SUB * t).astype(jnp.float32) for t in range(depth_tiles)]
    slot8 = lane8 % 4
    last_lane, first_lane = lane8 == 127, lane8 == 0
    own = pl.ds(planes, SUB)

    def tile(t):
        return pl.ds(SUB * t, SUB)

    sides = ((0, -1, 0), (1, 1, rows - SUB))
    for v, dlat, _ in sides:
        @pl.when(jnp.logical_not(has[-dlat]))
        def _(v=v):
            vert_ref[v] = jnp.zeros_like(vert_ref[v])
            corner_in[v] = jnp.zeros_like(corner_in[v])
            for r in range(2):
                jj = rows + 2 + r if v == 0 else r
                q_ref[jj] = jnp.zeros_like(q_ref[jj])

    for load in inputs:
        load.wait()
    lane_r = lax.broadcasted_iota(jnp.int32, (rows, 128), 1)
    sea = sea_buf[...].astype(jnp.float32)
    wet = sea * count_buf[...].astype(jnp.float32)
    force = sea * force_buf[...]
    pair_ref[0] = force
    pair_ref[1] = wet
    inner_half = jnp.where(lane_r < 64, pltpu.roll(wet, 32, 1), pltpu.roll(wet, 96, 1))
    pack_ref[...] = jnp.where((lane_r >= 32) & (lane_r < 96), inner_half, force)
    for j in range(rows):
        q_ref[j + 2, own, :] = jnp.broadcast_to(wet[j : j + 1], (SUB, 128))

    diagonals = 2 * (has[1].astype(jnp.int32) + has[-1].astype(jnp.int32))
    pl.semaphore_wait(barrier, n_lon + n_lat - 2 + diagonals)

    for h, dlon in ((0, 1), (1, -1)):
        remote(pack_ref, side_ref.at[h], side_sem, (), at(dlon, 0)).start()
    for v, dlat, start in sides:
        @pl.when(has[dlat])
        def _(v=v, dlat=dlat, start=start):
            part = pl.ds(start, SUB)
            for h, dlon in ((0, 1), (1, -1)):
                remote(pack_ref.at[part], vert_ref.at[v, 2 + h], vert_sem, (v,), at(dlon, dlat)).start()
            remote(pair_ref.at[:, part], vert_ref.at[v, pl.ds(0, 2)], vert_sem, (v,), at(0, dlat)).start()

    for off in range(1, n_lat):
        pl.semaphore_signal(ready_sem, inc=1, device_id=at(0, off), device_id_type=MESH)

    pltpu.make_async_copy(
        q_ref.at[pl.ds(2, rows), pl.ds(0, planes)], q_ref.at[pl.ds(2, rows), pl.ds(0, planes)], load_sem.at[3]
    ).wait()

    packed = [jnp.zeros((SUB, 128), jnp.float32)] * (tiles + 1)
    for j in range(rows):
        here = lane8 // 4 == j + 1
        level = q_ref[j + 2, own, :]
        active = [k < level for k in kio]
        for t in range(tiles + 1):
            if t < tiles:
                q = jnp.where(active[t % depth_tiles], q_ref[j + 2, tile(t), :], 0.0)
                q_ref[j + 2, tile(t), :] = q
            else:
                q = level
            packed[t] = jnp.where(here, pltpu.roll(q, 4 * (j + 1) + 2, 1), packed[t])
    corners = [jnp.zeros((SUB, 128), jnp.float32)] * 2
    for t in range(tiles + 1):
        strip_own[tile(t), :] = packed[t]
        for v, j in ((0, 0), (1, rows - 1)):
            moved = pltpu.roll(packed[t], (4 * t - 4 * (j + 1)) % 128, 1)
            corners[v] = jnp.where(lane8 // 4 == t, moved, corners[v])
    for t in range(0, tiles + 1, 2):
        odd = packed[min(t + 1, tiles)]
        strip_out[0, tile(t // 2), :] = jnp.where(slot8 < 2, packed[t], pltpu.roll(odd, 2, 1))
        strip_out[1, tile(t // 2), :] = jnp.where(slot8 < 2, pltpu.roll(packed[t], 126, 1), odd)
    for v in range(2):
        corner_out[v] = corners[v]

    for h, dlon in ((0, 1), (1, -1)):
        remote(strip_out.at[h], strip_in.at[h], strip_sem, (), at(dlon, 0)).start()
    for v, dlat, _ in sides:
        @pl.when(has[dlat])
        def _(v=v, dlat=dlat):
            mine = pl.ds(2, 2) if v == 0 else pl.ds(rows, 2)
            there = pl.ds(rows + 2, 2) if v == 0 else pl.ds(0, 2)
            for h, dlon in ((0, 1), (1, -1)):
                remote(corner_out.at[v], corner_in.at[v, h], corner_sem, (v,), at(dlon, dlat)).start()
            remote(q_ref.at[mine], q_ref.at[there], row_sem, (v,), at(0, dlat)).start()

    def received(ref, sems, v, dlat):
        @pl.when(has[-dlat])
        def _():
            drained(ref, sems, (1, v))

    drained(side_ref, side_sem, (1,))
    for v, dlat, _ in sides:
        received(vert_ref.at[v], vert_sem, v, dlat)

    from_west = jnp.concatenate([side_ref[0], vert_ref[0, 2], vert_ref[1, 2]], axis=0)
    from_east = jnp.concatenate([side_ref[1], vert_ref[0, 3], vert_ref[1, 3]], axis=0)
    lane_t = lax.broadcasted_iota(jnp.int32, (rows + 2 * SUB, 128), 1)
    low = lane_t < 64
    force_a = jnp.concatenate([pair_ref[0], vert_ref[0, 0], vert_ref[1, 0]], axis=0)
    wet_a = jnp.concatenate([pair_ref[1], vert_ref[0, 1], vert_ref[1, 1]], axis=0)
    force_b = jnp.where(low, from_east, from_west)
    wet_b = jnp.where(low, pltpu.roll(from_east, 96, 1), pltpu.roll(from_west, 32, 1))
    depth_a, depth_b = wet_a / levels, wet_b / levels
    da, db = east(depth_a, depth_b, lane_t)
    ea, eb = jnp.minimum(depth_a, da), jnp.minimum(depth_b, db)
    da, db = west(depth_a, depth_b, lane_t)
    wa, wb = jnp.minimum(depth_a, da), jnp.minimum(depth_b, db)
    na, nb = jnp.minimum(depth_a, north(depth_a)), jnp.minimum(depth_b, north(depth_b))
    sa, sb = south(na), south(nb)
    diag_a = DAMPING + ea + wa + na + sa
    diag_b = DAMPING + eb + wb + nb + sb
    inv_a, inv_b = 1.0 / diag_a, 1.0 / diag_b
    va, vb = force_a * inv_a, force_b * inv_b
    ea, wa, na, sa = (c * inv_a for c in (ea, wa, na, sa))
    eb, wb, nb, sb = (c * inv_b for c in (eb, wb, nb, sb))
    diag = diag_a[:rows]
    diag_ref[...] = diag
    basis = [va[:rows]]
    for _ in range(ITERS):
        qe, qeb = east(va, vb, lane_t)
        qw, qwb = west(va, vb, lane_t)
        va, vb = (
            ea * qe + wa * qw + na * north(va) + sa * south(va),
            eb * qeb + wb * qwb + nb * north(vb) + sb * south(vb),
        )
        basis.append(va[:rows])
    for i, x in enumerate(basis):
        basis_ref[i] = x
    moments = []
    for m in range(2 * ITERS):
        moments.append(jnp.sum(diag * basis[m // 2] * basis[(m + 1) // 2], axis=0, keepdims=True))
    sums = jnp.broadcast_to(jnp.sum(jnp.concatenate(moments, axis=0), axis=1, keepdims=True), (2 * ITERS, 128))
    sums = jnp.where(lane8 // (128 // (2 * ITERS)) == sub8, sums, 0.0)
    part_ref[...] = jnp.sum(sums, axis=0, keepdims=True)
    pl.semaphore_wait(ready_sem, n_lat - 1)
    for off in sorted(range(1, n_lon * n_lat), key=lambda off: -min(off % n_lat, n_lat - off % n_lat)):
        remote(part_ref, all_in.at[off - 1], all_sem, (), at(off // n_lat, off % n_lat)).start()

    drained(strip_in, strip_sem, (1,))
    for v, dlat, _ in sides:
        received(corner_in.at[v], corner_sem, v, dlat)

    def swap(x, step):
        return jnp.where(slot8 < 2, pltpu.roll(x, 128 - step, 1), pltpu.roll(x, step, 1))

    def arrange(t):
        west_pair, east_pair = strip_in[0, tile(t // 2), :], strip_in[1, tile(t // 2), :]
        if t % 2:
            west_pair = pltpu.roll(west_pair, 126, 1)
        else:
            east_pair = pltpu.roll(east_pair, 2, 1)
        g = jnp.where(slot8 < 2, west_pair, east_pair)
        for v, j in ((0, rows), (1, -1)):
            corner = jnp.where(slot8 < 2, corner_in[v, 0], corner_in[v, 1])
            moved = pltpu.roll(corner, (4 * (j + 1) - 4 * t) % 128, 1)
            g = jnp.where(lane8 // 4 == j + 1, moved, g)
        center = swap(g, 1)
        return center, strip_own[tile(t), :], swap(g, 2), pltpu.roll(center, 124, 1), pltpu.roll(center, 4, 1)

    ring = arrange(tiles)
    center_ref[tile(tiles), :] = ring[0]
    edge_coef = []
    for k in kio:
        count = sum(jnp.where(k < w, 1.0, 0.0) for w in ring[1:])
        first = jnp.where(k < ring[0], -VISCOSITY, 0.0)
        edge_coef.append((first, first * count))
    for t in range(tiles):
        center, a, b, c, d = arrange(t)
        center_ref[tile(t), :] = center
        first, second = edge_coef[t % depth_tiles]
        slap_ref[tile(t), :] = first * ((a + b) + (c + d)) - second * center

    def beside(x, edge):
        return (
            jnp.where(last_lane, edge, pltpu.roll(x, 127, 1)),
            jnp.where(first_lane, edge, pltpu.roll(x, 1, 1)),
        )

    def laplace(jj, inside):
        shift = 130 - 4 * jj
        level = q_ref[jj, own, :]
        around = beside(level, pltpu.roll(center_ref[own, :], shift, 1)) + (q_ref[jj + 1, own, :], q_ref[jj - 1, own, :])
        for k in range(depth_tiles):
            here, oe, ow, on, os = (kio[k] < x for x in (level,) + around)
            ones = [jnp.where(x, 1.0, 0.0) for x in (oe, ow, on, os)]
            count = (ones[0] + ones[1]) + (ones[2] + ones[3])
            first = jnp.where(here, -VISCOSITY, 0.0)
            second = first * count

            def plane(f):
                at_tile = tile(f * depth_tiles + k)
                q = q_ref[jj, at_tile, :]
                qe, qw = beside(q, pltpu.roll(center_ref[at_tile, :], shift, 1))
                qn, qs = q_ref[jj + 1, at_tile, :], q_ref[jj - 1, at_tile, :]
                lap_ref[jj - 1, at_tile, :] = first * ((qe + qw) + (qn + qs)) - second * q
                return q, qe, qw, qn, qs

            if not inside:
                for f in range(fields):
                    plane(f)
                continue
            near_ref[jj - 2, tile(k), :] = count
            quarter = jnp.where(here, 0.25, 0.0)
            planes_of = {2: plane(2), 3: plane(3)}
            u, ue, uw, _, _ = planes_of[2]
            v, _, _, vn, vs = planes_of[3]
            fe = jnp.where(oe, quarter * (u + ue), 0.0)
            fw = jnp.where(ow, quarter * (u + uw), 0.0)
            fn = jnp.where(on, quarter * (v + vn), 0.0)
            fs = jnp.where(os, quarter * (v + vs), 0.0)
            net = (fw - fe) + (fs - fn)
            for f in (2, 3, 0, 1):
                q, qe, qw, qn, qs = planes_of[f] if f in planes_of else plane(f)
                tend_ref[jj - 2, tile(f * depth_tiles + k), :] = (
                    net * q + (fw * qw - fe * qe) + (fs * qs - fn * qn)
                )

    def finish(j):
        shift = 122 - 4 * j
        level = q_ref[j + 2, own, :]
        for k in range(depth_tiles):
            here = kio[k] < level
            count = near_ref[j, tile(k), :]
            for f in range(fields):
                at_tile = tile(f * depth_tiles + k)
                lap = lap_ref[j + 1, at_tile, :]
                le, lw = beside(lap, pltpu.roll(slap_ref[at_tile, :], shift, 1))
                total = (le + lw) + (lap_ref[j + 2, at_tile, :] + lap_ref[j, at_tile, :])
                tend_ref[j, at_tile, :] += jnp.where(here, total, 0.0) - count * lap

    for jj in range(3, 7):
        laplace(jj, True)

    def both(i, carry):
        for r in range(2):
            finish(2 * i - 2 + r)
        for r in range(2):
            laplace(2 * i + 3 + r, True)
        return carry

    lax.fori_loop(2, rows // 2 - 1, both, 0)
    for j in (rows - 4, rows - 3):
        finish(j)

    for v, dlat, _ in sides:
        rim = q_ref.at[pl.ds(rows + 2, 2)] if v == 0 else q_ref.at[pl.ds(0, 2)]
        received(rim, row_sem, v, dlat)
    for jj, inside in ((1, False), (2, True), (rows + 1, True), (rows + 2, False)):
        laplace(jj, inside)
    for j in (0, 1, rows - 2, rows - 1):
        finish(j)

    drained(all_in, all_sem, (1,))
    total = part_ref[...]
    for i in range(n_lon * n_lat - 1):
        total = total + all_in[i]
    total_ref[...] = jnp.broadcast_to(total, total_ref.shape)

    drained(side_ref, side_sem, (0,))
    drained(strip_in, strip_sem, (0,))
    drained(all_in, all_sem, (0,))
    for v, dlat, _ in sides:
        @pl.when(has[dlat])
        def _(v=v):
            drained(vert_ref.at[v], vert_sem, (0, v))
            drained(corner_in.at[v], corner_sem, (0, v))
            drained(q_ref.at[pl.ds(0, 2)], row_sem, (0, v))


def deliver(tend_in, basis_in, diag_in, total_in, height_ref, resid_ref, tend_ref, height_buf, resid_buf, sem):
    rows = tend_in.shape[0]
    stores = [pltpu.make_async_copy(tend_in.at[j], tend_ref.at[:, j, :], sem.at[0]) for j in range(rows)]
    for store in stores:
        store.start()
    part = 128 // (2 * ITERS)
    shape = (2 * ITERS, 128)
    mine = lax.broadcasted_iota(jnp.int32, shape, 1) == part * lax.broadcasted_iota(jnp.int32, shape, 0)
    total = jnp.broadcast_to(jnp.sum(jnp.where(mine, total_in[...], 0.0), axis=1, keepdims=True), shape)
    mu = [total[m : m + 1] for m in range(2 * ITERS)]

    def inner(x, y):
        sums = [None] * (len(x) + len(y) - 1)
        for i, xi in enumerate(x):
            for j, yj in enumerate(y):
                sums[i + j] = xi * yj if sums[i + j] is None else sums[i + j] + xi * yj
        out = sums[0] * mu[0]
        for m in range(1, len(sums)):
            out = out + sums[m] * mu[m]
        return out

    one = jnp.ones((1, 128), jnp.float32)
    zero = jnp.zeros((1, 128), jnp.float32)
    z, p, h = [one], [one], []
    rz = mu[0]
    for it in range(ITERS):
        image = [hi - lo for hi, lo in zip(p + [zero], [zero] + p)]
        alpha = rz / inner(p, image)
        h = [x + alpha * y for x, y in zip(h + [zero], p)]
        z = [x - alpha * y for x, y in zip(z + [zero], image)]
        if it + 1 < ITERS:
            new = inner(z, z)
            beta = new / rz
            p = [x + beta * y for x, y in zip(z, p + [zero])]
            rz = new
    height = h[0] * basis_in[0]
    for i in range(1, ITERS):
        height = height + h[i] * basis_in[i]
    resid = z[0] * basis_in[0]
    for i in range(1, ITERS + 1):
        resid = resid + z[i] * basis_in[i]
    height_buf[...] = height
    resid_buf[...] = diag_in[...] * resid
    last = [
        pltpu.make_async_copy(height_buf, height_ref, sem.at[1]),
        pltpu.make_async_copy(resid_buf, resid_ref, sem.at[2]),
    ]
    for store in last:
        store.start()
    pltpu.make_async_copy(tend_in, tend_in, sem.at[0]).wait()
    for store in last:
        store.wait()


def per_device(n_lon, n_lat, forcing, sea, count, state):
    fields, levels, rows, width = state.shape
    planes = fields * levels
    tall = planes + SUB
    half = SUB * ((tall // SUB + 1) // 2)
    assert levels % SUB == 0 and width == 128 and rows % SUB == 0 and rows >= 2 * SUB
    assert 4 * (rows + 2) <= width and 4 * (planes // SUB + 1) <= width
    sizes = (n_lon, n_lat, fields, levels, rows)
    f32 = jnp.float32
    vmem = pl.BlockSpec(memory_space=pltpu.VMEM)
    hbm = pl.BlockSpec(memory_space=pltpu.HBM)
    dma = pltpu.SemaphoreType.DMA
    held = pl.pallas_call(
        functools.partial(exchange, sizes),
        out_shape=(
            pltpu.VMEM((rows, planes, width), f32),
            pltpu.VMEM((ITERS + 1, rows, width), f32),
            pltpu.VMEM((rows, width), f32),
            pltpu.VMEM((2 * ITERS, width), f32),
        ),
        in_specs=[hbm] * 4,
        out_specs=(vmem,) * 4,
        scratch_shapes=[
            pltpu.VMEM((rows, width), f32),
            pltpu.VMEM((rows, width), jnp.int32),
            pltpu.VMEM((rows, width), jnp.int32),
            pltpu.VMEM((rows + 4, tall, width), f32),
            pltpu.VMEM((rows + 2, planes, width), f32),
            pltpu.VMEM((rows, levels, width), f32),
            pltpu.VMEM((rows, width), f32),
            pltpu.VMEM((2, rows, width), f32),
            pltpu.VMEM((2, rows, width), f32),
            pltpu.VMEM((2, 4, SUB, width), f32),
            pltpu.VMEM((tall, width), f32),
            pltpu.VMEM((2, half, width), f32),
            pltpu.VMEM((2, half, width), f32),
            pltpu.VMEM((2, SUB, width), f32),
            pltpu.VMEM((2, 2, SUB, width), f32),
            pltpu.VMEM((tall, width), f32),
            pltpu.VMEM((planes, width), f32),
            pltpu.VMEM((1, width), f32),
            pltpu.VMEM((n_lon * n_lat - 1, 1, width), f32),
            dma((4,)),
            dma((2,)),
            dma((2, 2)),
            dma((2,)),
            dma((2, 2)),
            dma((2, 2)),
            dma((2,)),
            pltpu.SemaphoreType.REGULAR,
        ],
        compiler_params=pltpu.CompilerParams(collective_id=0, has_side_effects=True),
    )(forcing, sea, count, state.reshape(planes, rows, width))
    small = jax.ShapeDtypeStruct((rows, width), f32)
    height, resid, tend = pl.pallas_call(
        deliver,
        out_shape=(small, small, jax.ShapeDtypeStruct((planes, rows, width), f32)),
        in_specs=[vmem] * 4,
        out_specs=(hbm,) * 3,
        scratch_shapes=[
            pltpu.VMEM((rows, width), f32),
            pltpu.VMEM((rows, width), f32),
            dma((3,)),
        ],
        compiler_params=pltpu.CompilerParams(vmem_limit_bytes=16 << 20),
    )(*held)
    return height, resid, tend.reshape(state.shape)


def solution(mesh):
    return jax.shard_map(
        functools.partial(per_device, mesh.shape["lon"], mesh.shape["lat"]),
        mesh=mesh,
        in_specs=(P("lat", "lon"), P("lat", "lon"), P("lat", "lon"), P(None, None, "lat", "lon")),
        out_specs=(P("lat", "lon"), P("lat", "lon"), P(None, None, "lat", "lon")),
        check_vma=False,
    )
```

```python
import functools

import jax
import jax.numpy as jnp
from jax import lax
from jax.experimental import pallas as pl
from jax.experimental.pallas import tpu as pltpu
from jax.sharding import PartitionSpec as P

ITERS = 4
DAMPING = 0.05
VISCOSITY = 0.02
SUB = 8
MESH = pl.DeviceIdType.MESH


def east(a, b, lane):
    ra, rb = pltpu.roll(a, 127, 1), pltpu.roll(b, 127, 1)
    keep = lane < 127
    return jnp.where(keep, ra, rb), jnp.where(keep, rb, ra)


def west(a, b, lane):
    ra, rb = pltpu.roll(a, 1, 1), pltpu.roll(b, 1, 1)
    keep = lane > 0
    return jnp.where(keep, ra, rb), jnp.where(keep, rb, ra)


def north(x):
    return pltpu.roll(x, x.shape[0] - 1, 0)


def south(x):
    return pltpu.roll(x, 1, 0)


def exchange(
    sizes,
    forcing_ref, sea_ref, count_ref, state_ref,
    tend_ref, basis_ref, diag_ref, total_ref,
    force_buf, sea_buf, count_buf, q_ref, lap_ref, near_ref,
    pack_ref, side_ref, pair_ref, vert_ref,
    strip_own, strip_out, strip_in, corner_out, corner_in, center_ref, slap_ref,
    part_ref, all_in,
    load_sem, side_sem, vert_sem, strip_sem, row_sem, corner_sem, all_sem, ready_sem,
):
    n_lon, n_lat, fields, levels, rows = sizes
    planes = fields * levels
    depth_tiles = levels // SUB
    tiles = planes // SUB
    ilon, ilat = lax.axis_index("lon"), lax.axis_index("lat")
    has = {1: ilat < n_lat - 1, -1: ilat > 0}

    def at(dlon, dlat):
        return {
            "lon": lax.rem(ilon + dlon + n_lon, n_lon),
            "lat": lax.rem(ilat + dlat + n_lat, n_lat),
        }

    inputs = [
        pltpu.make_async_copy(src, dst, load_sem.at[i])
        for i, (src, dst) in enumerate(((forcing_ref, force_buf), (sea_ref, sea_buf), (count_ref, count_buf)))
    ]
    for load in inputs:
        load.start()
    barrier = pltpu.get_barrier_semaphore()
    for dlat in (-1, 1):
        @pl.when(has[dlat])
        def _(dlat=dlat):
            for dlon in (-1, 1):
                pl.semaphore_signal(barrier, inc=1, device_id=at(dlon, dlat), device_id_type=MESH)
    for off in range(1, n_lat):
        pl.semaphore_signal(barrier, inc=1, device_id=at(0, off), device_id_type=MESH)
    for off in range(1, n_lon):
        pl.semaphore_signal(barrier, inc=1, device_id=at(off, 0), device_id_type=MESH)

    for j in range(rows):
        pltpu.make_async_copy(state_ref.at[:, j, :], q_ref.at[j + 2, pl.ds(0, planes)], load_sem.at[3]).start()

    def remote(src, dst, sems, index, where):
        return pltpu.make_async_remote_copy(
            src_ref=src, dst_ref=dst, send_sem=sems.at[(0,) + index], recv_sem=sems.at[(1,) + index],
            device_id=where, device_id_type=MESH,
        )

    def drained(ref, sems, index):
        pltpu.make_async_copy(ref, ref, sems.at[index]).wait()

    lane8 = lax.broadcasted_iota(jnp.int32, (SUB, 128), 1)
    sub8 = lax.broadcasted_iota(jnp.int32, (SUB, 128), 0)
    kio = [(sub8 + SUB * t).astype(jnp.float32) for t in range(depth_tiles)]
    slot8 = lane8 % 4
    last_lane, first_lane = lane8 == 127, lane8 == 0
    own = pl.ds(planes, SUB)

    def tile(t):
        return pl.ds(SUB * t, SUB)

    sides = ((0, -1, 0), (1, 1, rows - SUB))
    for v, dlat, _ in sides:
        @pl.when(jnp.logical_not(has[-dlat]))
        def _(v=v):
            vert_ref[v] = jnp.zeros_like(vert_ref[v])
            corner_in[v] = jnp.zeros_like(corner_in[v])
            for r in range(2):
                jj = rows + 2 + r if v == 0 else r
                q_ref[jj] = jnp.zeros_like(q_ref[jj])

    for load in inputs:
        load.wait()
    lane_r = lax.broadcasted_iota(jnp.int32, (rows, 128), 1)
    sea = sea_buf[...].astype(jnp.float32)
    wet = sea * count_buf[...].astype(jnp.float32)
    force = sea * force_buf[...]
    pair_ref[0] = force
    pair_ref[1] = wet
    inner_half = jnp.where(lane_r < 64, pltpu.roll(wet, 32, 1), pltpu.roll(wet, 96, 1))
    pack_ref[...] = jnp.where((lane_r >= 32) & (lane_r < 96), inner_half, force)
    for j in range(rows):
        q_ref[j + 2, own, :] = jnp.broadcast_to(wet[j : j + 1], (SUB, 128))

    diagonals = 2 * (has[1].astype(jnp.int32) + has[-1].astype(jnp.int32))
    pl.semaphore_wait(barrier, n_lon + n_lat - 2 + diagonals)

    for h, dlon in ((0, 1), (1, -1)):
        remote(pack_ref, side_ref.at[h], side_sem, (), at(dlon, 0)).start()
    for v, dlat, start in sides:
        @pl.when(has[dlat])
        def _(v=v, dlat=dlat, start=start):
            part = pl.ds(start, SUB)
            for h, dlon in ((0, 1), (1, -1)):
                remote(pack_ref.at[part], vert_ref.at[v, 2 + h], vert_sem, (v,), at(dlon, dlat)).start()
            remote(pair_ref.at[:, part], vert_ref.at[v, pl.ds(0, 2)], vert_sem, (v,), at(0, dlat)).start()

    for off in range(1, n_lat):
        pl.semaphore_signal(ready_sem, inc=1, device_id=at(0, off), device_id_type=MESH)

    pltpu.make_async_copy(
        q_ref.at[pl.ds(2, rows), pl.ds(0, planes)], q_ref.at[pl.ds(2, rows), pl.ds(0, planes)], load_sem.at[3]
    ).wait()

    packed = [jnp.zeros((SUB, 128), jnp.float32)] * (tiles + 1)
    for j in range(rows):
        here = lane8 // 4 == j + 1
        level = q_ref[j + 2, own, :]
        active = [k < level for k in kio]
        for t in range(tiles + 1):
            if t < tiles:
                q = jnp.where(active[t % depth_tiles], q_ref[j + 2, tile(t), :], 0.0)
                q_ref[j + 2, tile(t), :] = q
            else:
                q = level
            packed[t] = jnp.where(here, pltpu.roll(q, 4 * (j + 1) + 2, 1), packed[t])
    corners = [jnp.zeros((SUB, 128), jnp.float32)] * 2
    for t in range(tiles + 1):
        strip_own[tile(t), :] = packed[t]
        for v, j in ((0, 0), (1, rows - 1)):
            moved = pltpu.roll(packed[t], (4 * t - 4 * (j + 1)) % 128, 1)
            corners[v] = jnp.where(lane8 // 4 == t, moved, corners[v])
    for t in range(0, tiles + 1, 2):
        odd = packed[min(t + 1, tiles)]
        strip_out[0, tile(t // 2), :] = jnp.where(slot8 < 2, packed[t], pltpu.roll(odd, 2, 1))
        strip_out[1, tile(t // 2), :] = jnp.where(slot8 < 2, pltpu.roll(packed[t], 126, 1), odd)
    for v in range(2):
        corner_out[v] = corners[v]

    for h, dlon in ((0, 1), (1, -1)):
        remote(strip_out.at[h], strip_in.at[h], strip_sem, (), at(dlon, 0)).start()
    for v, dlat, _ in sides:
        @pl.when(has[dlat])
        def _(v=v, dlat=dlat):
            mine = pl.ds(2, 2) if v == 0 else pl.ds(rows, 2)
            there = pl.ds(rows + 2, 2) if v == 0 else pl.ds(0, 2)
            for h, dlon in ((0, 1), (1, -1)):
                remote(corner_out.at[v], corner_in.at[v, h], corner_sem, (v,), at(dlon, dlat)).start()
            remote(q_ref.at[mine], q_ref.at[there], row_sem, (v,), at(0, dlat)).start()

    def received(ref, sems, v, dlat):
        @pl.when(has[-dlat])
        def _():
            drained(ref, sems, (1, v))

    drained(side_ref, side_sem, (1,))
    for v, dlat, _ in sides:
        received(vert_ref.at[v], vert_sem, v, dlat)

    from_west = jnp.concatenate([side_ref[0], vert_ref[0, 2], vert_ref[1, 2]], axis=0)
    from_east = jnp.concatenate([side_ref[1], vert_ref[0, 3], vert_ref[1, 3]], axis=0)
    lane_t = lax.broadcasted_iota(jnp.int32, (rows + 2 * SUB, 128), 1)
    low = lane_t < 64
    force_a = jnp.concatenate([pair_ref[0], vert_ref[0, 0], vert_ref[1, 0]], axis=0)
    wet_a = jnp.concatenate([pair_ref[1], vert_ref[0, 1], vert_ref[1, 1]], axis=0)
    force_b = jnp.where(low, from_east, from_west)
    wet_b = jnp.where(low, pltpu.roll(from_east, 96, 1), pltpu.roll(from_west, 32, 1))
    depth_a, depth_b = wet_a / levels, wet_b / levels
    da, db = east(depth_a, depth_b, lane_t)
    ea, eb = jnp.minimum(depth_a, da), jnp.minimum(depth_b, db)
    da, db = west(depth_a, depth_b, lane_t)
    wa, wb = jnp.minimum(depth_a, da), jnp.minimum(depth_b, db)
    na, nb = jnp.minimum(depth_a, north(depth_a)), jnp.minimum(depth_b, north(depth_b))
    sa, sb = south(na), south(nb)
    diag_a = DAMPING + ea + wa + na + sa
    diag_b = DAMPING + eb + wb + nb + sb
    inv_a, inv_b = 1.0 / diag_a, 1.0 / diag_b
    va, vb = force_a * inv_a, force_b * inv_b
    ea, wa, na, sa = (c * inv_a for c in (ea, wa, na, sa))
    eb, wb, nb, sb = (c * inv_b for c in (eb, wb, nb, sb))
    diag = diag_a[:rows]
    diag_ref[...] = diag
    basis = [va[:rows]]
    for _ in range(ITERS):
        qe, qeb = east(va, vb, lane_t)
        qw, qwb = west(va, vb, lane_t)
        va, vb = (
            ea * qe + wa * qw + na * north(va) + sa * south(va),
            eb * qeb + wb * qwb + nb * north(vb) + sb * south(vb),
        )
        basis.append(va[:rows])
    for i, x in enumerate(basis):
        basis_ref[i] = x
    moments = []
    for m in range(2 * ITERS):
        moments.append(jnp.sum(diag * basis[m // 2] * basis[(m + 1) // 2], axis=0, keepdims=True))
    sums = jnp.broadcast_to(jnp.sum(jnp.concatenate(moments, axis=0), axis=1, keepdims=True), (2 * ITERS, 128))
    sums = jnp.where(lane8 // (128 // (2 * ITERS)) == sub8, sums, 0.0)
    part_ref[...] = jnp.sum(sums, axis=0, keepdims=True)
    pl.semaphore_wait(ready_sem, n_lat - 1)
    for off in sorted(range(1, n_lon * n_lat), key=lambda off: -min(off % n_lat, n_lat - off % n_lat)):
        remote(part_ref, all_in.at[off - 1], all_sem, (), at(off // n_lat, off % n_lat)).start()

    drained(strip_in, strip_sem, (1,))
    for v, dlat, _ in sides:
        received(corner_in.at[v], corner_sem, v, dlat)

    def swap(x, step):
        return jnp.where(slot8 < 2, pltpu.roll(x, 128 - step, 1), pltpu.roll(x, step, 1))

    def arrange(t):
        west_pair, east_pair = strip_in[0, tile(t // 2), :], strip_in[1, tile(t // 2), :]
        if t % 2:
            west_pair = pltpu.roll(west_pair, 126, 1)
        else:
            east_pair = pltpu.roll(east_pair, 2, 1)
        g = jnp.where(slot8 < 2, west_pair, east_pair)
        for v, j in ((0, rows), (1, -1)):
            corner = jnp.where(slot8 < 2, corner_in[v, 0], corner_in[v, 1])
            moved = pltpu.roll(corner, (4 * (j + 1) - 4 * t) % 128, 1)
            g = jnp.where(lane8 // 4 == j + 1, moved, g)
        center = swap(g, 1)
        return center, strip_own[tile(t), :], swap(g, 2), pltpu.roll(center, 124, 1), pltpu.roll(center, 4, 1)

    ring = arrange(tiles)
    center_ref[tile(tiles), :] = ring[0]
    edge_coef = []
    for k in kio:
        count = sum(jnp.where(k < w, 1.0, 0.0) for w in ring[1:])
        first = jnp.where(k < ring[0], -VISCOSITY, 0.0)
        edge_coef.append((first, first * count))
    for t in range(tiles):
        center, a, b, c, d = arrange(t)
        center_ref[tile(t), :] = center
        first, second = edge_coef[t % depth_tiles]
        slap_ref[tile(t), :] = first * ((a + b) + (c + d)) - second * center

    def beside(x, edge):
        return (
            jnp.where(last_lane, edge, pltpu.roll(x, 127, 1)),
            jnp.where(first_lane, edge, pltpu.roll(x, 1, 1)),
        )

    def laplace(jj, inside):
        shift = 130 - 4 * jj
        level = q_ref[jj, own, :]
        around = beside(level, pltpu.roll(center_ref[own, :], shift, 1)) + (q_ref[jj + 1, own, :], q_ref[jj - 1, own, :])
        for k in range(depth_tiles):
            here, oe, ow, on, os = (kio[k] < x for x in (level,) + around)
            ones = [jnp.where(x, 1.0, 0.0) for x in (oe, ow, on, os)]
            count = (ones[0] + ones[1]) + (ones[2] + ones[3])
            first = jnp.where(here, -VISCOSITY, 0.0)
            second = first * count

            def plane(f):
                at_tile = tile(f * depth_tiles + k)
                q = q_ref[jj, at_tile, :]
                qe, qw = beside(q, pltpu.roll(center_ref[at_tile, :], shift, 1))
                qn, qs = q_ref[jj + 1, at_tile, :], q_ref[jj - 1, at_tile, :]
                lap_ref[jj - 1, at_tile, :] = first * ((qe + qw) + (qn + qs)) - second * q
                return q, qe, qw, qn, qs

            if not inside:
                for f in range(fields):
                    plane(f)
                continue
            near_ref[jj - 2, tile(k), :] = count
            quarter = jnp.where(here, 0.25, 0.0)
            planes_of = {2: plane(2), 3: plane(3)}
            u, ue, uw, _, _ = planes_of[2]
            v, _, _, vn, vs = planes_of[3]
            fe = jnp.where(oe, quarter * (u + ue), 0.0)
            fw = jnp.where(ow, quarter * (u + uw), 0.0)
            fn = jnp.where(on, quarter * (v + vn), 0.0)
            fs = jnp.where(os, quarter * (v + vs), 0.0)
            net = (fw - fe) + (fs - fn)
            for f in (2, 3, 0, 1):
                q, qe, qw, qn, qs = planes_of[f] if f in planes_of else plane(f)
                tend_ref[jj - 2, tile(f * depth_tiles + k), :] = (
                    net * q + (fw * qw - fe * qe) + (fs * qs - fn * qn)
                )

    def finish(j):
        shift = 122 - 4 * j
        level = q_ref[j + 2, own, :]
        for k in range(depth_tiles):
            here = kio[k] < level
            count = near_ref[j, tile(k), :]
            for f in range(fields):
                at_tile = tile(f * depth_tiles + k)
                lap = lap_ref[j + 1, at_tile, :]
                le, lw = beside(lap, pltpu.roll(slap_ref[at_tile, :], shift, 1))
                total = (le + lw) + (lap_ref[j + 2, at_tile, :] + lap_ref[j, at_tile, :])
                tend_ref[j, at_tile, :] += jnp.where(here, total, 0.0) - count * lap

    def ahead(i, carry):
        for r in range(2):
            laplace(2 * i + 3 + r, True)
        return carry

    lax.fori_loop(0, 2, ahead, 0)

    def both(i, carry):
        for r in range(2):
            finish(2 * i - 2 + r)
        for r in range(2):
            laplace(2 * i + 3 + r, True)
        return carry

    lax.fori_loop(2, rows // 2 - 1, both, 0)
    for j in (rows - 4, rows - 3):
        finish(j)

    for v, dlat, _ in sides:
        rim = q_ref.at[pl.ds(rows + 2, 2)] if v == 0 else q_ref.at[pl.ds(0, 2)]
        received(rim, row_sem, v, dlat)

    def rim(v, carry):
        laplace(1 + v * (rows + 1), False)
        laplace(2 + v * (rows - 1), True)
        for r in range(2):
            finish(v * (rows - 2) + r)
        return carry

    lax.fori_loop(0, 2, rim, 0)

    drained(all_in, all_sem, (1,))
    total = part_ref[...]
    for i in range(n_lon * n_lat - 1):
        total = total + all_in[i]
    total_ref[...] = jnp.broadcast_to(total, total_ref.shape)

    drained(side_ref, side_sem, (0,))
    drained(strip_in, strip_sem, (0,))
    drained(all_in, all_sem, (0,))
    for v, dlat, _ in sides:
        @pl.when(has[dlat])
        def _(v=v):
            drained(vert_ref.at[v], vert_sem, (0, v))
            drained(corner_in.at[v], corner_sem, (0, v))
            drained(q_ref.at[pl.ds(0, 2)], row_sem, (0, v))


def deliver(tend_in, basis_in, diag_in, total_in, height_ref, resid_ref, tend_ref, height_buf, resid_buf, sem):
    rows = tend_in.shape[0]
    stores = [pltpu.make_async_copy(tend_in.at[j], tend_ref.at[:, j, :], sem.at[0]) for j in range(rows)]
    for store in stores:
        store.start()
    part = 128 // (2 * ITERS)
    shape = (2 * ITERS, 128)
    mine = lax.broadcasted_iota(jnp.int32, shape, 1) == part * lax.broadcasted_iota(jnp.int32, shape, 0)
    total = jnp.broadcast_to(jnp.sum(jnp.where(mine, total_in[...], 0.0), axis=1, keepdims=True), shape)
    mu = [total[m : m + 1] for m in range(2 * ITERS)]

    def inner(x, y):
        sums = [None] * (len(x) + len(y) - 1)
        for i, xi in enumerate(x):
            for j, yj in enumerate(y):
                sums[i + j] = xi * yj if sums[i + j] is None else sums[i + j] + xi * yj
        out = sums[0] * mu[0]
        for m in range(1, len(sums)):
            out = out + sums[m] * mu[m]
        return out

    one = jnp.ones((1, 128), jnp.float32)
    zero = jnp.zeros((1, 128), jnp.float32)
    z, p, h = [one], [one], []
    rz = mu[0]
    for it in range(ITERS):
        image = [hi - lo for hi, lo in zip(p + [zero], [zero] + p)]
        alpha = rz / inner(p, image)
        h = [x + alpha * y for x, y in zip(h + [zero], p)]
        z = [x - alpha * y for x, y in zip(z + [zero], image)]
        if it + 1 < ITERS:
            new = inner(z, z)
            beta = new / rz
            p = [x + beta * y for x, y in zip(z, p + [zero])]
            rz = new
    height = h[0] * basis_in[0]
    for i in range(1, ITERS):
        height = height + h[i] * basis_in[i]
    resid = z[0] * basis_in[0]
    for i in range(1, ITERS + 1):
        resid = resid + z[i] * basis_in[i]
    height_buf[...] = height
    resid_buf[...] = diag_in[...] * resid
    last = [
        pltpu.make_async_copy(height_buf, height_ref, sem.at[1]),
        pltpu.make_async_copy(resid_buf, resid_ref, sem.at[2]),
    ]
    for store in last:
        store.start()
    pltpu.make_async_copy(tend_in, tend_in, sem.at[0]).wait()
    for store in last:
        store.wait()


def per_device(n_lon, n_lat, forcing, sea, count, state):
    fields, levels, rows, width = state.shape
    planes = fields * levels
    tall = planes + SUB
    half = SUB * ((tall // SUB + 1) // 2)
    assert levels % SUB == 0 and width == 128 and rows % SUB == 0 and rows >= 2 * SUB
    assert 4 * (rows + 2) <= width and 4 * (planes // SUB + 1) <= width
    sizes = (n_lon, n_lat, fields, levels, rows)
    f32 = jnp.float32
    vmem = pl.BlockSpec(memory_space=pltpu.VMEM)
    hbm = pl.BlockSpec(memory_space=pltpu.HBM)
    dma = pltpu.SemaphoreType.DMA
    held = pl.pallas_call(
        functools.partial(exchange, sizes),
        out_shape=(
            pltpu.VMEM((rows, planes, width), f32),
            pltpu.VMEM((ITERS + 1, rows, width), f32),
            pltpu.VMEM((rows, width), f32),
            pltpu.VMEM((2 * ITERS, width), f32),
        ),
        in_specs=[hbm] * 4,
        out_specs=(vmem,) * 4,
        scratch_shapes=[
            pltpu.VMEM((rows, width), f32),
            pltpu.VMEM((rows, width), jnp.int32),
            pltpu.VMEM((rows, width), jnp.int32),
            pltpu.VMEM((rows + 4, tall, width), f32),
            pltpu.VMEM((rows + 2, planes, width), f32),
            pltpu.VMEM((rows, levels, width), f32),
            pltpu.VMEM((rows, width), f32),
            pltpu.VMEM((2, rows, width), f32),
            pltpu.VMEM((2, rows, width), f32),
            pltpu.VMEM((2, 4, SUB, width), f32),
            pltpu.VMEM((tall, width), f32),
            pltpu.VMEM((2, half, width), f32),
            pltpu.VMEM((2, half, width), f32),
            pltpu.VMEM((2, SUB, width), f32),
            pltpu.VMEM((2, 2, SUB, width), f32),
            pltpu.VMEM((tall, width), f32),
            pltpu.VMEM((planes, width), f32),
            pltpu.VMEM((1, width), f32),
            pltpu.VMEM((n_lon * n_lat - 1, 1, width), f32),
            dma((4,)),
            dma((2,)),
            dma((2, 2)),
            dma((2,)),
            dma((2, 2)),
            dma((2, 2)),
            dma((2,)),
            pltpu.SemaphoreType.REGULAR,
        ],
        compiler_params=pltpu.CompilerParams(collective_id=0, has_side_effects=True),
    )(forcing, sea, count, state.reshape(planes, rows, width))
    small = jax.ShapeDtypeStruct((rows, width), f32)
    height, resid, tend = pl.pallas_call(
        deliver,
        out_shape=(small, small, jax.ShapeDtypeStruct((planes, rows, width), f32)),
        in_specs=[vmem] * 4,
        out_specs=(hbm,) * 3,
        scratch_shapes=[
            pltpu.VMEM((rows, width), f32),
            pltpu.VMEM((rows, width), f32),
            dma((3,)),
        ],
        compiler_params=pltpu.CompilerParams(vmem_limit_bytes=16 << 20),
    )(*held)
    return height, resid, tend.reshape(state.shape)


def solution(mesh):
    return jax.shard_map(
        functools.partial(per_device, mesh.shape["lon"], mesh.shape["lat"]),
        mesh=mesh,
        in_specs=(P("lat", "lon"), P("lat", "lon"), P("lat", "lon"), P(None, None, "lat", "lon")),
        out_specs=(P("lat", "lon"), P("lat", "lon"), P(None, None, "lat", "lon")),
        check_vma=False,
    )
```

```python
import functools

import jax
import jax.numpy as jnp
from jax import lax
from jax.experimental import pallas as pl
from jax.experimental.pallas import tpu as pltpu
from jax.sharding import PartitionSpec as P

ITERS = 4
DAMPING = 0.05
VISCOSITY = 0.02
SUB = 8
MESH = pl.DeviceIdType.MESH


def east(a, b, lane):
    ra, rb = pltpu.roll(a, 127, 1), pltpu.roll(b, 127, 1)
    keep = lane < 127
    return jnp.where(keep, ra, rb), jnp.where(keep, rb, ra)


def west(a, b, lane):
    ra, rb = pltpu.roll(a, 1, 1), pltpu.roll(b, 1, 1)
    keep = lane > 0
    return jnp.where(keep, ra, rb), jnp.where(keep, rb, ra)


def north(x):
    return pltpu.roll(x, x.shape[0] - 1, 0)


def south(x):
    return pltpu.roll(x, 1, 0)


def exchange(
    sizes,
    forcing_ref, sea_ref, count_ref, state_ref,
    tend_ref, basis_ref, diag_ref, total_ref,
    force_buf, sea_buf, count_buf, q_ref, lap_ref, near_ref,
    pack_ref, side_ref, pair_ref, vert_ref,
    strip_own, strip_out, strip_in, corner_out, corner_in, center_ref, slap_ref,
    part_ref, all_in,
    meter_ref, load_sem, send_sem, one_sem, vert_sem, row_sem, corner_sem, ready_sem,
):
    n_lon, n_lat, fields, levels, rows = sizes
    planes = fields * levels
    depth_tiles = levels // SUB
    tiles = planes // SUB
    ilon, ilat = lax.axis_index("lon"), lax.axis_index("lat")
    has = {1: ilat < n_lat - 1, -1: ilat > 0}

    def at(dlon, dlat):
        return {
            "lon": lax.rem(ilon + dlon + n_lon, n_lon),
            "lat": lax.rem(ilat + dlat + n_lat, n_lat),
        }

    inputs = [
        pltpu.make_async_copy(src, dst, load_sem.at[0])
        for src, dst in ((forcing_ref, force_buf), (sea_ref, sea_buf), (count_ref, count_buf))
    ]
    for load in inputs:
        load.start()
    barrier = pltpu.get_barrier_semaphore()
    for dlat in (-1, 1):
        @pl.when(has[dlat])
        def _(dlat=dlat):
            for dlon in (-1, 1):
                pl.semaphore_signal(barrier, inc=1, device_id=at(dlon, dlat), device_id_type=MESH)
    for off in range(1, n_lat):
        pl.semaphore_signal(barrier, inc=1, device_id=at(0, off), device_id_type=MESH)
    for off in range(1, n_lon):
        pl.semaphore_signal(barrier, inc=1, device_id=at(off, 0), device_id_type=MESH)

    for j in range(rows):
        pltpu.make_async_copy(state_ref.at[:, j, :], q_ref.at[j + 2, pl.ds(0, planes)], load_sem.at[1]).start()

    def remote(src, dst, sent, sem, where):
        return pltpu.make_async_remote_copy(
            src_ref=src, dst_ref=dst, send_sem=send_sem.at[sent], recv_sem=sem,
            device_id=where, device_id_type=MESH,
        )

    def drained(ref, sem):
        pltpu.make_async_copy(ref, ref, sem).wait()

    lane8 = lax.broadcasted_iota(jnp.int32, (SUB, 128), 1)
    sub8 = lax.broadcasted_iota(jnp.int32, (SUB, 128), 0)
    kio = [(sub8 + SUB * t).astype(jnp.float32) for t in range(depth_tiles)]
    slot8 = lane8 % 4
    last_lane, first_lane = lane8 == 127, lane8 == 0
    own = pl.ds(planes, SUB)

    def tile(t):
        return pl.ds(SUB * t, SUB)

    sides = ((0, -1, 0), (1, 1, rows - SUB))
    for v, dlat, _ in sides:
        @pl.when(jnp.logical_not(has[-dlat]))
        def _(v=v):
            vert_ref[v] = jnp.zeros_like(vert_ref[v])
            corner_in[v] = jnp.zeros_like(corner_in[v])
            for r in range(2):
                jj = rows + 2 + r if v == 0 else r
                q_ref[jj] = jnp.zeros_like(q_ref[jj])

    drained(meter_ref.at[pl.ds(0, 3 * rows)], load_sem.at[0])
    lane_r = lax.broadcasted_iota(jnp.int32, (rows, 128), 1)
    sea = sea_buf[...].astype(jnp.float32)
    wet = sea * count_buf[...].astype(jnp.float32)
    force = sea * force_buf[...]
    pair_ref[0] = force
    pair_ref[1] = wet
    inner_half = jnp.where(lane_r < 64, pltpu.roll(force, 32, 1), pltpu.roll(force, 96, 1))
    pack_ref[...] = jnp.where((lane_r >= 32) & (lane_r < 96), inner_half, wet)
    for j in range(rows):
        q_ref[j + 2, own, :] = jnp.broadcast_to(wet[j : j + 1], (SUB, 128))

    early = ilat < n_lat // 4

    def prepare():
        pltpu.make_async_copy(
            q_ref.at[pl.ds(2, rows), pl.ds(0, planes)], q_ref.at[pl.ds(2, rows), pl.ds(0, planes)], load_sem.at[1]
        ).wait()

        packed = [jnp.zeros((SUB, 128), jnp.float32)] * (tiles + 1)
        for j in range(rows):
            here = lane8 // 4 == j + 1
            level = q_ref[j + 2, own, :]
            active = [k < level for k in kio]
            for t in range(tiles + 1):
                if t < tiles:
                    q = jnp.where(active[t % depth_tiles], q_ref[j + 2, tile(t), :], 0.0)
                    q_ref[j + 2, tile(t), :] = q
                else:
                    q = level
                packed[t] = jnp.where(here, pltpu.roll(q, 4 * (j + 1) + 2, 1), packed[t])
        corners = [jnp.zeros((SUB, 128), jnp.float32)] * 2
        for t in range(tiles + 1):
            strip_own[tile(t), :] = packed[t]
            for v, j in ((0, 0), (1, rows - 1)):
                moved = pltpu.roll(packed[t], (4 * t - 4 * (j + 1)) % 128, 1)
                corners[v] = jnp.where(lane8 // 4 == t, moved, corners[v])
        for t in range(0, tiles + 1, 2):
            odd = packed[min(t + 1, tiles)]
            strip_out[0, tile(t // 2), :] = jnp.where(slot8 < 2, packed[t], pltpu.roll(odd, 2, 1))
            strip_out[1, tile(t // 2), :] = jnp.where(slot8 < 2, pltpu.roll(packed[t], 126, 1), odd)
        for v in range(2):
            corner_out[v] = corners[v]

    @pl.when(early)
    def _():
        prepare()

    diagonals = 2 * (has[1].astype(jnp.int32) + has[-1].astype(jnp.int32))
    pl.semaphore_wait(barrier, n_lon + n_lat - 2 + diagonals)

    for h, dlon in ((0, 1), (1, -1)):
        remote(pack_ref, side_ref.at[h], 2, one_sem.at[0], at(dlon, 0)).start()
    for v, dlat, start in sides:
        @pl.when(has[dlat])
        def _(v=v, dlat=dlat, start=start):
            part = pl.ds(start, SUB)
            for h, dlon in ((0, 1), (1, -1)):
                remote(pack_ref.at[part], vert_ref.at[v, 2 + h], v, vert_sem.at[v], at(dlon, dlat)).start()
            remote(pair_ref.at[:, part], vert_ref.at[v, pl.ds(0, 2)], v, vert_sem.at[v], at(0, dlat)).start()

    for off in range(1, n_lat):
        pl.semaphore_signal(ready_sem, inc=1, device_id=at(0, off), device_id_type=MESH)

    @pl.when(jnp.logical_not(early))
    def _():
        prepare()

    for h, dlon in ((0, 1), (1, -1)):
        remote(strip_out.at[h], strip_in.at[h], 2, one_sem.at[1], at(dlon, 0)).start()
    for v, dlat, _ in sides:
        @pl.when(has[dlat])
        def _(v=v, dlat=dlat):
            mine = pl.ds(2, 2) if v == 0 else pl.ds(rows, 2)
            there = pl.ds(rows + 2, 2) if v == 0 else pl.ds(0, 2)
            for h, dlon in ((0, 1), (1, -1)):
                remote(corner_out.at[v], corner_in.at[v, h], v, corner_sem.at[v], at(dlon, dlat)).start()
            remote(q_ref.at[mine], q_ref.at[there], v, row_sem.at[v], at(0, dlat)).start()

    def received(ref, sems, v, dlat):
        @pl.when(has[-dlat])
        def _():
            drained(ref, sems.at[v])

    drained(side_ref, one_sem.at[0])
    for v, dlat, _ in sides:
        received(vert_ref.at[v], vert_sem, v, dlat)

    from_west = jnp.concatenate([side_ref[0], vert_ref[0, 2], vert_ref[1, 2]], axis=0)
    from_east = jnp.concatenate([side_ref[1], vert_ref[0, 3], vert_ref[1, 3]], axis=0)
    lane_t = lax.broadcasted_iota(jnp.int32, (rows + 2 * SUB, 128), 1)
    low = lane_t < 64
    force_a = jnp.concatenate([pair_ref[0], vert_ref[0, 0], vert_ref[1, 0]], axis=0)
    wet_a = jnp.concatenate([pair_ref[1], vert_ref[0, 1], vert_ref[1, 1]], axis=0)
    wet_b = jnp.where(low, from_east, from_west)
    force_b = jnp.where(low, pltpu.roll(from_east, 96, 1), pltpu.roll(from_west, 32, 1))
    depth_a, depth_b = wet_a / levels, wet_b / levels
    da, db = east(depth_a, depth_b, lane_t)
    ea, eb = jnp.minimum(depth_a, da), jnp.minimum(depth_b, db)
    da, db = west(depth_a, depth_b, lane_t)
    wa, wb = jnp.minimum(depth_a, da), jnp.minimum(depth_b, db)
    na, nb = jnp.minimum(depth_a, north(depth_a)), jnp.minimum(depth_b, north(depth_b))
    sa, sb = south(na), south(nb)
    diag_a = DAMPING + ea + wa + na + sa
    diag_b = DAMPING + eb + wb + nb + sb
    inv_a, inv_b = 1.0 / diag_a, 1.0 / diag_b
    va, vb = force_a * inv_a, force_b * inv_b
    ea, wa, na, sa = (c * inv_a for c in (ea, wa, na, sa))
    eb, wb, nb, sb = (c * inv_b for c in (eb, wb, nb, sb))
    diag = diag_a[:rows]
    diag_ref[...] = diag
    basis = [va[:rows]]
    for _ in range(ITERS):
        qe, qeb = east(va, vb, lane_t)
        qw, qwb = west(va, vb, lane_t)
        va, vb = (
            ea * qe + wa * qw + na * north(va) + sa * south(va),
            eb * qeb + wb * qwb + nb * north(vb) + sb * south(vb),
        )
        basis.append(va[:rows])
    for i, x in enumerate(basis):
        basis_ref[i] = x
    moments = []
    for m in range(2 * ITERS):
        moments.append(jnp.sum(diag * basis[m // 2] * basis[(m + 1) // 2], axis=0, keepdims=True))
    sums = jnp.broadcast_to(jnp.sum(jnp.concatenate(moments, axis=0), axis=1, keepdims=True), (2 * ITERS, 128))
    sums = jnp.where(lane8 // (128 // (2 * ITERS)) == sub8, sums, 0.0)
    part_ref[...] = jnp.sum(sums, axis=0, keepdims=True)
    pl.semaphore_wait(ready_sem, n_lat - 1)
    all_in[ilat * n_lon] = part_ref[...]
    for k in range(n_lat):
        for off in range(n_lon):
            def share(k=k, off=off):
                where = {"lon": lax.rem(ilon + off, n_lon), "lat": k}
                remote(part_ref, all_in.at[ilat * n_lon + off], 2, one_sem.at[2], where).start()

            if off:
                share()
            else:
                pl.when(ilat != k)(share)

    drained(strip_in, one_sem.at[1])
    for v, dlat, _ in sides:
        received(corner_in.at[v], corner_sem, v, dlat)

    def swap(x, step):
        return jnp.where(slot8 < 2, pltpu.roll(x, 128 - step, 1), pltpu.roll(x, step, 1))

    def arrange(t):
        west_pair, east_pair = strip_in[0, tile(t // 2), :], strip_in[1, tile(t // 2), :]
        if t % 2:
            west_pair = pltpu.roll(west_pair, 126, 1)
        else:
            east_pair = pltpu.roll(east_pair, 2, 1)
        g = jnp.where(slot8 < 2, west_pair, east_pair)
        for v, j in ((0, rows), (1, -1)):
            corner = jnp.where(slot8 < 2, corner_in[v, 0], corner_in[v, 1])
            moved = pltpu.roll(corner, (4 * (j + 1) - 4 * t) % 128, 1)
            g = jnp.where(lane8 // 4 == j + 1, moved, g)
        center = swap(g, 1)
        return center, strip_own[tile(t), :], swap(g, 2), pltpu.roll(center, 124, 1), pltpu.roll(center, 4, 1)

    ring = arrange(tiles)
    center_ref[tile(tiles), :] = ring[0]
    edge_coef = []
    for k in kio:
        count = sum(jnp.where(k < w, 1.0, 0.0) for w in ring[1:])
        first = jnp.where(k < ring[0], -VISCOSITY, 0.0)
        edge_coef.append((first, first * count))
    for t in range(tiles):
        center, a, b, c, d = arrange(t)
        center_ref[tile(t), :] = center
        first, second = edge_coef[t % depth_tiles]
        slap_ref[tile(t), :] = first * ((a + b) + (c + d)) - second * center

    def beside(x, edge):
        return (
            jnp.where(last_lane, edge, pltpu.roll(x, 127, 1)),
            jnp.where(first_lane, edge, pltpu.roll(x, 1, 1)),
        )

    def laplace(jj, inside):
        shift = 130 - 4 * jj

        def row_beside(x, where):
            return beside(x, pltpu.roll(center_ref[where, :], shift, 1))

        level = q_ref[jj, own, :]
        around = row_beside(level, own) + (q_ref[jj + 1, own, :], q_ref[jj - 1, own, :])
        for k in range(depth_tiles):
            here, oe, ow, on, os = (kio[k] < x for x in (level,) + around)
            ones = [jnp.where(x, 1.0, 0.0) for x in (oe, ow, on, os)]
            count = (ones[0] + ones[1]) + (ones[2] + ones[3])
            first = jnp.where(here, -VISCOSITY, 0.0)
            second = first * count

            def plane(f):
                at_tile = tile(f * depth_tiles + k)
                q = q_ref[jj, at_tile, :]
                qe, qw = row_beside(q, at_tile)
                qn, qs = q_ref[jj + 1, at_tile, :], q_ref[jj - 1, at_tile, :]
                lap_ref[jj - 1, at_tile, :] = first * ((qe + qw) + (qn + qs)) - second * q
                return q, qe, qw, qn, qs

            if not inside:
                for f in range(fields):
                    plane(f)
                continue
            near_ref[jj - 2, tile(k), :] = count
            quarter = jnp.where(here, 0.25, 0.0)
            planes_of = {2: plane(2), 3: plane(3)}
            u, ue, uw, _, _ = planes_of[2]
            v, _, _, vn, vs = planes_of[3]
            fe = jnp.where(oe, quarter * (u + ue), 0.0)
            fw = jnp.where(ow, quarter * (u + uw), 0.0)
            fn = jnp.where(on, quarter * (v + vn), 0.0)
            fs = jnp.where(os, quarter * (v + vs), 0.0)
            net = (fw - fe) + (fs - fn)
            for f in (2, 3, 0, 1):
                q, qe, qw, qn, qs = planes_of[f] if f in planes_of else plane(f)
                tend_ref[jj - 2, tile(f * depth_tiles + k), :] = (
                    net * q + (fw * qw - fe * qe) + (fs * qs - fn * qn)
                )

    def finish(j):
        shift = 122 - 4 * j
        level = q_ref[j + 2, own, :]
        for k in range(depth_tiles):
            here = kio[k] < level
            count = near_ref[j, tile(k), :]
            for f in range(fields):
                at_tile = tile(f * depth_tiles + k)
                lap = lap_ref[j + 1, at_tile, :]
                le, lw = beside(lap, pltpu.roll(slap_ref[at_tile, :], shift, 1))
                total = (le + lw) + (lap_ref[j + 2, at_tile, :] + lap_ref[j, at_tile, :])
                tend_ref[j, at_tile, :] += jnp.where(here, total, 0.0) - count * lap

    def ahead(i, carry):
        for r in range(2):
            laplace(2 * i + 3 + r, True)
        return carry

    lax.fori_loop(0, 2, ahead, 0)

    def both(i, carry):
        for r in range(2):
            finish(2 * i - 2 + r)
        for r in range(2):
            laplace(2 * i + 3 + r, True)
        return carry

    lax.fori_loop(2, rows // 2 - 1, both, 0)
    for j in (rows - 4, rows - 3):
        finish(j)

    for v, dlat, _ in sides:
        rim = q_ref.at[pl.ds(rows + 2, 2)] if v == 0 else q_ref.at[pl.ds(0, 2)]
        received(rim, row_sem, v, dlat)

    def rim(v, carry):
        laplace(1 + v * (rows + 1), False)
        laplace(2 + v * (rows - 1), True)
        for r in range(2):
            finish(v * (rows - 2) + r)
        return carry

    lax.fori_loop(0, 2, rim, 0)

    drained(all_in.at[pl.ds(0, n_lon * n_lat - 1)], one_sem.at[2])
    terms = [all_in[i] for i in range(n_lon * n_lat)]
    while len(terms) > 1:
        terms = [a + b for a, b in zip(terms[::2], terms[1::2])] + terms[len(terms) - len(terms) % 2 :]
    total = terms[0]
    total_ref[...] = jnp.broadcast_to(total, total_ref.shape)

    half = strip_out.shape[1]
    drained(meter_ref.at[pl.ds(0, 2 * rows + 2 * half + n_lon * n_lat - 1)], send_sem.at[2])
    for v, dlat, _ in sides:
        @pl.when(has[dlat])
        def _(v=v):
            drained(meter_ref.at[pl.ds(0, 6 * SUB + 2 * (planes + SUB))], send_sem.at[v])


def deliver(tend_in, basis_in, diag_in, total_in, height_ref, resid_ref, tend_ref, height_buf, resid_buf, sem):
    rows = tend_in.shape[0]
    stores = [pltpu.make_async_copy(tend_in.at[j], tend_ref.at[:, j, :], sem.at[0]) for j in range(rows)]
    for store in stores:
        store.start()
    part = 128 // (2 * ITERS)
    shape = (2 * ITERS, 128)
    mine = lax.broadcasted_iota(jnp.int32, shape, 1) == part * lax.broadcasted_iota(jnp.int32, shape, 0)
    total = jnp.broadcast_to(jnp.sum(jnp.where(mine, total_in[...], 0.0), axis=1, keepdims=True), shape)
    mu = [total[m : m + 1] for m in range(2 * ITERS)]

    def inner(x, y):
        sums = [None] * (len(x) + len(y) - 1)
        for i, xi in enumerate(x):
            for j, yj in enumerate(y):
                sums[i + j] = xi * yj if sums[i + j] is None else sums[i + j] + xi * yj
        out = sums[0] * mu[0]
        for m in range(1, len(sums)):
            out = out + sums[m] * mu[m]
        return out

    one = jnp.ones((1, 128), jnp.float32)
    zero = jnp.zeros((1, 128), jnp.float32)
    z, p, h = [one], [one], []
    rz = mu[0]
    for it in range(ITERS):
        image = [hi - lo for hi, lo in zip(p + [zero], [zero] + p)]
        alpha = rz / inner(p, image)
        h = [x + alpha * y for x, y in zip(h + [zero], p)]
        z = [x - alpha * y for x, y in zip(z + [zero], image)]
        if it + 1 < ITERS:
            new = inner(z, z)
            beta = new / rz
            p = [x + beta * y for x, y in zip(z, p + [zero])]
            rz = new
    height = h[0] * basis_in[0]
    for i in range(1, ITERS):
        height = height + h[i] * basis_in[i]
    resid = z[0] * basis_in[0]
    for i in range(1, ITERS + 1):
        resid = resid + z[i] * basis_in[i]
    height_buf[...] = height
    resid_buf[...] = diag_in[...] * resid
    last = [
        pltpu.make_async_copy(height_buf, height_ref, sem.at[1]),
        pltpu.make_async_copy(resid_buf, resid_ref, sem.at[2]),
    ]
    for store in last:
        store.start()
    pltpu.make_async_copy(tend_in, tend_in, sem.at[0]).wait()
    for store in last:
        store.wait()


def per_device(n_lon, n_lat, forcing, sea, count, state):
    fields, levels, rows, width = state.shape
    planes = fields * levels
    tall = planes + SUB
    half = SUB * ((tall // SUB + 1) // 2)
    assert levels % SUB == 0 and width == 128 and rows % SUB == 0 and rows >= 2 * SUB
    assert 4 * (rows + 2) <= width and 4 * (planes // SUB + 1) <= width
    sizes = (n_lon, n_lat, fields, levels, rows)
    f32 = jnp.float32
    vmem = pl.BlockSpec(memory_space=pltpu.VMEM)
    hbm = pl.BlockSpec(memory_space=pltpu.HBM)
    dma = pltpu.SemaphoreType.DMA
    held = pl.pallas_call(
        functools.partial(exchange, sizes),
        out_shape=(
            pltpu.VMEM((rows, planes, width), f32),
            pltpu.VMEM((ITERS + 1, rows, width), f32),
            pltpu.VMEM((rows, width), f32),
            pltpu.VMEM((2 * ITERS, width), f32),
        ),
        in_specs=[hbm] * 4,
        out_specs=(vmem,) * 4,
        scratch_shapes=[
            pltpu.VMEM((rows, width), f32),
            pltpu.VMEM((rows, width), jnp.int32),
            pltpu.VMEM((rows, width), jnp.int32),
            pltpu.VMEM((rows + 4, tall, width), f32),
            pltpu.VMEM((rows + 2, planes, width), f32),
            pltpu.VMEM((rows, levels, width), f32),
            pltpu.VMEM((rows, width), f32),
            pltpu.VMEM((2, rows, width), f32),
            pltpu.VMEM((2, rows, width), f32),
            pltpu.VMEM((2, 4, SUB, width), f32),
            pltpu.VMEM((tall, width), f32),
            pltpu.VMEM((2, half, width), f32),
            pltpu.VMEM((2, half, width), f32),
            pltpu.VMEM((2, SUB, width), f32),
            pltpu.VMEM((2, 2, SUB, width), f32),
            pltpu.VMEM((tall, width), f32),
            pltpu.VMEM((planes, width), f32),
            pltpu.VMEM((1, width), f32),
            pltpu.VMEM((n_lon * n_lat, 1, width), f32),
            pltpu.VMEM((max(6 * SUB + 2 * tall, 2 * rows + 2 * half + n_lon * n_lat), 1, width), f32),
            dma((2,)),
            dma((3,)),
            dma((3,)),
            dma((2,)),
            dma((2,)),
            dma((2,)),
            pltpu.SemaphoreType.REGULAR,
        ],
        compiler_params=pltpu.CompilerParams(collective_id=0, has_side_effects=True),
    )(forcing, sea, count, state.reshape(planes, rows, width))
    small = jax.ShapeDtypeStruct((rows, width), f32)
    height, resid, tend = pl.pallas_call(
        deliver,
        out_shape=(small, small, jax.ShapeDtypeStruct((planes, rows, width), f32)),
        in_specs=[vmem] * 4,
        out_specs=(hbm,) * 3,
        scratch_shapes=[
            pltpu.VMEM((rows, width), f32),
            pltpu.VMEM((rows, width), f32),
            dma((3,)),
        ],
        compiler_params=pltpu.CompilerParams(vmem_limit_bytes=16 << 20),
    )(*held)
    return height, resid, tend.reshape(state.shape)


def solution(mesh):
    return jax.shard_map(
        functools.partial(per_device, mesh.shape["lon"], mesh.shape["lat"]),
        mesh=mesh,
        in_specs=(P("lat", "lon"), P("lat", "lon"), P("lat", "lon"), P(None, None, "lat", "lon")),
        out_specs=(P("lat", "lon"), P("lat", "lon"), P(None, None, "lat", "lon")),
        check_vma=False,
    )
```

```python
import functools

import jax
import jax.numpy as jnp
from jax import lax
from jax.experimental import pallas as pl
from jax.experimental.pallas import tpu as pltpu
from jax.sharding import PartitionSpec as P

ITERS = 4
DAMPING = 0.05
VISCOSITY = 0.02
SUB = 8
MESH = pl.DeviceIdType.MESH


def east(a, b, lane):
    ra, rb = pltpu.roll(a, 127, 1), pltpu.roll(b, 127, 1)
    keep = lane < 127
    return jnp.where(keep, ra, rb), jnp.where(keep, rb, ra)


def west(a, b, lane):
    ra, rb = pltpu.roll(a, 1, 1), pltpu.roll(b, 1, 1)
    keep = lane > 0
    return jnp.where(keep, ra, rb), jnp.where(keep, rb, ra)


def north(x):
    return pltpu.roll(x, x.shape[0] - 1, 0)


def south(x):
    return pltpu.roll(x, 1, 0)


def exchange(
    sizes,
    forcing_ref, sea_ref, count_ref, state_ref,
    tend_ref, basis_ref, diag_ref, total_ref,
    force_buf, sea_buf, count_buf, q_ref, lap_ref, near_ref,
    pack_ref, side_ref, pair_ref, north_ref, south_ref,
    strip_own, strip_out, strip_in, corner_out, corner_in, center_ref, slap_ref,
    part_ref, all_in,
    meter_ref, load_sem, send_sem, one_sem, vert_sem, row_sem, corner_sem, ready_sem,
):
    n_lon, n_lat, fields, levels, rows = sizes
    planes = fields * levels
    depth_tiles = levels // SUB
    tiles = planes // SUB
    ilon, ilat = lax.axis_index("lon"), lax.axis_index("lat")
    has = {1: ilat < n_lat - 1, -1: ilat > 0}

    def at(dlon, dlat):
        return {
            "lon": lax.rem(ilon + dlon + n_lon, n_lon),
            "lat": lax.rem(ilat + dlat + n_lat, n_lat),
        }

    inputs = [
        pltpu.make_async_copy(src, dst, load_sem.at[0])
        for src, dst in ((forcing_ref, force_buf), (sea_ref, sea_buf), (count_ref, count_buf))
    ]
    for load in inputs:
        load.start()
    barrier = pltpu.get_barrier_semaphore()
    for dlat in (-1, 1):
        @pl.when(has[dlat])
        def _(dlat=dlat):
            for dlon in (-1, 1):
                pl.semaphore_signal(barrier, inc=1, device_id=at(dlon, dlat), device_id_type=MESH)
    for off in range(1, n_lat):
        pl.semaphore_signal(barrier, inc=1, device_id=at(0, off), device_id_type=MESH)
    for off in range(1, n_lon):
        pl.semaphore_signal(barrier, inc=1, device_id=at(off, 0), device_id_type=MESH)

    for j in range(rows):
        pltpu.make_async_copy(state_ref.at[:, j, :], q_ref.at[j + 2, pl.ds(0, planes)], load_sem.at[1]).start()

    def remote(src, dst, sent, sem, where):
        return pltpu.make_async_remote_copy(
            src_ref=src, dst_ref=dst, send_sem=send_sem.at[sent], recv_sem=sem,
            device_id=where, device_id_type=MESH,
        )

    def drained(ref, sem):
        pltpu.make_async_copy(ref, ref, sem).wait()

    lane8 = lax.broadcasted_iota(jnp.int32, (SUB, 128), 1)
    sub8 = lax.broadcasted_iota(jnp.int32, (SUB, 128), 0)
    kio = [(sub8 + SUB * t).astype(jnp.float32) for t in range(depth_tiles)]
    slot8 = lane8 % 4
    last_lane, first_lane = lane8 == 127, lane8 == 0
    own = pl.ds(planes, SUB)

    def tile(t):
        return pl.ds(SUB * t, SUB)

    sides = ((0, -1), (1, 1))
    for v, dlat in sides:
        @pl.when(jnp.logical_not(has[-dlat]))
        def _(v=v):
            if v == 0:
                north_ref[...] = jnp.zeros_like(north_ref)
            corner_in[v] = jnp.zeros_like(corner_in[v])
            for r in range(2):
                jj = rows + 2 + r if v == 0 else r
                q_ref[jj] = jnp.zeros_like(q_ref[jj])

    drained(meter_ref.at[pl.ds(0, 3 * rows)], load_sem.at[0])
    lane_r = lax.broadcasted_iota(jnp.int32, (rows, 128), 1)
    sea = sea_buf[...].astype(jnp.float32)
    wet = sea * count_buf[...].astype(jnp.float32)
    force = sea * force_buf[...]
    pair_ref[0] = force
    pair_ref[1] = wet
    inner_half = jnp.where(lane_r < 64, pltpu.roll(force, 32, 1), pltpu.roll(force, 96, 1))
    pack_ref[...] = jnp.where((lane_r >= 32) & (lane_r < 96), inner_half, wet)
    for j in range(rows):
        q_ref[j + 2, own, :] = jnp.broadcast_to(wet[j : j + 1], (SUB, 128))

    early = ilat < n_lat // 4

    def prepare():
        pltpu.make_async_copy(
            q_ref.at[pl.ds(2, rows), pl.ds(0, planes)], q_ref.at[pl.ds(2, rows), pl.ds(0, planes)], load_sem.at[1]
        ).wait()

        packed = [jnp.zeros((SUB, 128), jnp.float32)] * (tiles + 1)
        for j in range(rows):
            here = lane8 // 4 == j + 1
            level = q_ref[j + 2, own, :]
            active = [k < level for k in kio]
            for t in range(tiles + 1):
                if t < tiles:
                    q = jnp.where(active[t % depth_tiles], q_ref[j + 2, tile(t), :], 0.0)
                    q_ref[j + 2, tile(t), :] = q
                else:
                    q = level
                packed[t] = jnp.where(here, pltpu.roll(q, 4 * (j + 1) + 2, 1), packed[t])
        corners = [jnp.zeros((SUB, 128), jnp.float32)] * 2
        for t in range(tiles + 1):
            strip_own[tile(t), :] = packed[t]
            for v, j in ((0, 0), (1, rows - 1)):
                moved = pltpu.roll(packed[t], (4 * t - 4 * (j + 1)) % 128, 1)
                corners[v] = jnp.where(lane8 // 4 == t, moved, corners[v])
        for t in range(0, tiles + 1, 2):
            odd = packed[min(t + 1, tiles)]
            strip_out[0, tile(t // 2), :] = jnp.where(slot8 < 2, packed[t], pltpu.roll(odd, 2, 1))
            strip_out[1, tile(t // 2), :] = jnp.where(slot8 < 2, pltpu.roll(packed[t], 126, 1), odd)
        for v in range(2):
            corner_out[v] = corners[v]

    @pl.when(early)
    def _():
        prepare()

    diagonals = 2 * (has[1].astype(jnp.int32) + has[-1].astype(jnp.int32))
    pl.semaphore_wait(barrier, n_lon + n_lat - 2 + diagonals)

    for h, dlon in ((0, 1), (1, -1)):
        remote(pack_ref, side_ref.at[h], 2, one_sem.at[0], at(dlon, 0)).start()
    for v, dlat, start, vert in ((0, -1, 0, north_ref), (1, 1, rows - SUB, south_ref)):
        @pl.when(has[dlat])
        def _(v=v, dlat=dlat, start=start, vert=vert):
            part = pl.ds(start, vert.shape[1])
            for h, dlon in ((0, 1), (1, -1)):
                remote(pack_ref.at[part], vert.at[2 + h], v, vert_sem.at[v], at(dlon, dlat)).start()
            remote(pair_ref.at[:, part], vert.at[pl.ds(0, 2)], v, vert_sem.at[v], at(0, dlat)).start()

    for off in range(1, n_lat):
        pl.semaphore_signal(ready_sem, inc=1, device_id=at(0, off), device_id_type=MESH)

    @pl.when(jnp.logical_not(early))
    def _():
        prepare()

    for h, dlon in ((0, 1), (1, -1)):
        remote(strip_out.at[h], strip_in.at[h], 2, one_sem.at[1], at(dlon, 0)).start()
    for v, dlat in sides:
        @pl.when(has[dlat])
        def _(v=v, dlat=dlat):
            for h, dlon in ((0, 1), (1, -1)):
                remote(corner_out.at[v], corner_in.at[v, h], v, corner_sem.at[v], at(dlon, dlat)).start()

    late = ilat >= n_lat // 2

    def send_rows(now):
        for v, dlat in sides:
            @pl.when(jnp.logical_and(has[dlat], now))
            def _(v=v, dlat=dlat):
                mine = pl.ds(2, 2) if v == 0 else pl.ds(rows, 2)
                there = pl.ds(rows + 2, 2) if v == 0 else pl.ds(0, 2)
                remote(q_ref.at[mine], q_ref.at[there], v, row_sem.at[v], at(0, dlat)).start()

    send_rows(jnp.logical_not(late))

    def received(ref, sems, v, dlat):
        @pl.when(has[-dlat])
        def _():
            drained(ref, sems.at[v])

    lane_t = lax.broadcasted_iota(jnp.int32, (rows + 2 * SUB, 128), 1)
    row_t = lax.broadcasted_iota(jnp.int32, (rows + 2 * SUB, 128), 0)

    def krylov(parts, closed):
        from_west = jnp.concatenate([side_ref[0]] + [p[2] for p in parts], axis=0)
        from_east = jnp.concatenate([side_ref[1]] + [p[3] for p in parts], axis=0)
        low = lane_t < 64
        force_a = jnp.concatenate([pair_ref[0]] + [p[0] for p in parts], axis=0)
        wet_a = jnp.concatenate([pair_ref[1]] + [p[1] for p in parts], axis=0)
        wet_b = jnp.where(low, from_east, from_west)
        force_b = jnp.where(low, pltpu.roll(from_east, 96, 1), pltpu.roll(from_west, 32, 1))
        depth_a, depth_b = wet_a / levels, wet_b / levels
        da, db = east(depth_a, depth_b, lane_t)
        ea, eb = jnp.minimum(depth_a, da), jnp.minimum(depth_b, db)
        da, db = west(depth_a, depth_b, lane_t)
        wa, wb = jnp.minimum(depth_a, da), jnp.minimum(depth_b, db)
        na, nb = jnp.minimum(depth_a, north(depth_a)), jnp.minimum(depth_b, north(depth_b))
        sa, sb = south(na), south(nb)
        if closed:
            sa, sb = (jnp.where(row_t > 0, x, 0.0) for x in (sa, sb))
        diag_a = DAMPING + ea + wa + na + sa
        diag_b = DAMPING + eb + wb + nb + sb
        inv_a, inv_b = 1.0 / diag_a, 1.0 / diag_b
        va, vb = force_a * inv_a, force_b * inv_b
        ea, wa, na, sa = (c * inv_a for c in (ea, wa, na, sa))
        eb, wb, nb, sb = (c * inv_b for c in (eb, wb, nb, sb))
        basis = [va]
        for _ in range(ITERS):
            qe, qeb = east(va, vb, lane_t)
            qw, qwb = west(va, vb, lane_t)
            va, vb = (
                ea * qe + wa * qw + na * north(va) + sa * south(va),
                eb * qeb + wb * qwb + nb * north(vb) + sb * south(vb),
            )
            basis.append(va)
        return diag_a, basis

    def keep(diag, basis):
        diag_ref[...] = diag[:rows]
        for i, x in enumerate(basis):
            basis_ref[i] = x[:rows]

    margin = ITERS + 1
    drained(side_ref, one_sem.at[0])
    received(north_ref, vert_sem, 0, -1)
    diag, basis = krylov([north_ref], True)
    first = jnp.where(ilat > 0, margin, 0)
    counted = (row_t >= first) & (row_t < rows + margin)
    weight = jnp.where(counted, diag, 0.0)
    moments = []
    for m in range(2 * ITERS):
        moments.append(jnp.sum(weight * basis[m // 2] * basis[(m + 1) // 2], axis=0, keepdims=True))
    sums = jnp.broadcast_to(jnp.sum(jnp.concatenate(moments, axis=0), axis=1, keepdims=True), (2 * ITERS, 128))
    sums = jnp.where(lane8 // (128 // (2 * ITERS)) == sub8, sums, 0.0)
    part_ref[...] = jnp.sum(sums, axis=0, keepdims=True)
    pl.semaphore_wait(ready_sem, n_lat - 1)
    all_in[ilat * n_lon] = part_ref[...]
    for k in range(n_lat):
        for off in range(n_lon):
            def share(k=k, off=off):
                where = {"lon": lax.rem(ilon + off, n_lon), "lat": k}
                remote(part_ref, all_in.at[ilat * n_lon + off], 2, one_sem.at[2], where).start()

            if off:
                share()
            else:
                pl.when(ilat != k)(share)

    send_rows(late)

    @pl.when(ilat == 0)
    def _():
        keep(diag, basis)

    @pl.when(ilat > 0)
    def _():
        drained(south_ref, vert_sem.at[1])
        keep(*krylov([north_ref.at[:, pl.ds(0, SUB)], south_ref], False))

    drained(strip_in, one_sem.at[1])
    for v, dlat in sides:
        received(corner_in.at[v], corner_sem, v, dlat)

    def swap(x, step):
        return jnp.where(slot8 < 2, pltpu.roll(x, 128 - step, 1), pltpu.roll(x, step, 1))

    def arrange(t):
        west_pair, east_pair = strip_in[0, tile(t // 2), :], strip_in[1, tile(t // 2), :]
        if t % 2:
            west_pair = pltpu.roll(west_pair, 126, 1)
        else:
            east_pair = pltpu.roll(east_pair, 2, 1)
        g = jnp.where(slot8 < 2, west_pair, east_pair)
        for v, j in ((0, rows), (1, -1)):
            corner = jnp.where(slot8 < 2, corner_in[v, 0], corner_in[v, 1])
            moved = pltpu.roll(corner, (4 * (j + 1) - 4 * t) % 128, 1)
            g = jnp.where(lane8 // 4 == j + 1, moved, g)
        center = swap(g, 1)
        return center, strip_own[tile(t), :], swap(g, 2), pltpu.roll(center, 124, 1), pltpu.roll(center, 4, 1)

    ring = arrange(tiles)
    center_ref[tile(tiles), :] = ring[0]
    edge_coef = []
    for k in kio:
        count = sum(jnp.where(k < w, 1.0, 0.0) for w in ring[1:])
        first = jnp.where(k < ring[0], -VISCOSITY, 0.0)
        edge_coef.append((first, first * count))
    for t in range(tiles):
        center, a, b, c, d = arrange(t)
        center_ref[tile(t), :] = center
        first, second = edge_coef[t % depth_tiles]
        slap_ref[tile(t), :] = first * ((a + b) + (c + d)) - second * center

    def beside(x, edge):
        return (
            jnp.where(last_lane, edge, pltpu.roll(x, 127, 1)),
            jnp.where(first_lane, edge, pltpu.roll(x, 1, 1)),
        )

    def laplace(jj, inside):
        shift = 130 - 4 * jj

        def row_beside(x, where):
            return beside(x, pltpu.roll(center_ref[where, :], shift, 1))

        level = q_ref[jj, own, :]
        around = row_beside(level, own) + (q_ref[jj + 1, own, :], q_ref[jj - 1, own, :])
        for k in range(depth_tiles):
            here, oe, ow, on, os = (kio[k] < x for x in (level,) + around)
            ones = [jnp.where(x, 1.0, 0.0) for x in (oe, ow, on, os)]
            count = (ones[0] + ones[1]) + (ones[2] + ones[3])
            first = jnp.where(here, -VISCOSITY, 0.0)
            second = first * count

            def plane(f):
                at_tile = tile(f * depth_tiles + k)
                q = q_ref[jj, at_tile, :]
                qe, qw = row_beside(q, at_tile)
                qn, qs = q_ref[jj + 1, at_tile, :], q_ref[jj - 1, at_tile, :]
                lap_ref[jj - 1, at_tile, :] = first * ((qe + qw) + (qn + qs)) - second * q
                return q, qe, qw, qn, qs

            if not inside:
                for f in range(fields):
                    plane(f)
                continue
            near_ref[jj - 2, tile(k), :] = count
            quarter = jnp.where(here, 0.25, 0.0)
            planes_of = {2: plane(2), 3: plane(3)}
            u, ue, uw, _, _ = planes_of[2]
            v, _, _, vn, vs = planes_of[3]
            fe = jnp.where(oe, quarter * (u + ue), 0.0)
            fw = jnp.where(ow, quarter * (u + uw), 0.0)
            fn = jnp.where(on, quarter * (v + vn), 0.0)
            fs = jnp.where(os, quarter * (v + vs), 0.0)
            net = (fw - fe) + (fs - fn)
            for f in (2, 3, 0, 1):
                q, qe, qw, qn, qs = planes_of[f] if f in planes_of else plane(f)
                tend_ref[jj - 2, tile(f * depth_tiles + k), :] = (
                    net * q + (fw * qw - fe * qe) + (fs * qs - fn * qn)
                )

    def finish(j):
        shift = 122 - 4 * j
        level = q_ref[j + 2, own, :]
        for k in range(depth_tiles):
            here = kio[k] < level
            count = near_ref[j, tile(k), :]
            for f in range(fields):
                at_tile = tile(f * depth_tiles + k)
                lap = lap_ref[j + 1, at_tile, :]
                le, lw = beside(lap, pltpu.roll(slap_ref[at_tile, :], shift, 1))
                total = (le + lw) + (lap_ref[j + 2, at_tile, :] + lap_ref[j, at_tile, :])
                tend_ref[j, at_tile, :] += jnp.where(here, total, 0.0) - count * lap

    def ahead(i, carry):
        for r in range(2):
            laplace(2 * i + 3 + r, True)
        return carry

    lax.fori_loop(0, 3, ahead, 0)

    def both(i, carry):
        for r in range(4):
            finish(4 * i + 2 + r)
        for r in range(4):
            laplace(4 * i + 9 + r, True)
        return carry

    lax.fori_loop(0, rows // 4 - 2, both, 0)
    for j in range(rows - 6, rows - 2):
        finish(j)

    for v, dlat in sides:
        rim = q_ref.at[pl.ds(rows + 2, 2)] if v == 0 else q_ref.at[pl.ds(0, 2)]
        received(rim, row_sem, v, dlat)

    def rim(v, carry):
        laplace(1 + v * (rows + 1), False)
        laplace(2 + v * (rows - 1), True)
        for r in range(2):
            finish(v * (rows - 2) + r)
        return carry

    lax.fori_loop(0, 2, rim, 0)

    drained(all_in.at[pl.ds(0, n_lon * n_lat - 1)], one_sem.at[2])
    terms = [all_in[i] for i in range(n_lon * n_lat)]
    while len(terms) > 1:
        terms = [a + b for a, b in zip(terms[::2], terms[1::2])] + terms[len(terms) - len(terms) % 2 :]
    total = terms[0]
    total_ref[...] = jnp.broadcast_to(total, total_ref.shape)

    half = strip_out.shape[1]
    drained(meter_ref.at[pl.ds(0, 2 * rows + 2 * half + n_lon * n_lat - 1)], send_sem.at[2])
    for v, dlat in sides:
        @pl.when(has[dlat])
        def _(v=v):
            vert = (north_ref, south_ref)[v].shape[1]
            drained(meter_ref.at[pl.ds(0, 4 * vert + 2 * SUB + 2 * (planes + SUB))], send_sem.at[v])


def deliver(tend_in, basis_in, diag_in, total_in, height_ref, resid_ref, tend_ref, height_buf, resid_buf, sem):
    rows = tend_in.shape[0]
    stores = [pltpu.make_async_copy(tend_in.at[j], tend_ref.at[:, j, :], sem.at[0]) for j in range(rows)]
    for store in stores:
        store.start()
    part = 128 // (2 * ITERS)
    shape = (2 * ITERS, 128)
    mine = lax.broadcasted_iota(jnp.int32, shape, 1) == part * lax.broadcasted_iota(jnp.int32, shape, 0)
    total = jnp.broadcast_to(jnp.sum(jnp.where(mine, total_in[...], 0.0), axis=1, keepdims=True), shape)
    mu = [total[m : m + 1] for m in range(2 * ITERS)]

    def inner(x, y):
        sums = [None] * (len(x) + len(y) - 1)
        for i, xi in enumerate(x):
            for j, yj in enumerate(y):
                sums[i + j] = xi * yj if sums[i + j] is None else sums[i + j] + xi * yj
        out = sums[0] * mu[0]
        for m in range(1, len(sums)):
            out = out + sums[m] * mu[m]
        return out

    one = jnp.ones((1, 128), jnp.float32)
    zero = jnp.zeros((1, 128), jnp.float32)
    z, p, h = [one], [one], []
    rz = mu[0]
    for it in range(ITERS):
        image = [hi - lo for hi, lo in zip(p + [zero], [zero] + p)]
        alpha = rz / inner(p, image)
        h = [x + alpha * y for x, y in zip(h + [zero], p)]
        z = [x - alpha * y for x, y in zip(z + [zero], image)]
        if it + 1 < ITERS:
            new = inner(z, z)
            beta = new / rz
            p = [x + beta * y for x, y in zip(z, p + [zero])]
            rz = new
    height = h[0] * basis_in[0]
    for i in range(1, ITERS):
        height = height + h[i] * basis_in[i]
    resid = z[0] * basis_in[0]
    for i in range(1, ITERS + 1):
        resid = resid + z[i] * basis_in[i]
    height_buf[...] = height
    resid_buf[...] = diag_in[...] * resid
    last = [
        pltpu.make_async_copy(height_buf, height_ref, sem.at[1]),
        pltpu.make_async_copy(resid_buf, resid_ref, sem.at[2]),
    ]
    for store in last:
        store.start()
    pltpu.make_async_copy(tend_in, tend_in, sem.at[0]).wait()
    for store in last:
        store.wait()


def per_device(n_lon, n_lat, forcing, sea, count, state):
    fields, levels, rows, width = state.shape
    planes = fields * levels
    tall = planes + SUB
    half = SUB * ((tall // SUB + 1) // 2)
    assert levels % SUB == 0 and width == 128 and rows % SUB == 0 and rows >= 2 * SUB and 2 * (ITERS + 1) <= 2 * SUB
    assert 4 * (rows + 2) <= width and 4 * (planes // SUB + 1) <= width
    sizes = (n_lon, n_lat, fields, levels, rows)
    f32 = jnp.float32
    vmem = pl.BlockSpec(memory_space=pltpu.VMEM)
    hbm = pl.BlockSpec(memory_space=pltpu.HBM)
    dma = pltpu.SemaphoreType.DMA
    held = pl.pallas_call(
        functools.partial(exchange, sizes),
        out_shape=(
            pltpu.VMEM((rows, planes, width), f32),
            pltpu.VMEM((ITERS + 1, rows, width), f32),
            pltpu.VMEM((rows, width), f32),
            pltpu.VMEM((2 * ITERS, width), f32),
        ),
        in_specs=[hbm] * 4,
        out_specs=(vmem,) * 4,
        scratch_shapes=[
            pltpu.VMEM((rows, width), f32),
            pltpu.VMEM((rows, width), jnp.int32),
            pltpu.VMEM((rows, width), jnp.int32),
            pltpu.VMEM((rows + 4, tall, width), f32),
            pltpu.VMEM((rows + 2, planes, width), f32),
            pltpu.VMEM((rows, levels, width), f32),
            pltpu.VMEM((rows, width), f32),
            pltpu.VMEM((2, rows, width), f32),
            pltpu.VMEM((2, rows, width), f32),
            pltpu.VMEM((4, 2 * SUB, width), f32),
            pltpu.VMEM((4, SUB, width), f32),
            pltpu.VMEM((tall, width), f32),
            pltpu.VMEM((2, half, width), f32),
            pltpu.VMEM((2, half, width), f32),
            pltpu.VMEM((2, SUB, width), f32),
            pltpu.VMEM((2, 2, SUB, width), f32),
            pltpu.VMEM((tall, width), f32),
            pltpu.VMEM((planes, width), f32),
            pltpu.VMEM((1, width), f32),
            pltpu.VMEM((n_lon * n_lat, 1, width), f32),
            pltpu.VMEM((max(10 * SUB + 2 * tall, 2 * rows + 2 * half + n_lon * n_lat), 1, width), f32),
            dma((2,)),
            dma((3,)),
            dma((3,)),
            dma((2,)),
            dma((2,)),
            dma((2,)),
            pltpu.SemaphoreType.REGULAR,
        ],
        compiler_params=pltpu.CompilerParams(collective_id=0, has_side_effects=True),
    )(forcing, sea, count, state.reshape(planes, rows, width))
    small = jax.ShapeDtypeStruct((rows, width), f32)
    height, resid, tend = pl.pallas_call(
        deliver,
        out_shape=(small, small, jax.ShapeDtypeStruct((planes, rows, width), f32)),
        in_specs=[vmem] * 4,
        out_specs=(hbm,) * 3,
        scratch_shapes=[
            pltpu.VMEM((rows, width), f32),
            pltpu.VMEM((rows, width), f32),
            dma((3,)),
        ],
        compiler_params=pltpu.CompilerParams(vmem_limit_bytes=16 << 20),
    )(*held)
    return height, resid, tend.reshape(state.shape)


def solution(mesh):
    return jax.shard_map(
        functools.partial(per_device, mesh.shape["lon"], mesh.shape["lat"]),
        mesh=mesh,
        in_specs=(P("lat", "lon"), P("lat", "lon"), P("lat", "lon"), P(None, None, "lat", "lon")),
        out_specs=(P("lat", "lon"), P("lat", "lon"), P(None, None, "lat", "lon")),
        check_vma=False,
    )
```

```python
import functools

import jax
import jax.numpy as jnp
from jax import lax
from jax.experimental import pallas as pl
from jax.experimental.pallas import tpu as pltpu
from jax.sharding import PartitionSpec as P

ITERS = 4
DAMPING = 0.05
VISCOSITY = 0.02
SUB = 8
MESH = pl.DeviceIdType.MESH


def east(a, b, lane):
    ra, rb = pltpu.roll(a, 127, 1), pltpu.roll(b, 127, 1)
    keep = lane < 127
    return jnp.where(keep, ra, rb), jnp.where(keep, rb, ra)


def west(a, b, lane):
    ra, rb = pltpu.roll(a, 1, 1), pltpu.roll(b, 1, 1)
    keep = lane > 0
    return jnp.where(keep, ra, rb), jnp.where(keep, rb, ra)


def north(x):
    return pltpu.roll(x, x.shape[0] - 1, 0)


def south(x):
    return pltpu.roll(x, 1, 0)


def exchange(
    sizes,
    forcing_ref, sea_ref, count_ref, state_ref,
    tend_ref, basis_ref, diag_ref, total_ref,
    force_buf, sea_buf, count_buf, q_ref, lap_ref, near_ref,
    pack_ref, side_ref, pair_ref, north_ref, south_ref,
    strip_own, strip_out, strip_in, corner_out, corner_in, center_ref, slap_ref,
    part_ref, all_in,
    meter_ref, load_sem, send_sem, one_sem, vert_sem, row_sem, corner_sem, ready_sem,
):
    n_lon, n_lat, fields, levels, rows = sizes
    planes = fields * levels
    depth_tiles = levels // SUB
    tiles = planes // SUB
    ilon, ilat = lax.axis_index("lon"), lax.axis_index("lat")
    has = {1: ilat < n_lat - 1, -1: ilat > 0}

    def at(dlon, dlat):
        return {
            "lon": lax.rem(ilon + dlon + n_lon, n_lon),
            "lat": lax.rem(ilat + dlat + n_lat, n_lat),
        }

    inputs = [
        pltpu.make_async_copy(src, dst, load_sem.at[0])
        for src, dst in ((forcing_ref, force_buf), (sea_ref, sea_buf), (count_ref, count_buf))
    ]
    for load in inputs:
        load.start()
    barrier = pltpu.get_barrier_semaphore()
    for dlat in (-1, 1):
        @pl.when(has[dlat])
        def _(dlat=dlat):
            for dlon in (-1, 1):
                pl.semaphore_signal(barrier, inc=1, device_id=at(dlon, dlat), device_id_type=MESH)
    for off in range(1, n_lat):
        pl.semaphore_signal(barrier, inc=1, device_id=at(0, off), device_id_type=MESH)
    for off in range(1, n_lon):
        pl.semaphore_signal(barrier, inc=1, device_id=at(off, 0), device_id_type=MESH)

    for j in range(rows):
        pltpu.make_async_copy(state_ref.at[:, j, :], q_ref.at[j + 2, pl.ds(0, planes)], load_sem.at[1]).start()

    def remote(src, dst, sent, sem, where):
        return pltpu.make_async_remote_copy(
            src_ref=src, dst_ref=dst, send_sem=send_sem.at[sent], recv_sem=sem,
            device_id=where, device_id_type=MESH,
        )

    def drained(ref, sem):
        pltpu.make_async_copy(ref, ref, sem).wait()

    lane8 = lax.broadcasted_iota(jnp.int32, (SUB, 128), 1)
    sub8 = lax.broadcasted_iota(jnp.int32, (SUB, 128), 0)
    kio = [(sub8 + SUB * t).astype(jnp.float32) for t in range(depth_tiles)]
    slot8 = lane8 % 4
    last_lane, first_lane = lane8 == 127, lane8 == 0
    own = pl.ds(planes, SUB)

    def tile(t):
        return pl.ds(SUB * t, SUB)

    sides = ((0, -1), (1, 1))
    for v, dlat in sides:
        @pl.when(jnp.logical_not(has[-dlat]))
        def _(v=v):
            if v == 0:
                north_ref[...] = jnp.zeros_like(north_ref)
            corner_in[v] = jnp.zeros_like(corner_in[v])
            for r in range(2):
                jj = rows + 2 + r if v == 0 else r
                q_ref[jj] = jnp.zeros_like(q_ref[jj])

    drained(meter_ref.at[pl.ds(0, 3 * rows)], load_sem.at[0])
    lane_r = lax.broadcasted_iota(jnp.int32, (rows, 128), 1)
    sea = sea_buf[...].astype(jnp.float32)
    wet = sea * count_buf[...].astype(jnp.float32)
    force = sea * force_buf[...]
    pair_ref[0] = force
    pair_ref[1] = wet
    inner_half = jnp.where(lane_r < 64, pltpu.roll(force, 32, 1), pltpu.roll(force, 96, 1))
    pack_ref[...] = jnp.where((lane_r >= 32) & (lane_r < 96), inner_half, wet)
    for j in range(rows):
        q_ref[j + 2, own, :] = jnp.broadcast_to(wet[j : j + 1], (SUB, 128))

    early = ilat < n_lat // 4

    def prepare():
        pltpu.make_async_copy(
            q_ref.at[pl.ds(2, rows), pl.ds(0, planes)], q_ref.at[pl.ds(2, rows), pl.ds(0, planes)], load_sem.at[1]
        ).wait()

        packed = [jnp.zeros((SUB, 128), jnp.float32)] * (tiles + 1)
        for j in range(rows):
            here = lane8 // 4 == j + 1
            level = q_ref[j + 2, own, :]
            active = [k < level for k in kio]
            for t in range(tiles + 1):
                if t < tiles:
                    q = jnp.where(active[t % depth_tiles], q_ref[j + 2, tile(t), :], 0.0)
                    q_ref[j + 2, tile(t), :] = q
                else:
                    q = level
                packed[t] = jnp.where(here, pltpu.roll(q, 4 * (j + 1) + 2, 1), packed[t])
        corners = [jnp.zeros((SUB, 128), jnp.float32)] * 2
        for t in range(tiles + 1):
            strip_own[tile(t), :] = packed[t]
            for v, j in ((0, 0), (1, rows - 1)):
                moved = pltpu.roll(packed[t], (4 * t - 4 * (j + 1)) % 128, 1)
                corners[v] = jnp.where(lane8 // 4 == t, moved, corners[v])
        for t in range(0, tiles + 1, 2):
            odd = packed[min(t + 1, tiles)]
            strip_out[0, tile(t // 2), :] = jnp.where(slot8 < 2, packed[t], pltpu.roll(odd, 2, 1))
            strip_out[1, tile(t // 2), :] = jnp.where(slot8 < 2, pltpu.roll(packed[t], 126, 1), odd)
        for v in range(2):
            corner_out[v] = corners[v]

    @pl.when(early)
    def _():
        prepare()

    diagonals = 2 * (has[1].astype(jnp.int32) + has[-1].astype(jnp.int32))
    pl.semaphore_wait(barrier, n_lon + n_lat - 2 + diagonals)

    for h, dlon in ((0, 1), (1, -1)):
        remote(pack_ref, side_ref.at[h], 2, one_sem.at[0], at(dlon, 0)).start()
    for v, dlat, start, vert in ((0, -1, 0, north_ref), (1, 1, rows - SUB, south_ref)):
        @pl.when(has[dlat])
        def _(v=v, dlat=dlat, start=start, vert=vert):
            part = pl.ds(start, vert.shape[1])
            for h, dlon in ((0, 1), (1, -1)):
                remote(pack_ref.at[part], vert.at[2 + h], v, vert_sem.at[v], at(dlon, dlat)).start()
            remote(pair_ref.at[:, part], vert.at[pl.ds(0, 2)], v, vert_sem.at[v], at(0, dlat)).start()

    for off in range(1, n_lat):
        pl.semaphore_signal(ready_sem, inc=1, device_id=at(0, off), device_id_type=MESH)

    @pl.when(jnp.logical_not(early))
    def _():
        prepare()

    for h, dlon in ((0, 1), (1, -1)):
        remote(strip_out.at[h], strip_in.at[h], 2, one_sem.at[1], at(dlon, 0)).start()
    for v, dlat in sides:
        @pl.when(has[dlat])
        def _(v=v, dlat=dlat):
            for h, dlon in ((0, 1), (1, -1)):
                remote(corner_out.at[v], corner_in.at[v, h], v, corner_sem.at[v], at(dlon, dlat)).start()

    late = ilat >= n_lat - n_lat // 4

    def send_rows(now):
        for v, dlat in sides:
            @pl.when(jnp.logical_and(has[dlat], now))
            def _(v=v, dlat=dlat):
                mine = pl.ds(2, 2) if v == 0 else pl.ds(rows, 2)
                there = pl.ds(rows + 2, 2) if v == 0 else pl.ds(0, 2)
                remote(q_ref.at[mine], q_ref.at[there], v, row_sem.at[v], at(0, dlat)).start()

    send_rows(jnp.logical_not(late))

    def received(ref, sems, v, dlat):
        @pl.when(has[-dlat])
        def _():
            drained(ref, sems.at[v])

    lane_t = lax.broadcasted_iota(jnp.int32, (rows + 2 * SUB, 128), 1)
    row_t = lax.broadcasted_iota(jnp.int32, (rows + 2 * SUB, 128), 0)

    def krylov(parts, closed):
        from_west = jnp.concatenate([side_ref[0]] + [p[2] for p in parts], axis=0)
        from_east = jnp.concatenate([side_ref[1]] + [p[3] for p in parts], axis=0)
        low = lane_t < 64
        force_a = jnp.concatenate([pair_ref[0]] + [p[0] for p in parts], axis=0)
        wet_a = jnp.concatenate([pair_ref[1]] + [p[1] for p in parts], axis=0)
        wet_b = jnp.where(low, from_east, from_west)
        force_b = jnp.where(low, pltpu.roll(from_east, 96, 1), pltpu.roll(from_west, 32, 1))
        depth_a, depth_b = wet_a / levels, wet_b / levels
        da, db = east(depth_a, depth_b, lane_t)
        ea, eb = jnp.minimum(depth_a, da), jnp.minimum(depth_b, db)
        da, db = west(depth_a, depth_b, lane_t)
        wa, wb = jnp.minimum(depth_a, da), jnp.minimum(depth_b, db)
        na, nb = jnp.minimum(depth_a, north(depth_a)), jnp.minimum(depth_b, north(depth_b))
        sa, sb = south(na), south(nb)
        if closed:
            sa, sb = (jnp.where(row_t > 0, x, 0.0) for x in (sa, sb))
        diag_a = DAMPING + ea + wa + na + sa
        diag_b = DAMPING + eb + wb + nb + sb
        inv_a, inv_b = 1.0 / diag_a, 1.0 / diag_b
        va, vb = force_a * inv_a, force_b * inv_b
        ea, wa, na, sa = (c * inv_a for c in (ea, wa, na, sa))
        eb, wb, nb, sb = (c * inv_b for c in (eb, wb, nb, sb))
        basis = [va]
        for _ in range(ITERS):
            qe, qeb = east(va, vb, lane_t)
            qw, qwb = west(va, vb, lane_t)
            va, vb = (
                ea * qe + wa * qw + na * north(va) + sa * south(va),
                eb * qeb + wb * qwb + nb * north(vb) + sb * south(vb),
            )
            basis.append(va)
        return diag_a, basis

    def keep(diag, basis):
        diag_ref[...] = diag[:rows]
        for i, x in enumerate(basis):
            basis_ref[i] = x[:rows]

    margin = ITERS + 1
    drained(side_ref, one_sem.at[0])
    received(north_ref, vert_sem, 0, -1)
    diag, basis = krylov([north_ref], True)
    first = jnp.where(ilat > 0, margin, 0)
    counted = (row_t >= first) & (row_t < rows + margin)
    weight = jnp.where(counted, diag, 0.0)
    moments = []
    for m in range(2 * ITERS):
        moments.append(jnp.sum(weight * basis[m // 2] * basis[(m + 1) // 2], axis=0, keepdims=True))
    sums = jnp.broadcast_to(jnp.sum(jnp.concatenate(moments, axis=0), axis=1, keepdims=True), (2 * ITERS, 128))
    sums = jnp.where(lane8 // (128 // (2 * ITERS)) == sub8, sums, 0.0)
    part_ref[...] = jnp.sum(sums, axis=0, keepdims=True)
    pl.semaphore_wait(ready_sem, n_lat - 1)
    all_in[ilat * n_lon] = part_ref[...]
    for k in range(n_lat):
        for off in range(n_lon):
            def share(k=k, off=off):
                where = {"lon": lax.rem(ilon + off, n_lon), "lat": k}
                remote(part_ref, all_in.at[ilat * n_lon + off], 2, one_sem.at[2], where).start()

            if off:
                share()
            else:
                pl.when(ilat != k)(share)

    send_rows(late)

    @pl.when(ilat == 0)
    def _():
        keep(diag, basis)

    @pl.when(ilat > 0)
    def _():
        drained(south_ref, vert_sem.at[1])
        keep(*krylov([north_ref.at[:, pl.ds(0, SUB)], south_ref], False))

    drained(strip_in, one_sem.at[1])
    for v, dlat in sides:
        received(corner_in.at[v], corner_sem, v, dlat)

    def swap(x, step):
        return jnp.where(slot8 < 2, pltpu.roll(x, 128 - step, 1), pltpu.roll(x, step, 1))

    def arrange(t):
        west_pair, east_pair = strip_in[0, tile(t // 2), :], strip_in[1, tile(t // 2), :]
        if t % 2:
            west_pair = pltpu.roll(west_pair, 126, 1)
        else:
            east_pair = pltpu.roll(east_pair, 2, 1)
        g = jnp.where(slot8 < 2, west_pair, east_pair)
        for v, j in ((0, rows), (1, -1)):
            corner = jnp.where(slot8 < 2, corner_in[v, 0], corner_in[v, 1])
            moved = pltpu.roll(corner, (4 * (j + 1) - 4 * t) % 128, 1)
            g = jnp.where(lane8 // 4 == j + 1, moved, g)
        center = swap(g, 1)
        return center, strip_own[tile(t), :], swap(g, 2), pltpu.roll(center, 124, 1), pltpu.roll(center, 4, 1)

    ring = arrange(tiles)
    center_ref[tile(tiles), :] = ring[0]
    edge_coef = []
    for k in kio:
        count = sum(jnp.where(k < w, 1.0, 0.0) for w in ring[1:])
        first = jnp.where(k < ring[0], -VISCOSITY, 0.0)
        edge_coef.append((first, first * count))
    for t in range(tiles):
        center, a, b, c, d = arrange(t)
        center_ref[tile(t), :] = center
        first, second = edge_coef[t % depth_tiles]
        slap_ref[tile(t), :] = first * ((a + b) + (c + d)) - second * center

    def beside(x, edge):
        return (
            jnp.where(last_lane, edge, pltpu.roll(x, 127, 1)),
            jnp.where(first_lane, edge, pltpu.roll(x, 1, 1)),
        )

    def laplace(jj, inside):
        shift = 130 - 4 * jj

        def row_beside(x, where):
            return beside(x, pltpu.roll(center_ref[where, :], shift, 1))

        level = q_ref[jj, own, :]
        around = row_beside(level, own) + (q_ref[jj + 1, own, :], q_ref[jj - 1, own, :])
        for k in range(depth_tiles):
            here, oe, ow, on, os = (kio[k] < x for x in (level,) + around)
            ones = [jnp.where(x, 1.0, 0.0) for x in (oe, ow, on, os)]
            count = (ones[0] + ones[1]) + (ones[2] + ones[3])
            first = jnp.where(here, -VISCOSITY, 0.0)
            second = first * count

            def plane(f):
                at_tile = tile(f * depth_tiles + k)
                q = q_ref[jj, at_tile, :]
                qe, qw = row_beside(q, at_tile)
                qn, qs = q_ref[jj + 1, at_tile, :], q_ref[jj - 1, at_tile, :]
                lap_ref[jj - 1, at_tile, :] = first * ((qe + qw) + (qn + qs)) - second * q
                return q, qe, qw, qn, qs

            if not inside:
                for f in range(fields):
                    plane(f)
                continue
            near_ref[jj - 2, tile(k), :] = count
            quarter = jnp.where(here, 0.25, 0.0)
            planes_of = {2: plane(2), 3: plane(3)}
            u, ue, uw, _, _ = planes_of[2]
            v, _, _, vn, vs = planes_of[3]
            fe = jnp.where(oe, quarter * (u + ue), 0.0)
            fw = jnp.where(ow, quarter * (u + uw), 0.0)
            fn = jnp.where(on, quarter * (v + vn), 0.0)
            fs = jnp.where(os, quarter * (v + vs), 0.0)
            net = (fw - fe) + (fs - fn)
            for f in (2, 3, 0, 1):
                q, qe, qw, qn, qs = planes_of[f] if f in planes_of else plane(f)
                tend_ref[jj - 2, tile(f * depth_tiles + k), :] = (
                    net * q + (fw * qw - fe * qe) + (fs * qs - fn * qn)
                )

    def finish(j):
        shift = 122 - 4 * j
        level = q_ref[j + 2, own, :]
        for k in range(depth_tiles):
            here = kio[k] < level
            count = near_ref[j, tile(k), :]
            for f in range(fields):
                at_tile = tile(f * depth_tiles + k)
                lap = lap_ref[j + 1, at_tile, :]
                le, lw = beside(lap, pltpu.roll(slap_ref[at_tile, :], shift, 1))
                total = (le + lw) + (lap_ref[j + 2, at_tile, :] + lap_ref[j, at_tile, :])
                tend_ref[j, at_tile, :] += jnp.where(here, total, 0.0) - count * lap

    def ahead(i, carry):
        for r in range(2):
            laplace(2 * i + 3 + r, True)
        return carry

    lax.fori_loop(0, 3, ahead, 0)

    def both(i, carry):
        for r in range(4):
            finish(4 * i + 2 + r)
        for r in range(4):
            laplace(4 * i + 9 + r, True)
        return carry

    lax.fori_loop(0, rows // 4 - 2, both, 0)
    for j in range(rows - 6, rows - 2):
        finish(j)

    for v, dlat in sides:
        rim = q_ref.at[pl.ds(rows + 2, 2)] if v == 0 else q_ref.at[pl.ds(0, 2)]
        received(rim, row_sem, v, dlat)

    def rim(_, carry):
        for jj, inside in ((1, False), (2, True), (rows + 1, True), (rows + 2, False)):
            laplace(jj, inside)
        for j in (0, 1, rows - 2, rows - 1):
            finish(j)
        return carry

    lax.fori_loop(0, jnp.minimum(ilat + 1, 1), rim, 0)

    drained(all_in.at[pl.ds(0, n_lon * n_lat - 1)], one_sem.at[2])
    terms = [all_in[i] for i in range(n_lon * n_lat)]
    while len(terms) > 1:
        terms = [a + b for a, b in zip(terms[::2], terms[1::2])] + terms[len(terms) - len(terms) % 2 :]
    total = terms[0]
    total_ref[...] = jnp.broadcast_to(total, total_ref.shape)

    half = strip_out.shape[1]
    drained(meter_ref.at[pl.ds(0, 2 * rows + 2 * half + n_lon * n_lat - 1)], send_sem.at[2])
    for v, dlat in sides:
        @pl.when(has[dlat])
        def _(v=v):
            vert = (north_ref, south_ref)[v].shape[1]
            drained(meter_ref.at[pl.ds(0, 4 * vert + 2 * SUB + 2 * (planes + SUB))], send_sem.at[v])


def deliver(tend_in, basis_in, diag_in, total_in, height_ref, resid_ref, tend_ref, height_buf, resid_buf, sem):
    rows = tend_in.shape[0]
    stores = [pltpu.make_async_copy(tend_in.at[j], tend_ref.at[:, j, :], sem.at[0]) for j in range(rows)]
    for store in stores:
        store.start()
    part = 128 // (2 * ITERS)
    shape = (2 * ITERS, 128)
    mine = lax.broadcasted_iota(jnp.int32, shape, 1) == part * lax.broadcasted_iota(jnp.int32, shape, 0)
    total = jnp.broadcast_to(jnp.sum(jnp.where(mine, total_in[...], 0.0), axis=1, keepdims=True), shape)
    mu = [total[m : m + 1] for m in range(2 * ITERS)]

    def inner(x, y):
        sums = [None] * (len(x) + len(y) - 1)
        for i, xi in enumerate(x):
            for j, yj in enumerate(y):
                sums[i + j] = xi * yj if sums[i + j] is None else sums[i + j] + xi * yj
        out = sums[0] * mu[0]
        for m in range(1, len(sums)):
            out = out + sums[m] * mu[m]
        return out

    one = jnp.ones((1, 128), jnp.float32)
    zero = jnp.zeros((1, 128), jnp.float32)
    z, p, h = [one], [one], []
    rz = mu[0]
    for it in range(ITERS):
        image = [hi - lo for hi, lo in zip(p + [zero], [zero] + p)]
        alpha = rz / inner(p, image)
        h = [x + alpha * y for x, y in zip(h + [zero], p)]
        z = [x - alpha * y for x, y in zip(z + [zero], image)]
        if it + 1 < ITERS:
            new = inner(z, z)
            beta = new / rz
            p = [x + beta * y for x, y in zip(z, p + [zero])]
            rz = new
    height = h[0] * basis_in[0]
    for i in range(1, ITERS):
        height = height + h[i] * basis_in[i]
    resid = z[0] * basis_in[0]
    for i in range(1, ITERS + 1):
        resid = resid + z[i] * basis_in[i]
    height_buf[...] = height
    resid_buf[...] = diag_in[...] * resid
    last = [
        pltpu.make_async_copy(height_buf, height_ref, sem.at[1]),
        pltpu.make_async_copy(resid_buf, resid_ref, sem.at[2]),
    ]
    for store in last:
        store.start()
    pltpu.make_async_copy(tend_in, tend_in, sem.at[0]).wait()
    for store in last:
        store.wait()


def per_device(n_lon, n_lat, forcing, sea, count, state):
    fields, levels, rows, width = state.shape
    planes = fields * levels
    tall = planes + SUB
    half = SUB * ((tall // SUB + 1) // 2)
    assert levels % SUB == 0 and width == 128 and rows % SUB == 0 and rows >= 2 * SUB and 2 * (ITERS + 1) <= 2 * SUB
    assert 4 * (rows + 2) <= width and 4 * (planes // SUB + 1) <= width
    sizes = (n_lon, n_lat, fields, levels, rows)
    f32 = jnp.float32
    vmem = pl.BlockSpec(memory_space=pltpu.VMEM)
    hbm = pl.BlockSpec(memory_space=pltpu.HBM)
    dma = pltpu.SemaphoreType.DMA
    held = pl.pallas_call(
        functools.partial(exchange, sizes),
        out_shape=(
            pltpu.VMEM((rows, planes, width), f32),
            pltpu.VMEM((ITERS + 1, rows, width), f32),
            pltpu.VMEM((rows, width), f32),
            pltpu.VMEM((2 * ITERS, width), f32),
        ),
        in_specs=[hbm] * 4,
        out_specs=(vmem,) * 4,
        scratch_shapes=[
            pltpu.VMEM((rows, width), f32),
            pltpu.VMEM((rows, width), jnp.int32),
            pltpu.VMEM((rows, width), jnp.int32),
            pltpu.VMEM((rows + 4, tall, width), f32),
            pltpu.VMEM((rows + 2, planes, width), f32),
            pltpu.VMEM((rows, levels, width), f32),
            pltpu.VMEM((rows, width), f32),
            pltpu.VMEM((2, rows, width), f32),
            pltpu.VMEM((2, rows, width), f32),
            pltpu.VMEM((4, 2 * SUB, width), f32),
            pltpu.VMEM((4, SUB, width), f32),
            pltpu.VMEM((tall, width), f32),
            pltpu.VMEM((2, half, width), f32),
            pltpu.VMEM((2, half, width), f32),
            pltpu.VMEM((2, SUB, width), f32),
            pltpu.VMEM((2, 2, SUB, width), f32),
            pltpu.VMEM((tall, width), f32),
            pltpu.VMEM((planes, width), f32),
            pltpu.VMEM((1, width), f32),
            pltpu.VMEM((n_lon * n_lat, 1, width), f32),
            pltpu.VMEM((max(10 * SUB + 2 * tall, 2 * rows + 2 * half + n_lon * n_lat), 1, width), f32),
            dma((2,)),
            dma((3,)),
            dma((3,)),
            dma((2,)),
            dma((2,)),
            dma((2,)),
            pltpu.SemaphoreType.REGULAR,
        ],
        compiler_params=pltpu.CompilerParams(collective_id=0, has_side_effects=True),
    )(forcing, sea, count, state.reshape(planes, rows, width))
    small = jax.ShapeDtypeStruct((rows, width), f32)
    height, resid, tend = pl.pallas_call(
        deliver,
        out_shape=(small, small, jax.ShapeDtypeStruct((planes, rows, width), f32)),
        in_specs=[vmem] * 4,
        out_specs=(hbm,) * 3,
        scratch_shapes=[
            pltpu.VMEM((rows, width), f32),
            pltpu.VMEM((rows, width), f32),
            dma((3,)),
        ],
        compiler_params=pltpu.CompilerParams(vmem_limit_bytes=16 << 20),
    )(*held)
    return height, resid, tend.reshape(state.shape)


def solution(mesh):
    return jax.shard_map(
        functools.partial(per_device, mesh.shape["lon"], mesh.shape["lat"]),
        mesh=mesh,
        in_specs=(P("lat", "lon"), P("lat", "lon"), P("lat", "lon"), P(None, None, "lat", "lon")),
        out_specs=(P("lat", "lon"), P("lat", "lon"), P(None, None, "lat", "lon")),
        check_vma=False,
    )
```

```python
import functools

import jax
import jax.numpy as jnp
from jax import lax
from jax.experimental import pallas as pl
from jax.experimental.pallas import tpu as pltpu
from jax.sharding import PartitionSpec as P

ITERS = 4
DAMPING = 0.05
VISCOSITY = 0.02
SUB = 8
MESH = pl.DeviceIdType.MESH


def east(a, b, lane):
    ra, rb = pltpu.roll(a, 127, 1), pltpu.roll(b, 127, 1)
    keep = lane < 127
    return jnp.where(keep, ra, rb), jnp.where(keep, rb, ra)


def west(a, b, lane):
    ra, rb = pltpu.roll(a, 1, 1), pltpu.roll(b, 1, 1)
    keep = lane > 0
    return jnp.where(keep, ra, rb), jnp.where(keep, rb, ra)


def north(x):
    return pltpu.roll(x, x.shape[0] - 1, 0)


def south(x):
    return pltpu.roll(x, 1, 0)


def exchange(
    sizes,
    forcing_ref, sea_ref, count_ref, state_ref,
    tend_ref, basis_ref, diag_ref, total_ref,
    force_buf, sea_buf, count_buf, q_ref, lap_ref, near_ref,
    pack_ref, side_ref, pair_ref, north_ref, south_ref,
    strip_own, strip_out, strip_in, corner_out, corner_in, center_ref, slap_ref,
    part_ref, all_in,
    meter_ref, load_sem, send_sem, one_sem, vert_sem, row_sem, corner_sem, ready_sem,
):
    n_lon, n_lat, fields, levels, rows = sizes
    planes = fields * levels
    depth_tiles = levels // SUB
    tiles = planes // SUB
    ilon, ilat = lax.axis_index("lon"), lax.axis_index("lat")
    has = {1: ilat < n_lat - 1, -1: ilat > 0}

    def at(dlon, dlat):
        return {
            "lon": lax.rem(ilon + dlon + n_lon, n_lon),
            "lat": lax.rem(ilat + dlat + n_lat, n_lat),
        }

    inputs = [
        pltpu.make_async_copy(src, dst, load_sem.at[0])
        for src, dst in ((forcing_ref, force_buf), (sea_ref, sea_buf), (count_ref, count_buf))
    ]
    for load in inputs:
        load.start()
    barrier = pltpu.get_barrier_semaphore()
    for dlat in (-1, 1):
        @pl.when(has[dlat])
        def _(dlat=dlat):
            for dlon in (-1, 1):
                pl.semaphore_signal(barrier, inc=1, device_id=at(dlon, dlat), device_id_type=MESH)
    for off in range(1, n_lat):
        pl.semaphore_signal(barrier, inc=1, device_id=at(0, off), device_id_type=MESH)
    for off in range(1, n_lon):
        pl.semaphore_signal(barrier, inc=1, device_id=at(off, 0), device_id_type=MESH)

    for j in range(rows):
        pltpu.make_async_copy(state_ref.at[:, j, :], q_ref.at[j + 2, pl.ds(0, planes)], load_sem.at[1]).start()

    def remote(src, dst, sent, sem, where):
        return pltpu.make_async_remote_copy(
            src_ref=src, dst_ref=dst, send_sem=send_sem.at[sent], recv_sem=sem,
            device_id=where, device_id_type=MESH,
        )

    def drained(ref, sem):
        pltpu.make_async_copy(ref, ref, sem).wait()

    lane8 = lax.broadcasted_iota(jnp.int32, (SUB, 128), 1)
    sub8 = lax.broadcasted_iota(jnp.int32, (SUB, 128), 0)
    kio = [(sub8 + SUB * t).astype(jnp.float32) for t in range(depth_tiles)]
    slot8 = lane8 % 4
    last_lane, first_lane = lane8 == 127, lane8 == 0
    own = pl.ds(planes, SUB)

    def tile(t):
        return pl.ds(SUB * t, SUB)

    sides = ((0, -1), (1, 1))
    for v, dlat in sides:
        @pl.when(jnp.logical_not(has[-dlat]))
        def _(v=v):
            if v == 0:
                north_ref[...] = jnp.zeros_like(north_ref)
            corner_in[v] = jnp.zeros_like(corner_in[v])
            for r in range(2):
                jj = rows + 2 + r if v == 0 else r
                q_ref[jj] = jnp.zeros_like(q_ref[jj])

    drained(meter_ref.at[pl.ds(0, 3 * rows)], load_sem.at[0])
    lane_r = lax.broadcasted_iota(jnp.int32, (rows, 128), 1)
    sea = sea_buf[...].astype(jnp.float32)
    wet = sea * count_buf[...].astype(jnp.float32)
    force = sea * force_buf[...]
    pair_ref[0] = force
    pair_ref[1] = wet
    inner_half = jnp.where(lane_r < 64, pltpu.roll(force, 32, 1), pltpu.roll(force, 96, 1))
    pack_ref[...] = jnp.where((lane_r >= 32) & (lane_r < 96), inner_half, wet)
    for j in range(rows):
        q_ref[j + 2, own, :] = jnp.broadcast_to(wet[j : j + 1], (SUB, 128))

    early = ilat < n_lat // 4

    def prepare():
        pltpu.make_async_copy(
            q_ref.at[pl.ds(2, rows), pl.ds(0, planes)], q_ref.at[pl.ds(2, rows), pl.ds(0, planes)], load_sem.at[1]
        ).wait()

        packed = [jnp.zeros((SUB, 128), jnp.float32)] * (tiles + 1)
        for j in range(rows):
            here = lane8 // 4 == j + 1
            level = q_ref[j + 2, own, :]
            active = [k < level for k in kio]
            for t in range(tiles + 1):
                if t < tiles:
                    q = jnp.where(active[t % depth_tiles], q_ref[j + 2, tile(t), :], 0.0)
                    q_ref[j + 2, tile(t), :] = q
                else:
                    q = level
                packed[t] = jnp.where(here, pltpu.roll(q, 4 * (j + 1) + 2, 1), packed[t])
        corners = [jnp.zeros((SUB, 128), jnp.float32)] * 2
        for t in range(tiles + 1):
            strip_own[tile(t), :] = packed[t]
            for v, j in ((0, 0), (1, rows - 1)):
                moved = pltpu.roll(packed[t], (4 * t - 4 * (j + 1)) % 128, 1)
                corners[v] = jnp.where(lane8 // 4 == t, moved, corners[v])
        for t in range(0, tiles + 1, 2):
            odd = packed[min(t + 1, tiles)]
            strip_out[0, tile(t // 2), :] = jnp.where(slot8 < 2, packed[t], pltpu.roll(odd, 2, 1))
            strip_out[1, tile(t // 2), :] = jnp.where(slot8 < 2, pltpu.roll(packed[t], 126, 1), odd)
        for v in range(2):
            corner_out[v] = corners[v]

    @pl.when(early)
    def _():
        prepare()

    diagonals = 2 * (has[1].astype(jnp.int32) + has[-1].astype(jnp.int32))
    pl.semaphore_wait(barrier, n_lon + n_lat - 2 + diagonals)

    for h, dlon in ((0, 1), (1, -1)):
        remote(pack_ref, side_ref.at[h], 2, one_sem.at[0], at(dlon, 0)).start()
    for v, dlat, start, vert in ((0, -1, 0, north_ref), (1, 1, rows - SUB, south_ref)):
        @pl.when(has[dlat])
        def _(v=v, dlat=dlat, start=start, vert=vert):
            part = pl.ds(start, vert.shape[1])
            for h, dlon in ((0, 1), (1, -1)):
                remote(pack_ref.at[part], vert.at[2 + h], v, vert_sem.at[v], at(dlon, dlat)).start()
            remote(pair_ref.at[:, part], vert.at[pl.ds(0, 2)], v, vert_sem.at[v], at(0, dlat)).start()

    for off in range(1, n_lat):
        pl.semaphore_signal(ready_sem, inc=1, device_id=at(0, off), device_id_type=MESH)

    @pl.when(jnp.logical_not(early))
    def _():
        prepare()

    for h, dlon in ((0, 1), (1, -1)):
        remote(strip_out.at[h], strip_in.at[h], 2, one_sem.at[1], at(dlon, 0)).start()
    for v, dlat in sides:
        @pl.when(has[dlat])
        def _(v=v, dlat=dlat):
            for h, dlon in ((0, 1), (1, -1)):
                remote(corner_out.at[v], corner_in.at[v, h], v, corner_sem.at[v], at(dlon, dlat)).start()

    late, middle = ilat >= n_lat - n_lat // 4, ilat >= n_lat // 2

    def send_row(r, now):
        for v, dlat in sides:
            @pl.when(jnp.logical_and(has[dlat], now))
            def _(v=v, dlat=dlat):
                mine = pl.ds((2 if v == 0 else rows) + r, 1)
                there = pl.ds((rows + 2 if v == 0 else 0) + r, 1)
                remote(q_ref.at[mine], q_ref.at[there], v, row_sem.at[v], at(0, dlat)).start()

    send_row(0, jnp.logical_not(late))
    send_row(1, jnp.logical_not(middle))

    def received(ref, sems, v, dlat):
        @pl.when(has[-dlat])
        def _():
            drained(ref, sems.at[v])

    lane_t = lax.broadcasted_iota(jnp.int32, (rows + 2 * SUB, 128), 1)
    row_t = lax.broadcasted_iota(jnp.int32, (rows + 2 * SUB, 128), 0)

    def krylov(parts, closed):
        from_west = jnp.concatenate([side_ref[0]] + [p[2] for p in parts], axis=0)
        from_east = jnp.concatenate([side_ref[1]] + [p[3] for p in parts], axis=0)
        low = lane_t < 64
        force_a = jnp.concatenate([pair_ref[0]] + [p[0] for p in parts], axis=0)
        wet_a = jnp.concatenate([pair_ref[1]] + [p[1] for p in parts], axis=0)
        wet_b = jnp.where(low, from_east, from_west)
        force_b = jnp.where(low, pltpu.roll(from_east, 96, 1), pltpu.roll(from_west, 32, 1))
        depth_a, depth_b = wet_a / levels, wet_b / levels
        da, db = east(depth_a, depth_b, lane_t)
        ea, eb = jnp.minimum(depth_a, da), jnp.minimum(depth_b, db)
        da, db = west(depth_a, depth_b, lane_t)
        wa, wb = jnp.minimum(depth_a, da), jnp.minimum(depth_b, db)
        na, nb = jnp.minimum(depth_a, north(depth_a)), jnp.minimum(depth_b, north(depth_b))
        sa, sb = south(na), south(nb)
        if closed:
            sa, sb = (jnp.where(row_t > 0, x, 0.0) for x in (sa, sb))
        diag_a = DAMPING + ea + wa + na + sa
        diag_b = DAMPING + eb + wb + nb + sb
        inv_a, inv_b = 1.0 / diag_a, 1.0 / diag_b
        va, vb = force_a * inv_a, force_b * inv_b
        ea, wa, na, sa = (c * inv_a for c in (ea, wa, na, sa))
        eb, wb, nb, sb = (c * inv_b for c in (eb, wb, nb, sb))
        basis = [va]
        for _ in range(ITERS):
            qe, qeb = east(va, vb, lane_t)
            qw, qwb = west(va, vb, lane_t)
            va, vb = (
                ea * qe + wa * qw + na * north(va) + sa * south(va),
                eb * qeb + wb * qwb + nb * north(vb) + sb * south(vb),
            )
            basis.append(va)
        return diag_a, basis

    def keep(diag, basis):
        diag_ref[...] = diag[:rows]
        for i, x in enumerate(basis):
            basis_ref[i] = x[:rows]

    margin = ITERS + 1
    drained(side_ref, one_sem.at[0])
    received(north_ref, vert_sem, 0, -1)
    diag, basis = krylov([north_ref], True)
    first = jnp.where(ilat > 0, margin, 0)
    counted = (row_t >= first) & (row_t < rows + margin)
    weight = jnp.where(counted, diag, 0.0)
    moments = []
    for m in range(2 * ITERS):
        moments.append(jnp.sum(weight * basis[m // 2] * basis[(m + 1) // 2], axis=0, keepdims=True))
    sums = jnp.broadcast_to(jnp.sum(jnp.concatenate(moments, axis=0), axis=1, keepdims=True), (2 * ITERS, 128))
    sums = jnp.where(lane8 // (128 // (2 * ITERS)) == sub8, sums, 0.0)
    part_ref[...] = jnp.sum(sums, axis=0, keepdims=True)
    pl.semaphore_wait(ready_sem, n_lat - 1)
    all_in[ilat * n_lon] = part_ref[...]
    for k in range(n_lat):
        for off in range(n_lon):
            def share(k=k, off=off):
                where = {"lon": lax.rem(ilon + off, n_lon), "lat": k}
                remote(part_ref, all_in.at[ilat * n_lon + off], 2, one_sem.at[2], where).start()

            if off:
                share()
            else:
                pl.when(ilat != k)(share)

    send_row(0, late)
    send_row(1, middle)

    @pl.when(ilat == 0)
    def _():
        keep(diag, basis)

    @pl.when(ilat > 0)
    def _():
        drained(south_ref, vert_sem.at[1])
        keep(*krylov([north_ref.at[:, pl.ds(0, SUB)], south_ref], False))

    drained(strip_in, one_sem.at[1])
    for v, dlat in sides:
        received(corner_in.at[v], corner_sem, v, dlat)

    def swap(x, step):
        return jnp.where(slot8 < 2, pltpu.roll(x, 128 - step, 1), pltpu.roll(x, step, 1))

    def arrange(t):
        west_pair, east_pair = strip_in[0, tile(t // 2), :], strip_in[1, tile(t // 2), :]
        if t % 2:
            west_pair = pltpu.roll(west_pair, 126, 1)
        else:
            east_pair = pltpu.roll(east_pair, 2, 1)
        g = jnp.where(slot8 < 2, west_pair, east_pair)
        for v, j in ((0, rows), (1, -1)):
            corner = jnp.where(slot8 < 2, corner_in[v, 0], corner_in[v, 1])
            moved = pltpu.roll(corner, (4 * (j + 1) - 4 * t) % 128, 1)
            g = jnp.where(lane8 // 4 == j + 1, moved, g)
        center = swap(g, 1)
        return center, strip_own[tile(t), :], swap(g, 2), pltpu.roll(center, 124, 1), pltpu.roll(center, 4, 1)

    ring = arrange(tiles)
    center_ref[tile(tiles), :] = ring[0]
    edge_coef = []
    for k in kio:
        count = sum(jnp.where(k < w, 1.0, 0.0) for w in ring[1:])
        first = jnp.where(k < ring[0], -VISCOSITY, 0.0)
        edge_coef.append((first, first * count))
    for t in range(tiles):
        center, a, b, c, d = arrange(t)
        center_ref[tile(t), :] = center
        first, second = edge_coef[t % depth_tiles]
        slap_ref[tile(t), :] = first * ((a + b) + (c + d)) - second * center

    def beside(x, edge):
        return (
            jnp.where(last_lane, edge, pltpu.roll(x, 127, 1)),
            jnp.where(first_lane, edge, pltpu.roll(x, 1, 1)),
        )

    def laplace(jj, inside):
        shift = 130 - 4 * jj

        def row_beside(x, where):
            return beside(x, pltpu.roll(center_ref[where, :], shift, 1))

        level = q_ref[jj, own, :]
        around = row_beside(level, own) + (q_ref[jj + 1, own, :], q_ref[jj - 1, own, :])
        for k in range(depth_tiles):
            here, oe, ow, on, os = (kio[k] < x for x in (level,) + around)
            ones = [jnp.where(x, 1.0, 0.0) for x in (oe, ow, on, os)]
            count = (ones[0] + ones[1]) + (ones[2] + ones[3])
            first = jnp.where(here, -VISCOSITY, 0.0)
            second = first * count

            def plane(f):
                at_tile = tile(f * depth_tiles + k)
                q = q_ref[jj, at_tile, :]
                qe, qw = row_beside(q, at_tile)
                qn, qs = q_ref[jj + 1, at_tile, :], q_ref[jj - 1, at_tile, :]
                lap_ref[jj - 1, at_tile, :] = first * ((qe + qw) + (qn + qs)) - second * q
                return q, qe, qw, qn, qs

            if not inside:
                for f in range(fields):
                    plane(f)
                continue
            near_ref[jj - 2, tile(k), :] = count
            quarter = jnp.where(here, 0.25, 0.0)
            planes_of = {2: plane(2), 3: plane(3)}
            u, ue, uw, _, _ = planes_of[2]
            v, _, _, vn, vs = planes_of[3]
            fe = jnp.where(oe, quarter * (u + ue), 0.0)
            fw = jnp.where(ow, quarter * (u + uw), 0.0)
            fn = jnp.where(on, quarter * (v + vn), 0.0)
            fs = jnp.where(os, quarter * (v + vs), 0.0)
            net = (fw - fe) + (fs - fn)
            for f in (2, 3, 0, 1):
                q, qe, qw, qn, qs = planes_of[f] if f in planes_of else plane(f)
                tend_ref[jj - 2, tile(f * depth_tiles + k), :] = (
                    net * q + (fw * qw - fe * qe) + (fs * qs - fn * qn)
                )

    def finish(j):
        shift = 122 - 4 * j
        level = q_ref[j + 2, own, :]
        for k in range(depth_tiles):
            here = kio[k] < level
            count = near_ref[j, tile(k), :]
            for f in range(fields):
                at_tile = tile(f * depth_tiles + k)
                lap = lap_ref[j + 1, at_tile, :]
                le, lw = beside(lap, pltpu.roll(slap_ref[at_tile, :], shift, 1))
                total = (le + lw) + (lap_ref[j + 2, at_tile, :] + lap_ref[j, at_tile, :])
                tend_ref[j, at_tile, :] += jnp.where(here, total, 0.0) - count * lap

    once = jnp.minimum(ilat + 1, 1)

    def ahead(_, carry):
        for jj in range(3, 9):
            laplace(jj, True)
        return carry

    lax.fori_loop(0, once, ahead, 0)

    def both(i, carry):
        for r in range(4):
            finish(4 * i + 2 + r)
        for r in range(4):
            laplace(4 * i + 9 + r, True)
        return carry

    lax.fori_loop(0, rows // 4 - 2, both, 0)
    for j in range(rows - 6, rows - 2):
        finish(j)

    for v, dlat in sides:
        rim = q_ref.at[pl.ds(rows + 2, 2)] if v == 0 else q_ref.at[pl.ds(0, 2)]
        received(rim, row_sem, v, dlat)

    def rim(_, carry):
        for jj, inside in ((1, False), (2, True), (rows + 1, True), (rows + 2, False)):
            laplace(jj, inside)
        for j in (0, 1, rows - 2, rows - 1):
            finish(j)
        return carry

    lax.fori_loop(0, once, rim, 0)

    drained(all_in.at[pl.ds(0, n_lon * n_lat - 1)], one_sem.at[2])
    terms = [all_in[i] for i in range(n_lon * n_lat)]
    while len(terms) > 1:
        terms = [a + b for a, b in zip(terms[::2], terms[1::2])] + terms[len(terms) - len(terms) % 2 :]
    total = terms[0]
    total_ref[...] = jnp.broadcast_to(total, total_ref.shape)

    half = strip_out.shape[1]
    drained(meter_ref.at[pl.ds(0, 2 * rows + 2 * half + n_lon * n_lat - 1)], send_sem.at[2])
    for v, dlat in sides:
        @pl.when(has[dlat])
        def _(v=v):
            vert = (north_ref, south_ref)[v].shape[1]
            drained(meter_ref.at[pl.ds(0, 4 * vert + 2 * SUB + 2 * (planes + SUB))], send_sem.at[v])


def deliver(tend_in, basis_in, diag_in, total_in, height_ref, resid_ref, tend_ref, height_buf, resid_buf, sem):
    rows = tend_in.shape[0]
    stores = [pltpu.make_async_copy(tend_in.at[j], tend_ref.at[:, j, :], sem.at[0]) for j in range(rows)]
    for store in stores:
        store.start()
    part = 128 // (2 * ITERS)
    shape = (2 * ITERS, 128)
    mine = lax.broadcasted_iota(jnp.int32, shape, 1) == part * lax.broadcasted_iota(jnp.int32, shape, 0)
    total = jnp.broadcast_to(jnp.sum(jnp.where(mine, total_in[...], 0.0), axis=1, keepdims=True), shape)
    mu = [total[m : m + 1] for m in range(2 * ITERS)]

    def inner(x, y):
        sums = [None] * (len(x) + len(y) - 1)
        for i, xi in enumerate(x):
            for j, yj in enumerate(y):
                sums[i + j] = xi * yj if sums[i + j] is None else sums[i + j] + xi * yj
        out = sums[0] * mu[0]
        for m in range(1, len(sums)):
            out = out + sums[m] * mu[m]
        return out

    one = jnp.ones((1, 128), jnp.float32)
    zero = jnp.zeros((1, 128), jnp.float32)
    z, p, h = [one], [one], []
    rz = mu[0]
    for it in range(ITERS):
        image = [hi - lo for hi, lo in zip(p + [zero], [zero] + p)]
        alpha = rz / inner(p, image)
        h = [x + alpha * y for x, y in zip(h + [zero], p)]
        z = [x - alpha * y for x, y in zip(z + [zero], image)]
        if it + 1 < ITERS:
            new = inner(z, z)
            beta = new / rz
            p = [x + beta * y for x, y in zip(z, p + [zero])]
            rz = new
    height = h[0] * basis_in[0]
    for i in range(1, ITERS):
        height = height + h[i] * basis_in[i]
    resid = z[0] * basis_in[0]
    for i in range(1, ITERS + 1):
        resid = resid + z[i] * basis_in[i]
    height_buf[...] = height
    resid_buf[...] = diag_in[...] * resid
    last = [
        pltpu.make_async_copy(height_buf, height_ref, sem.at[1]),
        pltpu.make_async_copy(resid_buf, resid_ref, sem.at[2]),
    ]
    for store in last:
        store.start()
    pltpu.make_async_copy(tend_in, tend_in, sem.at[0]).wait()
    for store in last:
        store.wait()


def per_device(n_lon, n_lat, forcing, sea, count, state):
    fields, levels, rows, width = state.shape
    planes = fields * levels
    tall = planes + SUB
    half = SUB * ((tall // SUB + 1) // 2)
    assert levels % SUB == 0 and width == 128 and rows % SUB == 0 and rows >= 2 * SUB and 2 * (ITERS + 1) <= 2 * SUB
    assert 4 * (rows + 2) <= width and 4 * (planes // SUB + 1) <= width
    sizes = (n_lon, n_lat, fields, levels, rows)
    f32 = jnp.float32
    vmem = pl.BlockSpec(memory_space=pltpu.VMEM)
    hbm = pl.BlockSpec(memory_space=pltpu.HBM)
    dma = pltpu.SemaphoreType.DMA
    held = pl.pallas_call(
        functools.partial(exchange, sizes),
        out_shape=(
            pltpu.VMEM((rows, planes, width), f32),
            pltpu.VMEM((ITERS + 1, rows, width), f32),
            pltpu.VMEM((rows, width), f32),
            pltpu.VMEM((2 * ITERS, width), f32),
        ),
        in_specs=[hbm] * 4,
        out_specs=(vmem,) * 4,
        scratch_shapes=[
            pltpu.VMEM((rows, width), f32),
            pltpu.VMEM((rows, width), jnp.int32),
            pltpu.VMEM((rows, width), jnp.int32),
            pltpu.VMEM((rows + 4, tall, width), f32),
            pltpu.VMEM((rows + 2, planes, width), f32),
            pltpu.VMEM((rows, levels, width), f32),
            pltpu.VMEM((rows, width), f32),
            pltpu.VMEM((2, rows, width), f32),
            pltpu.VMEM((2, rows, width), f32),
            pltpu.VMEM((4, 2 * SUB, width), f32),
            pltpu.VMEM((4, SUB, width), f32),
            pltpu.VMEM((tall, width), f32),
            pltpu.VMEM((2, half, width), f32),
            pltpu.VMEM((2, half, width), f32),
            pltpu.VMEM((2, SUB, width), f32),
            pltpu.VMEM((2, 2, SUB, width), f32),
            pltpu.VMEM((tall, width), f32),
            pltpu.VMEM((planes, width), f32),
            pltpu.VMEM((1, width), f32),
            pltpu.VMEM((n_lon * n_lat, 1, width), f32),
            pltpu.VMEM((max(10 * SUB + 2 * tall, 2 * rows + 2 * half + n_lon * n_lat), 1, width), f32),
            dma((2,)),
            dma((3,)),
            dma((3,)),
            dma((2,)),
            dma((2,)),
            dma((2,)),
            pltpu.SemaphoreType.REGULAR,
        ],
        compiler_params=pltpu.CompilerParams(collective_id=0, has_side_effects=True),
    )(forcing, sea, count, state.reshape(planes, rows, width))
    small = jax.ShapeDtypeStruct((rows, width), f32)
    height, resid, tend = pl.pallas_call(
        deliver,
        out_shape=(small, small, jax.ShapeDtypeStruct((planes, rows, width), f32)),
        in_specs=[vmem] * 4,
        out_specs=(hbm,) * 3,
        scratch_shapes=[
            pltpu.VMEM((rows, width), f32),
            pltpu.VMEM((rows, width), f32),
            dma((3,)),
        ],
        compiler_params=pltpu.CompilerParams(vmem_limit_bytes=16 << 20),
    )(*held)
    return height, resid, tend.reshape(state.shape)


def solution(mesh):
    return jax.shard_map(
        functools.partial(per_device, mesh.shape["lon"], mesh.shape["lat"]),
        mesh=mesh,
        in_specs=(P("lat", "lon"), P("lat", "lon"), P("lat", "lon"), P(None, None, "lat", "lon")),
        out_specs=(P("lat", "lon"), P("lat", "lon"), P(None, None, "lat", "lon")),
        check_vma=False,
    )
```

```python
import functools

import jax
import jax.numpy as jnp
from jax import lax
from jax.experimental import pallas as pl
from jax.experimental.pallas import tpu as pltpu
from jax.sharding import PartitionSpec as P

ITERS = 4
DAMPING = 0.05
VISCOSITY = 0.02
SUB = 8
MESH = pl.DeviceIdType.MESH


def east(a, b, lane):
    ra, rb = pltpu.roll(a, 127, 1), pltpu.roll(b, 127, 1)
    keep = lane < 127
    return jnp.where(keep, ra, rb), jnp.where(keep, rb, ra)


def west(a, b, lane):
    ra, rb = pltpu.roll(a, 1, 1), pltpu.roll(b, 1, 1)
    keep = lane > 0
    return jnp.where(keep, ra, rb), jnp.where(keep, rb, ra)


def north(x):
    return pltpu.roll(x, x.shape[0] - 1, 0)


def south(x):
    return pltpu.roll(x, 1, 0)


def exchange(
    sizes,
    forcing_ref, sea_ref, count_ref, state_ref,
    tend_ref, basis_ref, diag_ref, total_ref,
    force_buf, sea_buf, count_buf, q_ref, lap_ref, near_ref,
    pack_ref, side_ref, pair_ref, north_ref, south_ref,
    strip_own, strip_out, strip_in, corner_out, corner_in, center_ref, slap_ref,
    part_ref, all_in,
    meter_ref, load_sem, send_sem, one_sem, vert_sem, row_sem, corner_sem, ready_sem,
):
    n_lon, n_lat, fields, levels, rows = sizes
    planes = fields * levels
    depth_tiles = levels // SUB
    tiles = planes // SUB
    ilon, ilat = lax.axis_index("lon"), lax.axis_index("lat")
    has = {1: ilat < n_lat - 1, -1: ilat > 0}

    def at(dlon, dlat):
        return {
            "lon": lax.rem(ilon + dlon + n_lon, n_lon),
            "lat": lax.rem(ilat + dlat + n_lat, n_lat),
        }

    inputs = [
        pltpu.make_async_copy(src, dst, load_sem.at[0])
        for src, dst in ((forcing_ref, force_buf), (sea_ref, sea_buf), (count_ref, count_buf))
    ]
    for load in inputs:
        load.start()
    barrier = pltpu.get_barrier_semaphore()
    for dlat in (-1, 1):
        @pl.when(has[dlat])
        def _(dlat=dlat):
            for dlon in (-1, 1):
                pl.semaphore_signal(barrier, inc=1, device_id=at(dlon, dlat), device_id_type=MESH)
    for off in range(1, n_lat):
        pl.semaphore_signal(barrier, inc=1, device_id=at(0, off), device_id_type=MESH)
    for off in range(1, n_lon):
        pl.semaphore_signal(barrier, inc=1, device_id=at(off, 0), device_id_type=MESH)

    for j in range(rows):
        pltpu.make_async_copy(state_ref.at[:, j, :], q_ref.at[j + 2, pl.ds(0, planes)], load_sem.at[1]).start()

    def remote(src, dst, sent, sem, where):
        return pltpu.make_async_remote_copy(
            src_ref=src, dst_ref=dst, send_sem=send_sem.at[sent], recv_sem=sem,
            device_id=where, device_id_type=MESH,
        )

    def drained(ref, sem):
        pltpu.make_async_copy(ref, ref, sem).wait()

    lane8 = lax.broadcasted_iota(jnp.int32, (SUB, 128), 1)
    sub8 = lax.broadcasted_iota(jnp.int32, (SUB, 128), 0)
    kio = [(sub8 + SUB * t).astype(jnp.float32) for t in range(depth_tiles)]
    slot8 = lane8 % 4
    last_lane, first_lane = lane8 == 127, lane8 == 0
    own = pl.ds(planes, SUB)

    def tile(t):
        return pl.ds(SUB * t, SUB)

    sides = ((0, -1), (1, 1))
    for v, dlat in sides:
        @pl.when(jnp.logical_not(has[-dlat]))
        def _(v=v):
            if v == 0:
                north_ref[...] = jnp.zeros_like(north_ref)
            corner_in[v] = jnp.zeros_like(corner_in[v])
            for r in range(2):
                jj = rows + 2 + r if v == 0 else r
                q_ref[jj] = jnp.zeros_like(q_ref[jj])

    drained(meter_ref.at[pl.ds(0, 3 * rows)], load_sem.at[0])
    lane_r = lax.broadcasted_iota(jnp.int32, (rows, 128), 1)
    sea = sea_buf[...].astype(jnp.float32)
    wet = sea * count_buf[...].astype(jnp.float32)
    force = sea * force_buf[...]
    pair_ref[0] = force
    pair_ref[1] = wet
    inner_half = jnp.where(lane_r < 64, pltpu.roll(force, 32, 1), pltpu.roll(force, 96, 1))
    pack_ref[...] = jnp.where((lane_r >= 32) & (lane_r < 96), inner_half, wet)
    for j in range(rows):
        q_ref[j + 2, own, :] = jnp.broadcast_to(wet[j : j + 1], (SUB, 128))

    early = ilat < n_lat // 4

    def prepare():
        pltpu.make_async_copy(
            q_ref.at[pl.ds(2, rows), pl.ds(0, planes)], q_ref.at[pl.ds(2, rows), pl.ds(0, planes)], load_sem.at[1]
        ).wait()

        packed = [jnp.zeros((SUB, 128), jnp.float32)] * (tiles + 1)
        for j in range(rows):
            here = lane8 // 4 == j + 1
            level = q_ref[j + 2, own, :]
            active = [k < level for k in kio]
            for t in range(tiles + 1):
                if t < tiles:
                    q = jnp.where(active[t % depth_tiles], q_ref[j + 2, tile(t), :], 0.0)
                    q_ref[j + 2, tile(t), :] = q
                else:
                    q = level
                packed[t] = jnp.where(here, pltpu.roll(q, 4 * (j + 1) + 2, 1), packed[t])
        corners = [jnp.zeros((SUB, 128), jnp.float32)] * 2
        for t in range(tiles + 1):
            strip_own[tile(t), :] = packed[t]
            for v, j in ((0, 0), (1, rows - 1)):
                moved = pltpu.roll(packed[t], (4 * t - 4 * (j + 1)) % 128, 1)
                corners[v] = jnp.where(lane8 // 4 == t, moved, corners[v])
        for t in range(0, tiles + 1, 2):
            odd = packed[min(t + 1, tiles)]
            strip_out[0, tile(t // 2), :] = jnp.where(slot8 < 2, packed[t], pltpu.roll(odd, 2, 1))
            strip_out[1, tile(t // 2), :] = jnp.where(slot8 < 2, pltpu.roll(packed[t], 126, 1), odd)
        for v in range(2):
            corner_out[v] = corners[v]

    @pl.when(early)
    def _():
        prepare()

    diagonals = 2 * (has[1].astype(jnp.int32) + has[-1].astype(jnp.int32))
    pl.semaphore_wait(barrier, n_lon + n_lat - 2 + diagonals)

    for h, dlon in ((0, 1), (1, -1)):
        remote(pack_ref, side_ref.at[h], 2, one_sem.at[0], at(dlon, 0)).start()
    for v, dlat, start, vert in ((0, -1, 0, north_ref), (1, 1, rows - SUB, south_ref)):
        @pl.when(has[dlat])
        def _(v=v, dlat=dlat, start=start, vert=vert):
            part = pl.ds(start, vert.shape[1])
            for h, dlon in ((0, 1), (1, -1)):
                remote(pack_ref.at[part], vert.at[2 + h], v, vert_sem.at[v], at(dlon, dlat)).start()
            remote(pair_ref.at[:, part], vert.at[pl.ds(0, 2)], v, vert_sem.at[v], at(0, dlat)).start()

    for off in range(1, n_lat):
        pl.semaphore_signal(ready_sem, inc=1, device_id=at(0, off), device_id_type=MESH)

    @pl.when(jnp.logical_not(early))
    def _():
        prepare()

    for h, dlon in ((0, 1), (1, -1)):
        remote(strip_out.at[h], strip_in.at[h], 2, one_sem.at[1], at(dlon, 0)).start()
    for v, dlat in sides:
        @pl.when(has[dlat])
        def _(v=v, dlat=dlat):
            for h, dlon in ((0, 1), (1, -1)):
                remote(corner_out.at[v], corner_in.at[v, h], v, corner_sem.at[v], at(dlon, dlat)).start()

    late, middle = ilat >= n_lat - n_lat // 4, ilat >= n_lat // 2

    def send_row(r, now):
        for v, dlat in sides:
            @pl.when(jnp.logical_and(has[dlat], now))
            def _(v=v, dlat=dlat):
                mine = pl.ds((2 if v == 0 else rows) + r, 1)
                there = pl.ds((rows + 2 if v == 0 else 0) + r, 1)
                remote(q_ref.at[mine], q_ref.at[there], v, row_sem.at[v], at(0, dlat)).start()

    send_row(0, jnp.logical_not(late))
    send_row(1, jnp.logical_not(middle))

    def received(ref, sems, v, dlat):
        @pl.when(has[-dlat])
        def _():
            drained(ref, sems.at[v])

    lane_t = lax.broadcasted_iota(jnp.int32, (rows + 2 * SUB, 128), 1)
    row_t = lax.broadcasted_iota(jnp.int32, (rows + 2 * SUB, 128), 0)

    def krylov(parts, closed):
        from_west = jnp.concatenate([side_ref[0]] + [p[2] for p in parts], axis=0)
        from_east = jnp.concatenate([side_ref[1]] + [p[3] for p in parts], axis=0)
        low = lane_t < 64
        force_a = jnp.concatenate([pair_ref[0]] + [p[0] for p in parts], axis=0)
        wet_a = jnp.concatenate([pair_ref[1]] + [p[1] for p in parts], axis=0)
        wet_b = jnp.where(low, from_east, from_west)
        force_b = jnp.where(low, pltpu.roll(from_east, 96, 1), pltpu.roll(from_west, 32, 1))
        depth_a, depth_b = wet_a / levels, wet_b / levels
        da, db = east(depth_a, depth_b, lane_t)
        ea, eb = jnp.minimum(depth_a, da), jnp.minimum(depth_b, db)
        da, db = west(depth_a, depth_b, lane_t)
        wa, wb = jnp.minimum(depth_a, da), jnp.minimum(depth_b, db)
        na, nb = jnp.minimum(depth_a, north(depth_a)), jnp.minimum(depth_b, north(depth_b))
        sa, sb = south(na), south(nb)
        if closed:
            sa, sb = (jnp.where(row_t > 0, x, 0.0) for x in (sa, sb))
        diag_a = DAMPING + ea + wa + na + sa
        diag_b = DAMPING + eb + wb + nb + sb
        inv_a, inv_b = 1.0 / diag_a, 1.0 / diag_b
        va, vb = force_a * inv_a, force_b * inv_b
        ea, wa, na, sa = (c * inv_a for c in (ea, wa, na, sa))
        eb, wb, nb, sb = (c * inv_b for c in (eb, wb, nb, sb))
        basis = [va]
        for _ in range(ITERS):
            qe, qeb = east(va, vb, lane_t)
            qw, qwb = west(va, vb, lane_t)
            va, vb = (
                ea * qe + wa * qw + na * north(va) + sa * south(va),
                eb * qeb + wb * qwb + nb * north(vb) + sb * south(vb),
            )
            basis.append(va)
        return diag_a, basis

    def keep(diag, basis):
        diag_ref[...] = diag[:rows]
        for i, x in enumerate(basis):
            basis_ref[i] = x[:rows]

    margin = ITERS + 1
    drained(side_ref, one_sem.at[0])
    received(north_ref, vert_sem, 0, -1)
    diag, basis = krylov([north_ref], True)
    first = jnp.where(ilat > 0, margin, 0)
    counted = (row_t >= first) & (row_t < rows + margin)
    weight = jnp.where(counted, diag, 0.0)
    moments = []
    for m in range(2 * ITERS):
        moments.append(jnp.sum(weight * basis[m // 2] * basis[(m + 1) // 2], axis=0, keepdims=True))
    sums = jnp.broadcast_to(jnp.sum(jnp.concatenate(moments, axis=0), axis=1, keepdims=True), (2 * ITERS, 128))
    sums = jnp.where(lane8 // (128 // (2 * ITERS)) == sub8, sums, 0.0)
    part_ref[...] = jnp.sum(sums, axis=0, keepdims=True)
    pl.semaphore_wait(ready_sem, n_lat - 1)
    all_in[ilat * n_lon] = part_ref[...]
    for k in range(n_lat):
        for off in range(n_lon):
            def share(k=k, off=off):
                where = {"lon": lax.rem(ilon + off, n_lon), "lat": k}
                remote(part_ref, all_in.at[ilat * n_lon + off], 2, one_sem.at[2], where).start()

            if off:
                share()
            else:
                pl.when(ilat != k)(share)

    send_row(0, late)
    send_row(1, middle)

    @pl.when(ilat == 0)
    def _():
        keep(diag, basis)

    @pl.when(ilat > 0)
    def _():
        drained(south_ref, vert_sem.at[1])
        keep(*krylov([north_ref.at[:, pl.ds(0, SUB)], south_ref], False))

    drained(strip_in, one_sem.at[1])
    for v, dlat in sides:
        received(corner_in.at[v], corner_sem, v, dlat)

    def swap(x, step):
        return jnp.where(slot8 < 2, pltpu.roll(x, 128 - step, 1), pltpu.roll(x, step, 1))

    def arrange(t):
        west_pair, east_pair = strip_in[0, tile(t // 2), :], strip_in[1, tile(t // 2), :]
        if t % 2:
            west_pair = pltpu.roll(west_pair, 126, 1)
        else:
            east_pair = pltpu.roll(east_pair, 2, 1)
        g = jnp.where(slot8 < 2, west_pair, east_pair)
        for v, j in ((0, rows), (1, -1)):
            corner = jnp.where(slot8 < 2, corner_in[v, 0], corner_in[v, 1])
            moved = pltpu.roll(corner, (4 * (j + 1) - 4 * t) % 128, 1)
            g = jnp.where(lane8 // 4 == j + 1, moved, g)
        center = swap(g, 1)
        return center, strip_own[tile(t), :], swap(g, 2), pltpu.roll(center, 124, 1), pltpu.roll(center, 4, 1)

    ring = arrange(tiles)
    center_ref[tile(tiles), :] = ring[0]
    edge_coef = []
    for k in kio:
        count = sum(jnp.where(k < w, 1.0, 0.0) for w in ring[1:])
        first = jnp.where(k < ring[0], -VISCOSITY, 0.0)
        edge_coef.append((first, first * count))
    for t in range(tiles):
        center, a, b, c, d = arrange(t)
        center_ref[tile(t), :] = center
        first, second = edge_coef[t % depth_tiles]
        slap_ref[tile(t), :] = first * ((a + b) + (c + d)) - second * center

    def beside(x, edge):
        return (
            jnp.where(last_lane, edge, pltpu.roll(x, 127, 1)),
            jnp.where(first_lane, edge, pltpu.roll(x, 1, 1)),
        )

    def laplace(jj, inside):
        shift = 130 - 4 * jj

        def row_beside(x, where):
            return beside(x, pltpu.roll(center_ref[where, :], shift, 1))

        level = q_ref[jj, own, :]
        around = row_beside(level, own) + (q_ref[jj + 1, own, :], q_ref[jj - 1, own, :])
        for k in range(depth_tiles):
            here, oe, ow, on, os = (kio[k] < x for x in (level,) + around)
            ones = [jnp.where(x, 1.0, 0.0) for x in (oe, ow, on, os)]
            count = (ones[0] + ones[1]) + (ones[2] + ones[3])
            first = jnp.where(here, -VISCOSITY, 0.0)
            second = first * count

            def plane(f):
                at_tile = tile(f * depth_tiles + k)
                q = q_ref[jj, at_tile, :]
                qe, qw = row_beside(q, at_tile)
                qn, qs = q_ref[jj + 1, at_tile, :], q_ref[jj - 1, at_tile, :]
                lap_ref[jj - 1, at_tile, :] = first * ((qe + qw) + (qn + qs)) - second * q
                return q, qe, qw, qn, qs

            if not inside:
                for f in range(fields):
                    plane(f)
                continue
            near_ref[jj - 2, tile(k), :] = count
            quarter = jnp.where(here, 0.25, 0.0)
            planes_of = {2: plane(2), 3: plane(3)}
            u, ue, uw, _, _ = planes_of[2]
            v, _, _, vn, vs = planes_of[3]
            fe = jnp.where(oe, quarter * (u + ue), 0.0)
            fw = jnp.where(ow, quarter * (u + uw), 0.0)
            fn = jnp.where(on, quarter * (v + vn), 0.0)
            fs = jnp.where(os, quarter * (v + vs), 0.0)
            net = (fw - fe) + (fs - fn)
            for f in (2, 3, 0, 1):
                q, qe, qw, qn, qs = planes_of[f] if f in planes_of else plane(f)
                tend_ref[jj - 2, tile(f * depth_tiles + k), :] = (
                    net * q + (fw * qw - fe * qe) + (fs * qs - fn * qn)
                )

    def finish(j):
        shift = 122 - 4 * j
        level = q_ref[j + 2, own, :]
        for k in range(depth_tiles):
            here = kio[k] < level
            count = near_ref[j, tile(k), :]
            for f in range(fields):
                at_tile = tile(f * depth_tiles + k)
                lap = lap_ref[j + 1, at_tile, :]
                le, lw = beside(lap, pltpu.roll(slap_ref[at_tile, :], shift, 1))
                total = (le + lw) + (lap_ref[j + 2, at_tile, :] + lap_ref[j, at_tile, :])
                tend_ref[j, at_tile, :] += jnp.where(here, total, 0.0) - count * lap

    once = jnp.minimum(ilat + 1, 1)

    def ahead(_, carry):
        for jj in range(3, 9):
            laplace(jj, True)
        return carry

    lax.fori_loop(0, once, ahead, 0)

    def both(i, carry):
        for r in range(4):
            finish(4 * i + 2 + r)
        for r in range(4):
            laplace(4 * i + 9 + r, True)
        return carry

    lax.fori_loop(0, rows // 4 - 2, both, 0)
    for v, dlat in sides:
        rim = q_ref.at[pl.ds(rows + 2, 2)] if v == 0 else q_ref.at[pl.ds(0, 2)]
        received(rim, row_sem, v, dlat)

    def rim(_, carry):
        for jj, inside in ((1, False), (2, True), (rows + 1, True), (rows + 2, False)):
            laplace(jj, inside)
        for j in (*range(rows - 6, rows - 2), 0, 1, rows - 2, rows - 1):
            finish(j)
        return carry

    lax.fori_loop(0, once, rim, 0)

    drained(all_in.at[pl.ds(0, n_lon * n_lat - 1)], one_sem.at[2])
    terms = [all_in[i] for i in range(n_lon * n_lat)]
    while len(terms) > 1:
        terms = [a + b for a, b in zip(terms[::2], terms[1::2])] + terms[len(terms) - len(terms) % 2 :]
    total = terms[0]
    total_ref[...] = jnp.broadcast_to(total, total_ref.shape)

    half = strip_out.shape[1]
    drained(meter_ref.at[pl.ds(0, 2 * rows + 2 * half + n_lon * n_lat - 1)], send_sem.at[2])
    for v, dlat in sides:
        @pl.when(has[dlat])
        def _(v=v):
            vert = (north_ref, south_ref)[v].shape[1]
            drained(meter_ref.at[pl.ds(0, 4 * vert + 2 * SUB + 2 * (planes + SUB))], send_sem.at[v])


def deliver(tend_in, basis_in, diag_in, total_in, height_ref, resid_ref, tend_ref, height_buf, resid_buf, sem):
    rows = tend_in.shape[0]
    stores = [pltpu.make_async_copy(tend_in.at[j], tend_ref.at[:, j, :], sem.at[0]) for j in range(rows)]
    for store in stores:
        store.start()
    part = 128 // (2 * ITERS)
    shape = (2 * ITERS, 128)
    mine = lax.broadcasted_iota(jnp.int32, shape, 1) == part * lax.broadcasted_iota(jnp.int32, shape, 0)
    total = jnp.broadcast_to(jnp.sum(jnp.where(mine, total_in[...], 0.0), axis=1, keepdims=True), shape)
    mu = [total[m : m + 1] for m in range(2 * ITERS)]

    def inner(x, y):
        sums = [None] * (len(x) + len(y) - 1)
        for i, xi in enumerate(x):
            for j, yj in enumerate(y):
                sums[i + j] = xi * yj if sums[i + j] is None else sums[i + j] + xi * yj
        out = sums[0] * mu[0]
        for m in range(1, len(sums)):
            out = out + sums[m] * mu[m]
        return out

    one = jnp.ones((1, 128), jnp.float32)
    zero = jnp.zeros((1, 128), jnp.float32)
    z, p, h = [one], [one], []
    rz = mu[0]
    for it in range(ITERS):
        image = [hi - lo for hi, lo in zip(p + [zero], [zero] + p)]
        alpha = rz / inner(p, image)
        h = [x + alpha * y for x, y in zip(h + [zero], p)]
        z = [x - alpha * y for x, y in zip(z + [zero], image)]
        if it + 1 < ITERS:
            new = inner(z, z)
            beta = new / rz
            p = [x + beta * y for x, y in zip(z, p + [zero])]
            rz = new
    height = h[0] * basis_in[0]
    for i in range(1, ITERS):
        height = height + h[i] * basis_in[i]
    resid = z[0] * basis_in[0]
    for i in range(1, ITERS + 1):
        resid = resid + z[i] * basis_in[i]
    height_buf[...] = height
    resid_buf[...] = diag_in[...] * resid
    last = [
        pltpu.make_async_copy(height_buf, height_ref, sem.at[1]),
        pltpu.make_async_copy(resid_buf, resid_ref, sem.at[2]),
    ]
    for store in last:
        store.start()
    pltpu.make_async_copy(tend_in, tend_in, sem.at[0]).wait()
    for store in last:
        store.wait()


def per_device(n_lon, n_lat, forcing, sea, count, state):
    fields, levels, rows, width = state.shape
    planes = fields * levels
    tall = planes + SUB
    half = SUB * ((tall // SUB + 1) // 2)
    assert levels % SUB == 0 and width == 128 and rows % SUB == 0 and rows >= 2 * SUB and 2 * (ITERS + 1) <= 2 * SUB
    assert 4 * (rows + 2) <= width and 4 * (planes // SUB + 1) <= width
    sizes = (n_lon, n_lat, fields, levels, rows)
    f32 = jnp.float32
    vmem = pl.BlockSpec(memory_space=pltpu.VMEM)
    hbm = pl.BlockSpec(memory_space=pltpu.HBM)
    dma = pltpu.SemaphoreType.DMA
    held = pl.pallas_call(
        functools.partial(exchange, sizes),
        out_shape=(
            pltpu.VMEM((rows, planes, width), f32),
            pltpu.VMEM((ITERS + 1, rows, width), f32),
            pltpu.VMEM((rows, width), f32),
            pltpu.VMEM((2 * ITERS, width), f32),
        ),
        in_specs=[hbm] * 4,
        out_specs=(vmem,) * 4,
        scratch_shapes=[
            pltpu.VMEM((rows, width), f32),
            pltpu.VMEM((rows, width), jnp.int32),
            pltpu.VMEM((rows, width), jnp.int32),
            pltpu.VMEM((rows + 4, tall, width), f32),
            pltpu.VMEM((rows + 2, planes, width), f32),
            pltpu.VMEM((rows, levels, width), f32),
            pltpu.VMEM((rows, width), f32),
            pltpu.VMEM((2, rows, width), f32),
            pltpu.VMEM((2, rows, width), f32),
            pltpu.VMEM((4, 2 * SUB, width), f32),
            pltpu.VMEM((4, SUB, width), f32),
            pltpu.VMEM((tall, width), f32),
            pltpu.VMEM((2, half, width), f32),
            pltpu.VMEM((2, half, width), f32),
            pltpu.VMEM((2, SUB, width), f32),
            pltpu.VMEM((2, 2, SUB, width), f32),
            pltpu.VMEM((tall, width), f32),
            pltpu.VMEM((planes, width), f32),
            pltpu.VMEM((1, width), f32),
            pltpu.VMEM((n_lon * n_lat, 1, width), f32),
            pltpu.VMEM((max(10 * SUB + 2 * tall, 2 * rows + 2 * half + n_lon * n_lat), 1, width), f32),
            dma((2,)),
            dma((3,)),
            dma((3,)),
            dma((2,)),
            dma((2,)),
            dma((2,)),
            pltpu.SemaphoreType.REGULAR,
        ],
        compiler_params=pltpu.CompilerParams(collective_id=0, has_side_effects=True),
    )(forcing, sea, count, state.reshape(planes, rows, width))
    small = jax.ShapeDtypeStruct((rows, width), f32)
    height, resid, tend = pl.pallas_call(
        deliver,
        out_shape=(small, small, jax.ShapeDtypeStruct((planes, rows, width), f32)),
        in_specs=[vmem] * 4,
        out_specs=(hbm,) * 3,
        scratch_shapes=[
            pltpu.VMEM((rows, width), f32),
            pltpu.VMEM((rows, width), f32),
            dma((3,)),
        ],
        compiler_params=pltpu.CompilerParams(vmem_limit_bytes=16 << 20),
    )(*held)
    return height, resid, tend.reshape(state.shape)


def solution(mesh):
    return jax.shard_map(
        functools.partial(per_device, mesh.shape["lon"], mesh.shape["lat"]),
        mesh=mesh,
        in_specs=(P("lat", "lon"), P("lat", "lon"), P("lat", "lon"), P(None, None, "lat", "lon")),
        out_specs=(P("lat", "lon"), P("lat", "lon"), P(None, None, "lat", "lon")),
        check_vma=False,
    )
```
